32 devices in a mesh: seq: 16 (over z, x, core), row: 2 (over y).
Axes of the slice: x: 2, y: 2, z: 4, core: 2. Of those that a mesh axis runs over, the one named last changes fastest.
Arguments:
- patch_queries: bfloat16 [2048, 2048], P('seq', 'row'), may hold values from -15 to 15
- patch_keys: bfloat16 [2048, 2048], P('seq', 'row'), may hold values from -15 to 15
- patch_values: bfloat16 [2048, 2048], P('seq', 'row'), may hold values from -6 to 6
- patch_tasks: int32 [2048], P('seq'), may hold values from 0 to 7
- residual: bfloat16 [2048, 2048], P('seq', 'row'), may hold values from -6 to 6
- output_weight: bfloat16 [2048, 2048], P('row'), may hold values from -0.5 to 0.5
- global_down: bfloat16 [2048, 16], P('row'), may hold values from -0.5 to 0.5
- global_up: bfloat16 [16, 2048], P(None, 'row'), may hold values from -1.5 to 1.5
- global_scales: float32 [8, 16], replicated, may hold values from 0.25 to 4
- local_weight: bfloat16 [2048, 512], P('row'), may hold values from -0.125 to 0.125
- byte_ids: int32 [16384], P('seq'), may hold values from 0 to 255
- byte_table: bfloat16 [256, 512], replicated, may hold values from -6 to 6
- position_table: bfloat16 [8, 512], replicated, may hold values from -6 to 6
- norm_gain: float32 [512], replicated, may hold values from 0.5 to 1.5
- hidden_in: bfloat16 [2048, 512], P('row', 'seq'), may hold values from -0.25 to 0.25
- hidden_out: bfloat16 [2048, 512], P('row', 'seq'), may hold values from -0.125 to 0.125
- local_down: bfloat16 [512, 16], replicated, may hold values from -0.25 to 0.25
- local_up: bfloat16 [16, 2048], P(None, 'row'), may hold values from -1.5 to 1.5
- local_scales: float32 [8, 16], replicated, may hold values from 0.25 to 4
- cotangent: bfloat16 [16384, 512], P(('seq', 'row')), may hold values from -6 to 6
Outputs:
- grad_global_down: float32 [2048, 16], P('row')
- grad_global_up: float32 [16, 2048], P(None, 'row')
- grad_global_scales: float32 [8, 16], replicated
- grad_local_down: float32 [512, 16], replicated
- grad_local_up: float32 [16, 2048], P(None, 'row')
- grad_local_scales: float32 [8, 16], replicated
The draws below stay inside these ranges and needn't reach their ends.
All inputs are finite; a program needn't handle non-finite values.
Results may differ from the reference program's by a relative error of at most 0.028.
Values may be sent and summed in bfloat16 or wider, within the bound.
A program may use at most 64 MiB of HBM per device.

```python
import math
import jax
import jax.numpy as jnp
import numpy as np
from jax import lax

D = 2048
HEADS = 16
HEAD = 128
L = 512
FF_L = 2048
VOCAB = 256
PATCH = 8
RANK = 16
TASKS = 8
PATCHES = 2048
BYTES = 16384
N_ROW = 2


def draw_patch_queries(key, part):
    values = 2.5 * jnp.clip(jax.random.normal(jax.random.fold_in(key, 11), (PATCHES, HEADS * HEAD), jnp.float32), -6.0, 6.0)
    return values.astype(jnp.bfloat16)


def draw_patch_keys(key, part):
    values = jnp.clip(jax.random.normal(jax.random.fold_in(key, 13), (PATCHES, HEADS * HEAD), jnp.float32), -6.0, 6.0)
    return values.astype(jnp.bfloat16)


def plant(array, rng, least, high):
    longest = array.shape.index(max(array.shape))
    spots = []
    for shift in (0, 1):
        where = [jax.random.randint(jax.random.fold_in(rng, axis), (), 0, length) for axis, length in enumerate(array.shape)]
        where[longest] = (where[longest] + shift) % array.shape[longest]
        spots.append(tuple(where))
    return array.at[spots[0]].set(least).at[spots[1]].set(high)


def block_scale(own_key, shape, pieces, smallest, largest):
    loudness = 1.0
    for axis_at, blocks in pieces:
        draws = jax.random.uniform(jax.random.fold_in(jax.random.fold_in(own_key, 6), axis_at), (blocks,), jnp.float32, smallest / len(pieces), largest / len(pieces))
        loudness = loudness * jnp.repeat(jnp.exp(draws), shape[axis_at] // blocks).reshape((-1,) + (1,) * (len(shape) - 1 - axis_at))
    return loudness


def rank_table(count, skew):
    portions = [(1 << 20) // math.isqrt(rank ** skew) + 1 for rank in range(1, count + 1)]
    scale = 1 + sum(portions) // (1 << 30)
    return np.cumsum(np.array([max(1, weight // scale) for weight in portions]))


def skewed_ids(stream_key, dims, count, lean):
    table = rank_table(count, lean)
    lot = jax.random.randint(jax.random.fold_in(stream_key, 1), dims, 0, int(table[count - 1]))
    grade = jnp.searchsorted(jnp.asarray(table, jnp.int32), lot, side="right")
    return jax.random.permutation(jax.random.fold_in(stream_key, 2), count)[grade].astype(jnp.int32)


def centred(own_key, shape, spread, bound, pieces=(), held_as=jnp.bfloat16):
    loudness = block_scale(own_key, shape, pieces, -0.22, 0.18) if pieces else 1.0
    result = jax.random.normal(own_key, shape, jnp.float32) * spread * loudness
    return jnp.minimum(jnp.maximum(result, -bound), bound).astype(held_as)


def setup_inputs(seed: int = 0) -> dict:
    seeds = jax.random.split(jax.random.key(seed), 21)
    patch_queries = draw_patch_queries(jax.random.fold_in(seeds[20], 71), 0)
    patch_keys = draw_patch_keys(jax.random.fold_in(seeds[20], 71), 0)
    patch_values = centred(seeds[2], (PATCHES, HEADS * HEAD), 1.0, 6.0, ((0, 16), (1, 2)))
    patch_tasks = plant(jax.random.randint(seeds[3], (PATCHES,), 0, TASKS), jax.random.fold_in(seeds[3], 1), 0, TASKS - 1).astype(jnp.int32)
    residual = centred(seeds[4], (PATCHES, D), 1.0, 6.0, ((0, 16), (1, 2)))
    output_weight = centred(seeds[5], (HEADS * HEAD, D), HEAD ** -0.5, 0.5, ((0, 2),))
    global_down = centred(seeds[6], (HEADS * HEAD, RANK), HEAD ** -0.5, 0.5, ((0, 2),))
    global_up = centred(seeds[7], (RANK, D), RANK ** -0.5, 1.5, ((1, 2),))
    global_scales = jnp.clip(jnp.exp(jax.random.uniform(seeds[8], (TASKS, RANK), jnp.float32, math.log(0.25), math.log(4.0))), 0.25, 4.0)
    local_weight = centred(seeds[9], (D, L), D ** -0.5, 0.125, ((0, 2),))
    byte_ids = plant(skewed_ids(seeds[10], (BYTES,), VOCAB, 2), jax.random.fold_in(seeds[10], 3), 0, VOCAB - 1).astype(jnp.int32)
    byte_table = centred(seeds[11], (VOCAB, L), 1.0, 6.0)
    position_table = centred(seeds[12], (PATCH, L), 1.0, 6.0)
    norm_gain = jnp.clip(1.0 + 0.1 * jax.random.normal(seeds[13], (L,), jnp.float32), 0.5, 1.5)
    hidden_in = centred(seeds[14], (FF_L, L), L ** -0.5, 0.25, ((0, 2), (1, 16)))
    hidden_out = centred(seeds[15], (FF_L, L), FF_L ** -0.5, 0.125, ((0, 2), (1, 16)))
    local_down = centred(seeds[16], (L, RANK), L ** -0.5, 0.25)
    local_up = centred(seeds[17], (RANK, FF_L), RANK ** -0.5, 1.5, ((1, 2),))
    local_scales = jnp.clip(jnp.exp(jax.random.uniform(seeds[18], (TASKS, RANK), jnp.float32, math.log(0.25), math.log(4.0))), 0.25, 4.0)
    cotangent = centred(seeds[19], (BYTES, L), 1.0, 6.0, ((0, 32),))
    return {"patch_queries": patch_queries, "patch_keys": patch_keys, "patch_values": patch_values, "patch_tasks": patch_tasks, "residual": residual, "output_weight": output_weight, "global_down": global_down, "global_up": global_up, "global_scales": global_scales, "local_weight": local_weight, "byte_ids": byte_ids, "byte_table": byte_table, "position_table": position_table, "norm_gain": norm_gain, "hidden_in": hidden_in, "hidden_out": hidden_out, "local_down": local_down, "local_up": local_up, "local_scales": local_scales, "cotangent": cotangent}


def rounded(value):
    return lax.optimization_barrier(value.astype(jnp.bfloat16)).astype(jnp.float32)

def contract(left, right, left_dim, right_dim):
    return lax.dot_general(left, right, (((left_dim,), (right_dim,)), ((), ())), preferred_element_type=jnp.float32)

def select_rows(table, tasks):
    picks = (tasks[:, None] == jnp.arange(table.shape[0], dtype=jnp.int32)[None, :]).astype(jnp.float32)
    return jnp.dot(picks, table, precision=lax.Precision.HIGHEST)

def task_totals(tasks, values):
    picks = (tasks[:, None] == jnp.arange(TASKS, dtype=jnp.int32)[None, :]).astype(jnp.float32)
    return lax.dot_general(picks, values, (((0,), (0,)), ((), ())), precision=lax.Precision.HIGHEST)

def gelu_slope(upper):
    cumulative = 0.5 * (1.0 + lax.erf(upper * 0.7071067811865476))
    density = jnp.exp(-0.5 * upper * upper) * 0.3989422804014327
    return cumulative + upper * density

def local_inputs(identities, projected, tasks, byte_table, position_table, norm_gain, local_down, local_scales):
    count = identities.shape[0]
    picks = (identities[:, None] == jnp.arange(VOCAB, dtype=jnp.int32)[None, :]).astype(jnp.bfloat16)
    embedded = jnp.dot(picks, byte_table, preferred_element_type=jnp.float32)
    patches = count // PATCH
    inputs = embedded.reshape(patches, PATCH, -1) + position_table.astype(jnp.float32)[None] + projected.astype(jnp.float32)[:, None, :]
    inputs = inputs.reshape(count, -1)
    inverse = lax.rsqrt(lax.optimization_barrier(jnp.mean(inputs * inputs, axis=1, keepdims=True)) + 1e-06)
    normed = (inputs * inverse * norm_gain).astype(jnp.bfloat16)
    lowered = jnp.dot(normed, local_down, preferred_element_type=jnp.float32)
    byte_tasks = jnp.repeat(tasks, PATCH)
    scales = select_rows(local_scales, byte_tasks)
    shrunk = (lowered * scales).astype(jnp.bfloat16)
    return (inputs, inverse, normed, lowered, scales, shrunk, byte_tasks)

def backward_norm(back_total, inputs, inverse, norm_gain, cotangent):
    gained = back_total * norm_gain
    average = lax.optimization_barrier(jnp.mean(gained * inputs, axis=1, keepdims=True))
    return cotangent.astype(jnp.float32) + inverse * (gained - inputs * inverse * inverse * average)

def causal_attention(patch_queries, patch_keys, patch_values):
    total = patch_queries.shape[0]
    width = patch_queries.shape[1]
    heads = width // HEAD
    block = math.gcd(total, 512)
    key_heads = patch_keys.reshape(total, heads, HEAD).astype(jnp.float32)
    value_heads = patch_values.reshape(total, heads, HEAD).astype(jnp.float32)
    places = jnp.arange(total, dtype=jnp.int32)
    scale = 1.0 / math.sqrt(HEAD)

    def one_block(index):
        first = index * block
        query_heads = lax.dynamic_slice_in_dim(patch_queries, first, block, 0).reshape(block, heads, HEAD).astype(jnp.float32)
        scores = jnp.einsum('qhd,khd->hqk', query_heads, key_heads) * scale
        allowed = places[None, :] <= (first + jnp.arange(block, dtype=jnp.int32))[:, None]
        scores = jnp.where(allowed[None], scores, -1e+30)
        top = lax.optimization_barrier(jnp.max(scores, axis=2, keepdims=True))
        weights = jnp.where(allowed[None], jnp.exp(scores - top), 0.0)
        mass = lax.optimization_barrier(jnp.sum(weights, axis=2))
        mixed = jnp.einsum('hqk,khd->qhd', rounded(weights), value_heads)
        mixed = mixed / jnp.transpose(mass)[:, :, None]
        return mixed.reshape(block, width).astype(jnp.bfloat16)
    blocks = lax.map(one_block, jnp.arange(total // block, dtype=jnp.int32))
    return blocks.reshape(total, width)

def reference(patch_queries, patch_keys, patch_values, patch_tasks, residual, output_weight, global_down, global_up, global_scales, local_weight, byte_ids, byte_table, position_table, norm_gain, hidden_in, hidden_out, local_down, local_up, local_scales, cotangent):
    attended = causal_attention(patch_queries, patch_keys, patch_values)
    reduced = jnp.dot(attended, global_down, preferred_element_type=jnp.float32)
    task_scales = select_rows(global_scales, patch_tasks)
    scaled = (reduced * task_scales).astype(jnp.bfloat16)
    mixed = residual.astype(jnp.float32) + jnp.dot(scaled, global_up, preferred_element_type=jnp.float32)
    group = HEADS * HEAD // N_ROW
    for index in range(N_ROW):
        part = jnp.dot(attended[:, index * group:(index + 1) * group], output_weight[index * group:(index + 1) * group], preferred_element_type=jnp.float32)
        mixed = mixed + rounded(part)
    mixed_b = mixed.astype(jnp.bfloat16)
    projected = jnp.dot(mixed_b, local_weight, preferred_element_type=jnp.float32).astype(jnp.bfloat16)
    inputs, inverse, normed, lowered, scales, shrunk, byte_tasks = local_inputs(byte_ids, projected, patch_tasks, byte_table, position_table, norm_gain, local_down, local_scales)
    hidden = FF_L // N_ROW
    back_norm = jnp.zeros(inputs.shape, jnp.float32)
    back_rank = jnp.zeros(lowered.shape, jnp.float32)
    pieces_up = []
    for index in range(N_ROW):
        rows_in = hidden_in[index * hidden:(index + 1) * hidden]
        rows_out = hidden_out[index * hidden:(index + 1) * hidden]
        columns_up = local_up[:, index * hidden:(index + 1) * hidden]
        upper = contract(normed, rows_in, 1, 1) + jnp.dot(shrunk, columns_up, preferred_element_type=jnp.float32)
        through = contract(cotangent, rows_out, 1, 1)
        grown = (through * gelu_slope(upper)).astype(jnp.bfloat16)
        pieces_up.append(contract(shrunk, grown, 0, 0))
        back_norm = back_norm + rounded(jnp.dot(grown, rows_in, preferred_element_type=jnp.float32))
        back_rank = back_rank + rounded(contract(grown, columns_up, 1, 1))
    grad_local_up = jnp.concatenate(pieces_up, axis=1)
    grad_local_scales = task_totals(byte_tasks, back_rank * lowered)
    moved = (back_rank * scales).astype(jnp.bfloat16)
    grad_local_down = contract(normed, moved, 0, 0)
    back_total = back_norm + contract(moved, local_down, 1, 1)
    back_inputs = backward_norm(back_total, inputs, inverse, norm_gain, cotangent)
    patch_grad = back_inputs.reshape(-1, PATCH, back_inputs.shape[1]).sum(axis=1).astype(jnp.bfloat16)
    back_mixed = contract(patch_grad, local_weight, 1, 1).astype(jnp.bfloat16)
    grad_global_up = contract(scaled, back_mixed, 0, 0)
    back_scaled = contract(back_mixed, global_up, 1, 1)
    grad_global_scales = task_totals(patch_tasks, back_scaled * reduced)
    back_reduced = (back_scaled * task_scales).astype(jnp.bfloat16)
    grad_global_down = contract(attended, back_reduced, 0, 0)
    return (grad_global_down, grad_global_up, grad_global_scales, grad_local_down, grad_local_up, grad_local_scales)
```

```python
import functools
import math

import jax
import jax.numpy as jnp
from jax import lax
from jax.experimental import pallas as pl
from jax.experimental.pallas import tpu as pltpu
from jax.sharding import PartitionSpec as P

HEAD = 128
VOCAB = 256
PATCH = 8
TASKS = 8


def contract(left, right, left_dim, right_dim):
    return lax.dot_general(
        left, right, (((left_dim,), (right_dim,)), ((), ())), preferred_element_type=jnp.float32
    )


def select_rows(table, tasks):
    picks = (tasks[:, None] == jnp.arange(table.shape[0], dtype=jnp.int32)[None, :]).astype(
        jnp.float32
    )
    return jnp.dot(picks, table, precision=lax.Precision.HIGHEST)


def task_totals(tasks, values):
    picks = (tasks[:, None] == jnp.arange(TASKS, dtype=jnp.int32)[None, :]).astype(jnp.float32)
    return lax.dot_general(picks, values, (((0,), (0,)), ((), ())), precision=lax.Precision.HIGHEST)


def gelu_slope(upper):
    cumulative = 0.5 * (1.0 + lax.erf(upper * 0.7071067811865476))
    density = jnp.exp(-0.5 * upper * upper) * 0.3989422804014327
    return cumulative + upper * density


def local_inputs(
    identities, projected, tasks, byte_table, position_table, norm_gain, local_down, local_scales
):
    count = identities.shape[0]
    picks = (identities[:, None] == jnp.arange(VOCAB, dtype=jnp.int32)[None, :]).astype(
        jnp.bfloat16
    )
    embedded = jnp.dot(picks, byte_table, preferred_element_type=jnp.float32)
    patches = count // PATCH
    inputs = (
        embedded.reshape(patches, PATCH, -1)
        + position_table.astype(jnp.float32)[None]
        + projected.astype(jnp.float32)[:, None, :]
    )
    inputs = inputs.reshape(count, -1)
    inverse = lax.rsqrt(jnp.mean(inputs * inputs, axis=1, keepdims=True) + 1e-06)
    normed = (inputs * inverse * norm_gain).astype(jnp.bfloat16)
    lowered = jnp.dot(normed, local_down, preferred_element_type=jnp.float32)
    byte_tasks = jnp.repeat(tasks, PATCH)
    scales = select_rows(local_scales, byte_tasks)
    shrunk = (lowered * scales).astype(jnp.bfloat16)
    return (inputs, inverse, normed, lowered, scales, shrunk, byte_tasks)


def keep_state(current):
    return current


def update_state(state, query_rows, first, key_heads, value_heads, key_places, scale):
    running_max, running_sum, running_out = state
    count = query_rows.shape[0]
    heads = key_heads.shape[1]
    query_heads = query_rows.reshape(count, heads, HEAD)
    scores = (
        jnp.einsum("qhd,khd->hqk", query_heads, key_heads, preferred_element_type=jnp.float32)
        * scale
    )
    query_places = first + jnp.arange(count, dtype=jnp.int32)
    allowed = key_places[None, :] <= query_places[:, None]
    scores = jnp.where(allowed[None], scores, -1e30)
    new_max = jnp.maximum(running_max, jnp.max(scores, axis=2))
    weights = jnp.where(allowed[None], jnp.exp(scores - new_max[:, :, None]), 0.0)
    shrink = jnp.exp(running_max - new_max)
    running_sum = running_sum * shrink + jnp.sum(weights, axis=2)
    mixed = jnp.einsum(
        "hqk,khd->qhd",
        weights.astype(jnp.bfloat16),
        value_heads,
        preferred_element_type=jnp.float32,
    )
    running_out = running_out * jnp.transpose(shrink)[:, :, None] + mixed
    return (new_max, running_sum, running_out)


def finish_state(state):
    running_max, running_sum, running_out = state
    result = running_out / jnp.transpose(running_sum)[:, :, None]
    return result.reshape(result.shape[0], -1).astype(jnp.bfloat16)


def general_body(
    patch_queries,
    patch_keys,
    patch_values,
    patch_tasks,
    residual,
    output_weight,
    global_down,
    global_up,
    global_scales,
    local_weight,
    byte_ids,
    byte_table,
    position_table,
    norm_gain,
    hidden_in,
    hidden_out,
    local_down,
    local_up,
    local_scales,
    cotangent,
):
    rows = patch_queries.shape[0]
    width = patch_queries.shape[1]
    heads = width // HEAD
    row_count = lax.axis_size("row")
    seq_index = lax.axis_index("seq")
    row_index = lax.axis_index("row")
    scale = 1.0 / math.sqrt(HEAD)
    own_first = seq_index * rows
    groups = [(patch_queries, own_first)]

    def visit(state, query_rows, first, key_heads, value_heads, key_places):

        def refresh(current):
            return update_state(
                current, query_rows, first, key_heads, value_heads, key_places, scale
            )

        return lax.cond(
            key_places[0] <= first + query_rows.shape[0] - 1, refresh, keep_state, state
        )

    initial = tuple(
        (
            (
                jnp.full((heads, query_rows.shape[0]), -1e30, jnp.float32),
                jnp.zeros((heads, query_rows.shape[0]), jnp.float32),
                jnp.zeros((query_rows.shape[0], heads, HEAD), jnp.float32),
            )
            for query_rows, first in groups
        )
    )
    key_piece = lax.all_gather(patch_keys, "seq", axis=0, tiled=True)
    value_piece = lax.all_gather(patch_values, "seq", axis=0, tiled=True)
    count = key_piece.shape[0]
    span = math.gcd(count, 1024)

    def one_span(index, states):
        offset = index * span
        key_heads = lax.dynamic_slice_in_dim(key_piece, offset, span, 0).reshape(span, heads, HEAD)
        value_heads = lax.dynamic_slice_in_dim(value_piece, offset, span, 0).reshape(
            span, heads, HEAD
        )
        key_places = offset + jnp.arange(span, dtype=jnp.int32)
        updated = []
        for (query_rows, first), state in zip(groups, states):
            updated.append(visit(state, query_rows, first, key_heads, value_heads, key_places))
        return tuple(updated)

    states = lax.fori_loop(0, count // span, one_span, initial)
    outputs = [finish_state(state) for state in states]
    attended = outputs[0]
    reduced = lax.psum(jnp.dot(attended, global_down, preferred_element_type=jnp.float32), "row")
    task_scales = select_rows(global_scales, patch_tasks)
    scaled = (reduced * task_scales).astype(jnp.bfloat16)
    mixed = lax.psum_scatter(
        contract(output_weight, attended, 0, 1).astype(jnp.bfloat16),
        "row",
        scatter_dimension=0,
        tiled=True,
    ).astype(jnp.float32)
    mixed = mixed + jnp.transpose(residual.astype(jnp.float32)) + contract(global_up, scaled, 0, 1)
    mixed_b = mixed.astype(jnp.bfloat16)
    own_patches = rows // row_count
    own_bytes = own_patches * PATCH
    rows_in, rows_out = (
        lax.all_gather(hidden_in, "seq", axis=1, tiled=True),
        lax.all_gather(hidden_out, "seq", axis=1, tiled=True),
    )
    partial_value = contract(mixed_b, local_weight, 0, 0)
    projected = lax.psum(partial_value.astype(jnp.bfloat16), "row")
    every = local_inputs(
        byte_ids,
        projected,
        patch_tasks,
        byte_table,
        position_table,
        norm_gain,
        local_down,
        local_scales,
    )
    normed_all = every[2]
    shrunk_all = every[5]
    cotangent_all = lax.all_gather(cotangent, "row", axis=0, tiled=True)
    inputs, inverse, normed, lowered, scales, shrunk, byte_tasks = [
        lax.dynamic_slice_in_dim(value, row_index * own_bytes, own_bytes, 0) for value in every
    ]
    upper = contract(normed_all, rows_in, 1, 1) + jnp.dot(
        shrunk_all, local_up, preferred_element_type=jnp.float32
    )
    through = contract(cotangent_all, rows_out, 1, 1)
    grown = (through * gelu_slope(upper)).astype(jnp.bfloat16)
    grad_local_up = contract(shrunk_all, grown, 0, 0)
    back_norm, back_rank = (
        lax.psum_scatter(
            jnp.dot(grown, rows_in, preferred_element_type=jnp.float32).astype(jnp.bfloat16),
            "row",
            scatter_dimension=0,
            tiled=True,
        ).astype(jnp.float32),
        lax.psum_scatter(
            contract(grown, local_up, 1, 1).astype(jnp.bfloat16),
            "row",
            scatter_dimension=0,
            tiled=True,
        ).astype(jnp.float32),
    )
    grad_local_scales = task_totals(byte_tasks, back_rank * lowered)
    moved = (back_rank * scales).astype(jnp.bfloat16)
    grad_local_down = contract(normed, moved, 0, 0)
    back_total = back_norm + contract(moved, local_down, 1, 1)
    gained = back_total * norm_gain
    average = jnp.mean(gained * inputs, axis=1, keepdims=True)
    back_inputs = cotangent.astype(jnp.float32) + inverse * (
        gained - inputs * inverse * inverse * average
    )
    patch_grad = back_inputs.reshape(own_patches, PATCH, -1).sum(axis=1).astype(jnp.bfloat16)
    back_mixed = contract(
        lax.all_gather(patch_grad, "row", axis=0, tiled=True), local_weight, 1, 1
    ).astype(jnp.bfloat16)
    grad_global_up = contract(scaled, back_mixed, 0, 0)
    back_scaled = lax.psum(contract(back_mixed, global_up, 1, 1), "row")
    grad_global_scales = task_totals(patch_tasks, back_scaled * reduced)
    back_reduced = (back_scaled * task_scales).astype(jnp.bfloat16)
    grad_global_down = contract(attended, back_reduced, 0, 0)
    grad_global_down, grad_global_up, grad_global_scales, grad_local_up = lax.psum(
        (grad_global_down, grad_global_up, grad_global_scales, grad_local_up), "seq"
    )
    grad_local_down, grad_local_scales = lax.psum(
        (grad_local_down, grad_local_scales), ("seq", "row")
    )
    return (
        grad_global_down,
        grad_global_up,
        grad_global_scales,
        grad_local_down,
        grad_local_up,
        grad_local_scales,
    )


MESH = pl.DeviceIdType.MESH
SPAN = 256


def remote(src, dst, send, recv, seq, row):
    return pltpu.make_async_remote_copy(
        src_ref=src,
        dst_ref=dst,
        send_sem=send,
        recv_sem=recv,
        device_id=(seq, row),
        device_id_type=MESH,
    )


def exact(left, right, left_dim, right_dim):
    return lax.dot_general(
        left, right, (((left_dim,), (right_dim,)), ((), ())), precision=lax.Precision.HIGHEST,
        preferred_element_type=jnp.float32,
    )


def split_pair(value):
    high = value.astype(jnp.bfloat16)
    low = (value - high.astype(jnp.float32)).astype(jnp.bfloat16)
    return high, low


def step_kernel(
    chips, depth,
    q_hbm, k_hbm, v_hbm, tasks_hbm, res_hbm, ow_hbm, gd_hbm, gu_hbm, gs_hbm, lw_hbm, ids_hbm,
    table_hbm, pos_hbm, gain_hbm, hi_hbm, ho_hbm, ld_hbm, lu_hbm, ls_hbm, cot_hbm,
    ggd_out, ggu_out, gsc_out, gld_out, glu_out, lsc_out,
    q_ref, k_ref, v_ref, tasks_ref, res_ref, ow_ref, gd_ref, gu_ref, gs_ref, lw_ref, ids_ref,
    pos_ref, gain_ref, ld_ref, ls_ref, cot_ref, wi, wo,
    qb, kb, vb, ob, att, lwb, w2, acc, e1, e1r, mb, mr, bridge,
    emb, inp, nrm, inv, low, sca, bl, gr, mv, bp, bpr, cross, crossr, grads, part, result, full,
    in_sem, a_send, a_recv, f_send, f_recv, o_send, o_recv, z_send, z_recv, x_send, x_recv,
    p_send, p_recv, c_send, c_recv, y_send, y_recv, b_send, b_recv, r_send, r_recv, g_send, g_recv,
):
    bf, f32 = jnp.bfloat16, jnp.float32
    count = 2 * chips
    me = lax.axis_index("seq")
    row = lax.axis_index("row")
    other = 1 - row
    chip, core = me // 2, lax.rem(me, 2)
    mate = 2 * chip + (1 - core)
    rows, width = q_hbm.shape
    half = width // 2
    columns = lw_hbm.shape[1]
    rank = gu_hbm.shape[0]
    wide = columns + HEAD
    shard = hi_hbm.shape[0]
    vocab = table_hbm.shape[0]
    total = rows * PATCH

    def at(number):
        return lax.rem(number + 2 * chips, chips)

    def heads_of(number):
        return pl.ds(pl.multiple_of(number * HEAD, HEAD), HEAD)

    def shard_of(slot):
        return pl.ds(pl.multiple_of(slot * shard, shard), shard)

    barrier = pltpu.get_barrier_semaphore()
    peers = [(lax.rem(me + d, count), row) for d in range(1, count)] + [(me, other)]
    for seq, line in peers:
        pl.semaphore_signal(barrier, inc=1, device_id=(seq, line), device_id_type=MESH)

    loads = {}

    def load(name, src, dst):
        copy = pltpu.make_async_copy(src, dst, in_sem.at[len(loads)])
        copy.start()
        loads[name] = copy

    load("k", k_hbm, k_ref)
    load("v", v_hbm, v_ref)
    load("q", q_hbm, q_ref)
    load("lw", lw_hbm, lw_ref)
    load("hi", hi_hbm, wi.at[shard_of(me)])
    load("ho", ho_hbm, wo.at[shard_of(me)])
    load("cot", cot_hbm, cot_ref.at[row])
    load("gu", gu_hbm, gu_ref)
    load("ow", ow_hbm, ow_ref)
    load("res", res_hbm, res_ref)
    load("gd", gd_hbm, gd_ref.at[pl.ds(0, rank)])
    load("lu", lu_hbm, wi.at[pl.ds(columns, rank)])
    load("ld", ld_hbm, ld_ref.at[pl.ds(0, rank)])
    load("table", table_hbm, emb.at[pl.ds(0, vocab), pl.ds(0, columns)])
    load("tasks", tasks_hbm, tasks_ref)
    load("ids", ids_hbm, ids_ref)
    load("pos", pos_hbm, pos_ref)
    load("gain", gain_hbm, gain_ref)
    load("gs", gs_hbm, gs_ref)
    load("ls", ls_hbm, ls_ref)

    gd_ref[rank:] = jnp.zeros((HEAD - rank, width), bf)
    ld_ref[rank:] = jnp.zeros((HEAD - rank, columns), bf)
    wi[columns + rank :] = jnp.zeros((HEAD - rank, width), bf)
    bridge[...] = jnp.zeros((HEAD, columns), bf)
    emb[:vocab, columns:] = jnp.zeros((vocab, 2 * HEAD), bf)
    emb[vocab + HEAD :] = jnp.zeros((HEAD, wide + HEAD), bf)
    grads[13:] = jnp.zeros((count - 13, 2 * rank, HEAD), bf)

    pl.semaphore_wait(barrier, len(peers))

    own = heads_of(chip)
    arrivals = {}
    forwards = {}
    own_half = pl.ds(pl.multiple_of(core * half, half), half)
    loads["k"].wait()
    loads["v"].wait()
    loads["q"].wait()
    order = sorted(range(1, chips), key=lambda d: -min(d, chips - d))
    for which, (src, dst) in enumerate(
        ((k_ref, kb.at[me]), (v_ref, vb.at[me]), (q_ref, qb.at[chip]))
    ):
        for d in order:
            to = at(chip + d)
            copy = remote(
                src.at[:, heads_of(to)], dst, a_send.at[which, d], a_recv.at[which, d],
                2 * to + core, row,
            )
            copy.start()
            arrivals[which, d] = copy
    for which, (src, dst) in enumerate(((k_ref, kb), (v_ref, vb))):
        copy = remote(
            src.at[:, own], dst.at[me], f_send.at[which, 0], f_recv.at[which, 0], mate, row
        )
        copy.start()
        forwards[which, 0] = copy
    loads["lw"].wait()
    lw_copy = remote(lw_ref.at[own_half], lwb.at[own_half], y_send.at[0], y_recv.at[0], me, other)
    lw_copy.start()
    loads["cot"].wait()
    cot_copy = remote(
        cot_ref.at[row], cot_ref.at[row], c_send.at[0], c_recv.at[0], me, other
    )
    cot_copy.start()

    levels = chips // depth
    level, side = chip // depth, lax.rem(chip, depth)
    loads["hi"].wait()
    loads["ho"].wait()
    weights_in = ((0, wi), (1, wo))
    z_copies = []
    x_copies = []
    p_copies = []
    neighbour = 2 * (level * depth + (1 - side)) + core

    def slot_of(number, line):
        return 2 * (lax.rem(number + levels, levels) * depth + line) + core

    def pass_side(d, slot):
        for which, buffer in weights_in:
            part_of = buffer.at[shard_of(slot)]
            copy = remote(
                part_of, part_of, x_send.at[which, d], x_recv.at[which, d], neighbour, row
            )
            copy.start()
            x_copies.append((d, copy))

    def pass_mate(number, slot):
        for which, buffer in weights_in:
            part_of = buffer.at[shard_of(slot)]
            copy = remote(
                part_of, part_of, p_send.at[which, number], p_recv.at[which, number], mate, row
            )
            copy.start()
            p_copies.append(copy)

    for d in range(1, levels):
        to = lax.rem(level + d, levels) * depth + side
        for which, buffer in weights_in:
            part_of = buffer.at[shard_of(me)]
            copy = remote(
                part_of, part_of, z_send.at[which, d], z_recv.at[which, d], 2 * to + core, row
            )
            copy.start()
            z_copies.append((d, copy))
    pass_side(0, me)
    pass_mate(0, me)

    qb[chip] = q_ref[:, own]
    kb[me] = k_ref[:, own]
    vb[me] = v_ref[:, own]

    loads["gu"].wait()
    mb[...] = jnp.dot(gu_ref[...], lw_ref[...], preferred_element_type=f32).astype(bf)
    m_copy = remote(mb, mr, y_send.at[2], y_recv.at[2], me, other)
    m_copy.start()

    tile = math.gcd(width, SPAN)
    loads["ow"].wait()

    @pl.loop(0, width // tile)
    def _(index):
        block = pl.ds(pl.multiple_of(index * tile, tile), tile)
        acc[block] = jnp.dot(
            ow_ref[block, pl.ds(pl.multiple_of(row * width, width), width)],
            lw_ref[...],
            preferred_element_type=f32,
        )

    lw_copy.wait_recv()
    lw_mate = remote(lwb.at[own_half], lwb.at[own_half], y_send.at[1], y_recv.at[1], mate, row)
    lw_mate.start()
    lw_mate.wait_recv()

    @pl.loop(0, width // tile)
    def _(index):
        block = pl.ds(pl.multiple_of(index * tile, tile), tile)
        summed = acc[block] + jnp.dot(
            ow_ref[block, pl.ds(pl.multiple_of(other * width, width), width)],
            lwb[...],
            preferred_element_type=f32,
        )
        w2[block] = summed.astype(bf)

    for name in ("res", "gd", "lu", "ld", "table", "tasks", "ids", "pos", "gain", "gs", "ls"):
        loads[name].wait()
    picks = (
        lax.broadcasted_iota(jnp.int32, (TASKS, rows), 0) == tasks_ref[...]
    ).astype(f32)

    def widen(table):
        return jnp.concatenate([table, jnp.zeros((TASKS, HEAD - rank), f32)], axis=1)

    task_scales = exact(picks, widen(gs_ref[...]), 0, 0)
    high, low_part = split_pair(exact(picks, widen(ls_ref[...]), 0, 0))
    emb[vocab : vocab + rows, columns:wide] = high
    emb[vocab : vocab + rows, wide:] = low_part
    emb[vocab + rows : vocab + rows + 2 * PATCH, :columns] = jnp.concatenate(
        [pos_ref[...].astype(f32), jnp.zeros((PATCH, columns), f32)], axis=0
    ).astype(bf)
    direct = jnp.dot(res_ref[...], lw_ref[...], preferred_element_type=f32)
    inp[:rows] = direct

    for d in reversed(range(1, chips)):
        for which, buffer in ((0, kb), (1, vb)):
            arrivals[which, d].wait_recv()
            slot = 2 * at(chip - d) + core
            copy = remote(
                buffer.at[slot], buffer.at[slot], f_send.at[which, d], f_recv.at[which, d],
                mate, row,
            )
            copy.start()
            forwards[which, d] = copy
    for d in range(1, chips):
        arrivals[2, d].wait_recv()
    for copy in forwards.values():
        copy.wait_recv()

    factor = 1.0 / math.sqrt(HEAD) / math.log(2.0)
    for i in reversed(range(chips)):
        before = 2 * i * rows
        query = qb[i]
        new_keys = kb[2 * i : 2 * i + 2].reshape(2 * rows, HEAD)
        new_values = vb[2 * i : 2 * i + 2].reshape(2 * rows, HEAD)
        fresh = contract(query, new_keys, 1, 1)
        places = lax.broadcasted_iota(jnp.int32, (rows, 2 * rows), 1)
        queries = lax.broadcasted_iota(jnp.int32, (rows, 2 * rows), 0) + core * rows
        fresh = jnp.where(places <= queries, fresh, -1e30)
        top = jnp.max(fresh, axis=1, keepdims=True)
        if i:
            old_keys = kb[: 2 * i].reshape(before, HEAD)
            old_values = vb[: 2 * i].reshape(before, HEAD)
            scores = contract(query, old_keys, 1, 1)
            top = jnp.maximum(top, jnp.max(scores, axis=1, keepdims=True))
        weights = jnp.exp2((fresh - top) * factor)
        mass = jnp.sum(weights, axis=1, keepdims=True)
        mixed = jnp.dot(weights.astype(bf), new_values, preferred_element_type=f32)
        if i:
            weights = jnp.exp2((scores - top) * factor)
            mass = mass + jnp.sum(weights, axis=1, keepdims=True)
            mixed = mixed + jnp.dot(weights.astype(bf), old_values, preferred_element_type=f32)
        ob[i] = (mixed / mass).astype(bf)

        @pl.when(i != chip)
        def _():
            remote(
                ob.at[i], att.at[:, own], o_send.at[i], o_recv.at[chip], 2 * i + core, row
            ).start()

        @pl.when(i == chip)
        def _():
            att[:, own] = ob[i]

    for d in range(1, levels):
        for number, copy in z_copies:
            if number == d:
                copy.wait_recv()
        slot = slot_of(level - d, side)
        pass_side(d, slot)
        pass_mate(d, slot)
    for d in range(levels):
        for number, copy in x_copies:
            if number == d:
                copy.wait_recv()
        pass_mate(levels + d, slot_of(level - d, 1 - side))

    for i in range(chips):

        @pl.when(i != chip)
        def _():
            back = remote(
                ob.at[i], att.at[:, heads_of(i)], o_send.at[i], o_recv.at[i], 2 * i + core, row
            )
            back.wait_recv()
            back.wait_send()

    attended = att[...]
    e1[:, :columns] = (
        jnp.dot(attended, w2[...], preferred_element_type=f32) + inp[:rows]
    ).astype(bf)
    e1[:, columns:] = contract(attended, gd_ref[...], 1, 1).astype(bf)
    e_copy = remote(e1, e1r, y_send.at[3], y_recv.at[3], me, other)
    e_copy.start()
    cot_copy.wait_recv()
    m_copy.wait_recv()
    bridge[:rank] = (mb[...].astype(f32) + mr[...].astype(f32)).astype(bf)
    belongs = (
        lax.broadcasted_iota(jnp.int32, (rows, total), 1) // PATCH
        == lax.broadcasted_iota(jnp.int32, (rows, total), 0)
    ).astype(f32).astype(bf)
    own_bytes = total // 2
    cot_sum = sum(
        jnp.dot(
            belongs[:, index * own_bytes : (index + 1) * own_bytes], cot_ref[index],
            preferred_element_type=f32,
        )
        for index in range(2)
    )
    e_copy.wait_recv()
    reduced = e1[:, columns:].astype(f32) + e1r[:, columns:].astype(f32)
    scaled = (reduced * task_scales).astype(bf)
    emb[vocab : vocab + rows, :columns] = (
        e1[:, :columns].astype(f32)
        + e1r[:, :columns].astype(f32)
        + jnp.dot(scaled, bridge[...], preferred_element_type=f32)
    ).astype(bf)

    depth_all = emb.shape[0]
    pieces = total // SPAN
    per_piece = SPAN // PATCH

    @pl.loop(0, pieces)
    def _(index):
        block = pl.ds(pl.multiple_of(index * SPAN, SPAN), SPAN)
        line = lax.broadcasted_iota(jnp.int32, (depth_all, SPAN), 0)
        byte = lax.broadcasted_iota(jnp.int32, (depth_all, SPAN), 1) + index * SPAN
        chosen = (
            (line == ids_ref[:, block])
            | (line == vocab + byte // PATCH)
            | (line == vocab + rows + lax.rem(byte, PATCH))
        )
        found = contract(jnp.where(chosen, 1.0, 0.0).astype(bf), emb[...], 0, 0)
        inputs = found[:, :columns]
        scales = found[:, columns:wide] + found[:, wide:]
        inverse = lax.rsqrt(jnp.mean(inputs * inputs, axis=1, keepdims=True) + 1e-06)
        normed = (inputs * inverse * gain_ref[...]).astype(bf)
        lowered = contract(normed, ld_ref[...], 1, 1)
        inp[block] = inputs
        inv[block] = jnp.broadcast_to(inverse, (SPAN, HEAD))
        sca[block] = scales
        low[block] = lowered
        nrm[block, :columns] = normed
        nrm[block, columns:] = (lowered * scales).astype(bf)

    for copy in p_copies:
        copy.wait_recv()

    @pl.loop(0, pieces)
    def _(index):
        block = pl.ds(pl.multiple_of(index * SPAN, SPAN), SPAN)
        upper = jnp.dot(nrm[block], wi[...], preferred_element_type=f32)
        inner = pl.ds(pl.multiple_of(lax.rem(index * SPAN, own_bytes), SPAN), SPAN)
        through = jnp.dot(
            cot_ref[index * SPAN // own_bytes, inner], wo[...], preferred_element_type=f32
        )
        grown = (through * gelu_slope(upper)).astype(bf)
        gr[block] = grown
        both = contract(grown, wi[...], 1, 1)
        back_rank = both[:, columns:]
        moved = (back_rank * sca[block]).astype(bf)
        mv[block] = moved
        bl[block] = back_rank * low[block]
        back_total = both[:, :columns] + jnp.dot(
            moved, ld_ref[...], preferred_element_type=f32
        )
        inputs = inp[block]
        inverse = inv[block][:, :1]
        gained = back_total * gain_ref[...]
        average = jnp.mean(gained * inputs, axis=1, keepdims=True)
        back_inputs = inverse * (gained - inputs * (inverse * inverse * average))
        near = (
            lax.broadcasted_iota(jnp.int32, (per_piece, SPAN), 1) // PATCH
            == lax.broadcasted_iota(jnp.int32, (per_piece, SPAN), 0)
        ).astype(f32).astype(bf)
        patches = pl.ds(pl.multiple_of(index * per_piece, per_piece), per_piece)
        bp[patches] = jnp.dot(
            near, back_inputs.astype(bf), preferred_element_type=f32
        ).astype(bf)
        remote(
            bp.at[patches], bpr.at[patches], b_send.at[index], b_recv.at[index], me, other
        ).start()

    down = contract(mv[...], nrm[:, :columns], 0, 0)[:rank]
    high, low_part = split_pair(bl[...])
    by_patch = jnp.dot(belongs, high, preferred_element_type=f32) + jnp.dot(
        belongs, low_part, preferred_element_type=f32
    )
    small = exact(picks, by_patch, 1, 0)
    small = jnp.concatenate([small, jnp.zeros_like(small)], axis=0)
    cross[:, :columns] = down.astype(bf)
    cross[:, columns:] = small.astype(bf)
    cross_copy = remote(cross, crossr, y_send.at[4], y_recv.at[4], me, other)
    cross_copy.start()
    lift = contract(nrm[:, columns:], gr[...], 0, 0)[:rank].astype(bf)
    spread = width // HEAD
    for t in range(spread):
        grads[t, :rank] = lift[:, t * HEAD : (t + 1) * HEAD]

    for index in range(pieces):
        patches = pl.ds(index * per_piece, per_piece)
        remote(
            bp.at[patches], bpr.at[patches], b_send.at[index], b_recv.at[index], me, other
        ).wait()
    patch_grad = (bp[...].astype(f32) + bpr[...].astype(f32) + cot_sum).astype(bf)
    pulled = contract(scaled, patch_grad, 0, 0)[:rank].astype(bf)
    back_scaled = contract(patch_grad, bridge[...], 1, 1)
    back_reduced = (back_scaled * task_scales).astype(bf)
    outward = contract(back_reduced, att[...], 0, 0)[:rank].astype(bf)
    tops = exact(picks, back_scaled * reduced, 1, 0)
    tops = jnp.concatenate([tops, jnp.zeros_like(tops)], axis=0)
    for t in range(spread):
        grads[t, rank:] = outward[:, t * HEAD : (t + 1) * HEAD]
    cross_copy.wait_recv()
    joint = (cross[...].astype(f32) + crossr[...].astype(f32)).astype(bf)
    thin = columns // HEAD
    for t in range(thin):
        grads[spread + t, :rank] = joint[:, t * HEAD : (t + 1) * HEAD]
        grads[spread + t, rank:] = pulled[:, t * HEAD : (t + 1) * HEAD]
    grads[spread + thin, :rank] = joint[:, columns:]
    grads[spread + thin, rank:] = tops.astype(bf)

    first = []
    for d in range(1, count):
        to = lax.rem(me + d, count)
        copy = remote(grads.at[to], part.at[me], r_send.at[d], r_recv.at[d], to, row)
        copy.start()
        first.append(copy)
    part[me] = grads[me]
    for copy in first:
        copy.wait_recv()
    result[...] = jnp.sum(part[...].astype(f32), axis=0).astype(bf)
    second = []
    for d in range(1, count):
        to = lax.rem(me + d, count)
        copy = remote(result, full.at[me], g_send.at[d], g_recv.at[d], to, row)
        copy.start()
        second.append(copy)
    full[me] = result[...]
    for copy in second:
        copy.wait_recv()
    for t in range(spread):
        glu_out[:, t * HEAD : (t + 1) * HEAD] = full[t, :rank].astype(f32)
        ggd_out[:, t * HEAD : (t + 1) * HEAD] = full[t, rank:].astype(f32)
    for t in range(thin):
        gld_out[:, t * HEAD : (t + 1) * HEAD] = full[spread + t, :rank].astype(f32)
        bridge[:rank, t * HEAD : (t + 1) * HEAD] = full[spread + t, rank:]
    ggu_out[...] = contract(bridge[:rank], lw_ref[...], 1, 1)
    lsc_out[...] = full[spread + thin, :TASKS, :rank].astype(f32)
    gsc_out[...] = full[spread + thin, rank : rank + TASKS, :rank].astype(f32)
    for copy in (
        [lw_copy, lw_mate, cot_copy, m_copy, e_copy, cross_copy]
        + list(arrivals.values())
        + list(forwards.values())
        + [copy for d, copy in z_copies + x_copies]
        + p_copies
        + first
        + second
    ):
        copy.wait_send()


def paired_body(
    patch_queries, patch_keys, patch_values, patch_tasks, residual, output_weight, global_down,
    global_up, global_scales, local_weight, byte_ids, byte_table, position_table, norm_gain,
    hidden_in, hidden_out, local_down, local_up, local_scales, cotangent,
):
    count = lax.axis_size("seq")
    rows, width = patch_queries.shape
    chips = count // 2
    depth = 2
    levels = chips // depth
    columns = local_weight.shape[1]
    rank = global_up.shape[0]
    vocab = byte_table.shape[0]
    total = byte_ids.shape[0]
    wide = columns + HEAD
    pieces = total // SPAN
    bf, f32 = jnp.bfloat16, jnp.float32
    vm = pltpu.VMEM
    dma = pltpu.SemaphoreType.DMA
    args = (
        patch_queries, patch_keys, patch_values, patch_tasks.reshape(1, rows), residual,
        output_weight, jnp.transpose(global_down), global_up, global_scales, local_weight,
        byte_ids.reshape(1, total), byte_table, position_table, norm_gain.reshape(1, columns),
        jnp.transpose(hidden_in), jnp.transpose(hidden_out), jnp.transpose(local_down), local_up,
        local_scales, cotangent,
    )
    outs = pl.pallas_call(
        functools.partial(step_kernel, chips, depth),
        out_shape=(
            jax.ShapeDtypeStruct((rank, width), f32),
            jax.ShapeDtypeStruct((rank, width), f32),
            jax.ShapeDtypeStruct((TASKS, rank), f32),
            jax.ShapeDtypeStruct((rank, columns), f32),
            jax.ShapeDtypeStruct((rank, width), f32),
            jax.ShapeDtypeStruct((TASKS, rank), f32),
        ),
        in_specs=[pl.BlockSpec(memory_space=pl.ANY)] * len(args),
        out_specs=(pl.BlockSpec(memory_space=vm),) * 6,
        scratch_shapes=[
            vm((rows, width), bf), vm((rows, width), bf), vm((rows, width), bf),
            vm((1, rows), jnp.int32), vm((rows, width), bf), vm(output_weight.shape, bf),
            vm((HEAD, width), bf), vm((rank, width), bf), vm((TASKS, rank), f32),
            vm((width, columns), bf), vm((1, total), jnp.int32), vm((PATCH, columns), bf),
            vm((1, columns), f32), vm((HEAD, columns), bf), vm((TASKS, rank), f32),
            vm((2, total // 2, columns), bf), vm((wide, width), bf), vm((columns, width), bf),
            vm((chips, rows, HEAD), bf), vm((count, rows, HEAD), bf), vm((count, rows, HEAD), bf),
            vm((chips, rows, HEAD), bf), vm((rows, width), bf), vm((width, columns), bf),
            vm((width, columns), bf), vm((width, columns), f32), vm((rows, wide), bf),
            vm((rows, wide), bf), vm((rank, columns), bf), vm((rank, columns), bf),
            vm((HEAD, columns), bf),
            vm((vocab + 2 * HEAD, wide + HEAD), bf), vm((total, columns), f32),
            vm((total, wide), bf), vm((total, HEAD), f32), vm((total, HEAD), f32),
            vm((total, HEAD), f32), vm((total, HEAD), f32), vm((total, width), bf),
            vm((total, HEAD), bf), vm((rows, columns), bf), vm((rows, columns), bf),
            vm((rank, wide), bf), vm((rank, wide), bf), vm((count, 2 * rank, HEAD), bf),
            vm((count, 2 * rank, HEAD), bf), vm((2 * rank, HEAD), bf),
            vm((count, 2 * rank, HEAD), bf),
            dma((len(args),)), dma((3, chips)), dma((3, chips)), dma((2, chips)), dma((2, chips)),
            dma((chips,)), dma((chips,)), dma((2, levels)), dma((2, levels)), dma((2, levels)),
            dma((2, levels)), dma((2, chips)), dma((2, chips)), dma((1,)), dma((1,)), dma((5,)),
            dma((5,)), dma((pieces,)), dma((pieces,)), dma((count,)), dma((count,)),
            dma((count,)), dma((count,)),
        ],
        compiler_params=pltpu.CompilerParams(
            collective_id=0, has_side_effects=True, vmem_limit_bytes=60 * 1024 * 1024
        ),
        name="step",
    )(*args)
    ggd, ggu, gsc, gld, glu, lsc = outs
    return (jnp.transpose(ggd), ggu, gsc, jnp.transpose(gld), glu, lsc)


def pick_body(seq_count, row_count, *args):
    heads = args[0].shape[1] // HEAD
    rank = args[7].shape[0]
    hidden = args[14].shape[0]
    fits = (
        row_count == 2
        and seq_count == 2 * heads
        and heads % 4 == 0
        and rank == 2 * TASKS
        and args[0].shape[1] == hidden
        and (4 * rank * hidden) % (seq_count * 16 * HEAD) == 0
        and hidden >= args[9].shape[1] + rank
    )
    return paired_body(*args) if fits else general_body(*args)


def solution(mesh):
    placed = (
        P("seq", "row"),
        P("seq", "row"),
        P("seq", "row"),
        P("seq"),
        P("seq", "row"),
        P("row", None),
        P("row", None),
        P(None, "row"),
        P(),
        P("row", None),
        P("seq"),
        P(),
        P(),
        P(),
        P("row", "seq"),
        P("row", "seq"),
        P(),
        P(None, "row"),
        P(),
        P(("seq", "row"), None),
    )
    chosen = functools.partial(pick_body, mesh.shape["seq"], mesh.shape["row"])
    return jax.shard_map(
        chosen,
        mesh=mesh,
        in_specs=placed,
        out_specs=(P("row", None), P(None, "row"), P(), P(), P(None, "row"), P()),
        check_vma=False,
    )
```

```python
import functools
import math

import jax
import jax.numpy as jnp
from jax import lax
from jax.experimental import pallas as pl
from jax.experimental.pallas import tpu as pltpu
from jax.sharding import PartitionSpec as P

HEAD = 128
VOCAB = 256
PATCH = 8
TASKS = 8


def contract(left, right, left_dim, right_dim):
    return lax.dot_general(
        left, right, (((left_dim,), (right_dim,)), ((), ())), preferred_element_type=jnp.float32
    )


def select_rows(table, tasks):
    picks = (tasks[:, None] == jnp.arange(table.shape[0], dtype=jnp.int32)[None, :]).astype(
        jnp.float32
    )
    return jnp.dot(picks, table, precision=lax.Precision.HIGHEST)


def task_totals(tasks, values):
    picks = (tasks[:, None] == jnp.arange(TASKS, dtype=jnp.int32)[None, :]).astype(jnp.float32)
    return lax.dot_general(picks, values, (((0,), (0,)), ((), ())), precision=lax.Precision.HIGHEST)


def gelu_slope(upper):
    cumulative = 0.5 * (1.0 + lax.erf(upper * 0.7071067811865476))
    density = jnp.exp(-0.5 * upper * upper) * 0.3989422804014327
    return cumulative + upper * density


def local_inputs(
    identities, projected, tasks, byte_table, position_table, norm_gain, local_down, local_scales
):
    count = identities.shape[0]
    picks = (identities[:, None] == jnp.arange(VOCAB, dtype=jnp.int32)[None, :]).astype(
        jnp.bfloat16
    )
    embedded = jnp.dot(picks, byte_table, preferred_element_type=jnp.float32)
    patches = count // PATCH
    inputs = (
        embedded.reshape(patches, PATCH, -1)
        + position_table.astype(jnp.float32)[None]
        + projected.astype(jnp.float32)[:, None, :]
    )
    inputs = inputs.reshape(count, -1)
    inverse = lax.rsqrt(jnp.mean(inputs * inputs, axis=1, keepdims=True) + 1e-06)
    normed = (inputs * inverse * norm_gain).astype(jnp.bfloat16)
    lowered = jnp.dot(normed, local_down, preferred_element_type=jnp.float32)
    byte_tasks = jnp.repeat(tasks, PATCH)
    scales = select_rows(local_scales, byte_tasks)
    shrunk = (lowered * scales).astype(jnp.bfloat16)
    return (inputs, inverse, normed, lowered, scales, shrunk, byte_tasks)


def keep_state(current):
    return current


def update_state(state, query_rows, first, key_heads, value_heads, key_places, scale):
    running_max, running_sum, running_out = state
    count = query_rows.shape[0]
    heads = key_heads.shape[1]
    query_heads = query_rows.reshape(count, heads, HEAD)
    scores = (
        jnp.einsum("qhd,khd->hqk", query_heads, key_heads, preferred_element_type=jnp.float32)
        * scale
    )
    query_places = first + jnp.arange(count, dtype=jnp.int32)
    allowed = key_places[None, :] <= query_places[:, None]
    scores = jnp.where(allowed[None], scores, -1e30)
    new_max = jnp.maximum(running_max, jnp.max(scores, axis=2))
    weights = jnp.where(allowed[None], jnp.exp(scores - new_max[:, :, None]), 0.0)
    shrink = jnp.exp(running_max - new_max)
    running_sum = running_sum * shrink + jnp.sum(weights, axis=2)
    mixed = jnp.einsum(
        "hqk,khd->qhd",
        weights.astype(jnp.bfloat16),
        value_heads,
        preferred_element_type=jnp.float32,
    )
    running_out = running_out * jnp.transpose(shrink)[:, :, None] + mixed
    return (new_max, running_sum, running_out)


def finish_state(state):
    running_max, running_sum, running_out = state
    result = running_out / jnp.transpose(running_sum)[:, :, None]
    return result.reshape(result.shape[0], -1).astype(jnp.bfloat16)


def general_body(
    patch_queries,
    patch_keys,
    patch_values,
    patch_tasks,
    residual,
    output_weight,
    global_down,
    global_up,
    global_scales,
    local_weight,
    byte_ids,
    byte_table,
    position_table,
    norm_gain,
    hidden_in,
    hidden_out,
    local_down,
    local_up,
    local_scales,
    cotangent,
):
    rows = patch_queries.shape[0]
    width = patch_queries.shape[1]
    heads = width // HEAD
    row_count = lax.axis_size("row")
    seq_index = lax.axis_index("seq")
    row_index = lax.axis_index("row")
    scale = 1.0 / math.sqrt(HEAD)
    own_first = seq_index * rows
    groups = [(patch_queries, own_first)]

    def visit(state, query_rows, first, key_heads, value_heads, key_places):

        def refresh(current):
            return update_state(
                current, query_rows, first, key_heads, value_heads, key_places, scale
            )

        return lax.cond(
            key_places[0] <= first + query_rows.shape[0] - 1, refresh, keep_state, state
        )

    initial = tuple(
        (
            (
                jnp.full((heads, query_rows.shape[0]), -1e30, jnp.float32),
                jnp.zeros((heads, query_rows.shape[0]), jnp.float32),
                jnp.zeros((query_rows.shape[0], heads, HEAD), jnp.float32),
            )
            for query_rows, first in groups
        )
    )
    key_piece = lax.all_gather(patch_keys, "seq", axis=0, tiled=True)
    value_piece = lax.all_gather(patch_values, "seq", axis=0, tiled=True)
    count = key_piece.shape[0]
    span = math.gcd(count, 1024)

    def one_span(index, states):
        offset = index * span
        key_heads = lax.dynamic_slice_in_dim(key_piece, offset, span, 0).reshape(span, heads, HEAD)
        value_heads = lax.dynamic_slice_in_dim(value_piece, offset, span, 0).reshape(
            span, heads, HEAD
        )
        key_places = offset + jnp.arange(span, dtype=jnp.int32)
        updated = []
        for (query_rows, first), state in zip(groups, states):
            updated.append(visit(state, query_rows, first, key_heads, value_heads, key_places))
        return tuple(updated)

    states = lax.fori_loop(0, count // span, one_span, initial)
    outputs = [finish_state(state) for state in states]
    attended = outputs[0]
    reduced = lax.psum(jnp.dot(attended, global_down, preferred_element_type=jnp.float32), "row")
    task_scales = select_rows(global_scales, patch_tasks)
    scaled = (reduced * task_scales).astype(jnp.bfloat16)
    mixed = lax.psum_scatter(
        contract(output_weight, attended, 0, 1).astype(jnp.bfloat16),
        "row",
        scatter_dimension=0,
        tiled=True,
    ).astype(jnp.float32)
    mixed = mixed + jnp.transpose(residual.astype(jnp.float32)) + contract(global_up, scaled, 0, 1)
    mixed_b = mixed.astype(jnp.bfloat16)
    own_patches = rows // row_count
    own_bytes = own_patches * PATCH
    rows_in, rows_out = (
        lax.all_gather(hidden_in, "seq", axis=1, tiled=True),
        lax.all_gather(hidden_out, "seq", axis=1, tiled=True),
    )
    partial_value = contract(mixed_b, local_weight, 0, 0)
    projected = lax.psum(partial_value.astype(jnp.bfloat16), "row")
    every = local_inputs(
        byte_ids,
        projected,
        patch_tasks,
        byte_table,
        position_table,
        norm_gain,
        local_down,
        local_scales,
    )
    normed_all = every[2]
    shrunk_all = every[5]
    cotangent_all = lax.all_gather(cotangent, "row", axis=0, tiled=True)
    inputs, inverse, normed, lowered, scales, shrunk, byte_tasks = [
        lax.dynamic_slice_in_dim(value, row_index * own_bytes, own_bytes, 0) for value in every
    ]
    upper = contract(normed_all, rows_in, 1, 1) + jnp.dot(
        shrunk_all, local_up, preferred_element_type=jnp.float32
    )
    through = contract(cotangent_all, rows_out, 1, 1)
    grown = (through * gelu_slope(upper)).astype(jnp.bfloat16)
    grad_local_up = contract(shrunk_all, grown, 0, 0)
    back_norm, back_rank = (
        lax.psum_scatter(
            jnp.dot(grown, rows_in, preferred_element_type=jnp.float32).astype(jnp.bfloat16),
            "row",
            scatter_dimension=0,
            tiled=True,
        ).astype(jnp.float32),
        lax.psum_scatter(
            contract(grown, local_up, 1, 1).astype(jnp.bfloat16),
            "row",
            scatter_dimension=0,
            tiled=True,
        ).astype(jnp.float32),
    )
    grad_local_scales = task_totals(byte_tasks, back_rank * lowered)
    moved = (back_rank * scales).astype(jnp.bfloat16)
    grad_local_down = contract(normed, moved, 0, 0)
    back_total = back_norm + contract(moved, local_down, 1, 1)
    gained = back_total * norm_gain
    average = jnp.mean(gained * inputs, axis=1, keepdims=True)
    back_inputs = cotangent.astype(jnp.float32) + inverse * (
        gained - inputs * inverse * inverse * average
    )
    patch_grad = back_inputs.reshape(own_patches, PATCH, -1).sum(axis=1).astype(jnp.bfloat16)
    back_mixed = contract(
        lax.all_gather(patch_grad, "row", axis=0, tiled=True), local_weight, 1, 1
    ).astype(jnp.bfloat16)
    grad_global_up = contract(scaled, back_mixed, 0, 0)
    back_scaled = lax.psum(contract(back_mixed, global_up, 1, 1), "row")
    grad_global_scales = task_totals(patch_tasks, back_scaled * reduced)
    back_reduced = (back_scaled * task_scales).astype(jnp.bfloat16)
    grad_global_down = contract(attended, back_reduced, 0, 0)
    grad_global_down, grad_global_up, grad_global_scales, grad_local_up = lax.psum(
        (grad_global_down, grad_global_up, grad_global_scales, grad_local_up), "seq"
    )
    grad_local_down, grad_local_scales = lax.psum(
        (grad_local_down, grad_local_scales), ("seq", "row")
    )
    return (
        grad_global_down,
        grad_global_up,
        grad_global_scales,
        grad_local_down,
        grad_local_up,
        grad_local_scales,
    )


MESH = pl.DeviceIdType.MESH
SPAN = 256


def remote(src, dst, send, recv, seq, row):
    return pltpu.make_async_remote_copy(
        src_ref=src,
        dst_ref=dst,
        send_sem=send,
        recv_sem=recv,
        device_id=(seq, row),
        device_id_type=MESH,
    )


def exact(left, right, left_dim, right_dim):
    return lax.dot_general(
        left, right, (((left_dim,), (right_dim,)), ((), ())), precision=lax.Precision.HIGHEST,
        preferred_element_type=jnp.float32,
    )


def split_pair(value):
    high = value.astype(jnp.bfloat16)
    low = (value - high.astype(jnp.float32)).astype(jnp.bfloat16)
    return high, low


def step_kernel(
    chips, depth,
    q_hbm, k_hbm, v_hbm, tasks_hbm, res_hbm, ow_hbm, gd_hbm, gu_hbm, gs_hbm, lw_hbm, ids_hbm,
    table_hbm, pos_hbm, gain_hbm, hi_hbm, ho_hbm, ld_hbm, lu_hbm, ls_hbm, cot_hbm,
    ggd_out, ggu_out, gsc_out, gld_out, glu_out, lsc_out,
    q_ref, k_ref, v_ref, tasks_ref, res_ref, ow_ref, gd_ref, gu_ref, gs_ref, lw_ref, ids_ref,
    pos_ref, gain_ref, ld_ref, ls_ref, cot_ref, wi, wo, wit,
    qb, kb, vb, ob, att, lwb, w2, acc, e1, e1r, mb, mr, bridge,
    red, redr, lif, emb, inp, nrm, inv, low, sca, bl, gr, mv, bp, bpr, cross, crossr,
    early, early_in, early_full, late, late_in, late_full,
    in_sem, a_send, a_recv, f_send, f_recv, o_send, o_recv, z_send, z_recv, x_send, x_recv,
    p_send, p_recv, c_send, c_recv, y_send, y_recv, e_send, e_recv, b_send, b_recv,
    r_send, r_recv, g_send, g_recv,
):
    bf, f32 = jnp.bfloat16, jnp.float32
    count = 2 * chips
    owners = chips
    me = lax.axis_index("seq")
    row = lax.axis_index("row")
    other = 1 - row
    chip, core = me // 2, lax.rem(me, 2)
    mate = 2 * chip + (1 - core)
    rows, width = q_hbm.shape
    half = width // 2
    columns = lw_hbm.shape[1]
    rank = gu_hbm.shape[0]
    wide = columns + HEAD
    shard = hi_hbm.shape[0]
    vocab = table_hbm.shape[0]
    total = rows * PATCH
    pieces = total // SPAN
    per_piece = SPAN // PATCH
    tiles = width // HEAD + columns // HEAD + 1

    def heads_of(number):
        return pl.ds(pl.multiple_of(number * HEAD, HEAD), HEAD)

    def shard_of(slot):
        return pl.ds(pl.multiple_of(slot * shard, shard), shard)

    barrier = pltpu.get_barrier_semaphore()
    peers = [(lax.rem(me + d, count), row) for d in range(1, count)] + [(me, other)]
    for seq, line in peers:
        pl.semaphore_signal(barrier, inc=1, device_id=(seq, line), device_id_type=MESH)

    loads = {}

    def load(name, src, dst):
        copy = pltpu.make_async_copy(src, dst, in_sem.at[len(loads)])
        copy.start()
        loads[name] = copy

    load("ho", ho_hbm, wo.at[shard_of(me)])
    load("hi", hi_hbm, wi.at[shard_of(me)])
    load("k", k_hbm, k_ref)
    load("v", v_hbm, v_ref)
    load("q", q_hbm, q_ref)
    load("lw", lw_hbm, lw_ref)
    load("cot", cot_hbm, cot_ref.at[row])
    load("gu", gu_hbm, gu_ref)
    load("ow", ow_hbm, ow_ref)
    load("res", res_hbm, res_ref)
    load("gd", gd_hbm, gd_ref)
    load("lu", lu_hbm, wi.at[pl.ds(columns, rank)])
    load("ld", ld_hbm, ld_ref.at[pl.ds(0, rank)])
    load("table", table_hbm, emb.at[pl.ds(0, vocab), pl.ds(0, columns)])
    load("tasks", tasks_hbm, tasks_ref)
    load("ids", ids_hbm, ids_ref)
    load("pos", pos_hbm, pos_ref)
    load("gain", gain_hbm, gain_ref)
    load("gs", gs_hbm, gs_ref)
    load("ls", ls_hbm, ls_ref)

    ld_ref[rank:] = jnp.zeros((HEAD - rank, columns), bf)
    wi[columns + rank :] = jnp.zeros((HEAD - rank, width), bf)
    emb[vocab : vocab + rows, :columns] = jnp.zeros((rows, columns), bf)
    emb[:vocab, columns:] = jnp.zeros((vocab, 2 * HEAD), bf)
    emb[vocab + HEAD :] = jnp.zeros((HEAD, wide + HEAD), bf)
    for buffer in (early, late):
        buffer[tiles:] = jnp.zeros((count - tiles, rank, HEAD), bf)

    pl.semaphore_wait(barrier, len(peers))

    own = heads_of(chip)
    near = chips // 2
    place_in = lax.rem(chip, near)
    home = chip - place_in
    away = near - home
    own_half = pl.ds(pl.multiple_of(core * half, half), half)

    def hand(which, to):
        src, dst = (
            (k_ref, kb.at[me]), (v_ref, vb.at[me]), (q_ref, qb.at[chip])
        )[which]
        return remote(
            src.at[:, heads_of(to)], dst, a_send.at[which, to], a_recv.at[which, chip],
            2 * to + core, row,
        )

    def landed(which, source):
        dst = (kb.at[2 * source + core], vb.at[2 * source + core], qb.at[source])[which]
        remote(
            dst, dst, a_send.at[which, source], a_recv.at[which, source], me, row
        ).wait_recv()

    targets = [away + lax.rem(place_in + j, near) for j in range(near)] + [
        home + lax.rem(place_in + j, near) for j in range(1, near)
    ]
    levels = chips // depth
    level, side = chip // depth, lax.rem(chip, depth)
    weights_in = ((1, wo), (0, wi))
    neighbour = 2 * (level * depth + (1 - side)) + core

    def slot_of(number, line):
        return 2 * (number * depth + line) + core

    def move(which, slot, sends, recvs, to):
        buffer = wo if which else wi
        piece = buffer.at[shard_of(slot)]
        return remote(piece, piece, sends, recvs, to, row)

    def pass_along(which, source):
        slot = slot_of(source, side)
        for way, step in ((0, 1), (1, -1)):
            ahead = level + step
            fits = (ahead >= 0) & (ahead < levels) & ((source - level) * step <= 0)

            @pl.when(fits)
            def _():
                move(
                    which, slot, z_send.at[which, source, way], z_recv.at[which, source],
                    slot_of(ahead, side),
                ).start()

    def settle_along(which, source):
        slot = slot_of(source, side)
        for way, step in ((0, 1), (1, -1)):
            ahead = level + step
            fits = (ahead >= 0) & (ahead < levels) & ((source - level) * step <= 0)

            @pl.when(fits)
            def _():
                move(
                    which, slot, z_send.at[which, source, way], z_recv.at[which, source],
                    slot_of(ahead, side),
                ).wait_send()

    def across(which, source, line):
        return move(
            which, slot_of(source, line), x_send.at[which, source], x_recv.at[which, source],
            neighbour,
        )

    def to_mate(which, source, line):
        number = jnp.where(line == side, source, levels + source)
        return move(
            which, slot_of(source, line), p_send.at[which, number], p_recv.at[which, number], mate
        )

    def relay(hop):
        for which, buffer in weights_in:
            for source in (level - hop, level + hop):

                @pl.when((source >= 0) & (source < levels))
                def _():
                    move(
                        which, slot_of(source, side), z_send.at[which, source, 0],
                        z_recv.at[which, source], me,
                    ).wait_recv()
                    pass_along(which, source)
                    across(which, source, side).start()
                    to_mate(which, source, side).start()

    def cross_over(hop):
        for which, buffer in weights_in:
            for source in {0: (level,)}.get(hop, (level - hop, level + hop)):

                @pl.when((source >= 0) & (source < levels))
                def _():
                    across(which, source, 1 - side).wait_recv()
                    to_mate(which, source, 1 - side).start()

    loads["ho"].wait()
    loads["hi"].wait()
    for which, buffer in weights_in:
        pass_along(which, level)
        across(which, level, side).start()
        to_mate(which, level, side).start()

    loads["k"].wait()
    loads["v"].wait()
    loads["q"].wait()


    def share(which, source):
        buffer = (kb, vb)[which]
        slot = 2 * source + core
        return remote(
            buffer.at[slot], buffer.at[slot], f_send.at[which, source], f_recv.at[which, source],
            mate, row,
        )

    kb[me] = k_ref[:, own]
    vb[me] = v_ref[:, own]
    qb[chip] = q_ref[:, own]
    for to in targets:
        for which in range(2):
            hand(which, to).start()
    for which, src in enumerate((k_ref, v_ref)):
        remote(
            src.at[:, own], (kb, vb)[which].at[me], f_send.at[which, chip],
            f_recv.at[which, chip], mate, row,
        ).start()
    loads["lw"].wait()
    lw_copy = remote(lw_ref.at[own_half], lwb.at[own_half], y_send.at[0], y_recv.at[0], me, other)
    lw_copy.start()
    loads["cot"].wait()
    cot_copy = remote(
        cot_ref.at[row], cot_ref.at[row], c_send.at[0], c_recv.at[0], me, other
    )
    cot_copy.start()

    loads["gu"].wait()
    mb[...] = jnp.dot(gu_ref[...], lw_ref[...], preferred_element_type=f32).astype(bf)
    m_copy = remote(mb, mr, y_send.at[2], y_recv.at[2], me, other)
    m_copy.start()

    tile = math.gcd(width, SPAN)
    loads["ow"].wait()

    @pl.loop(0, width // tile)
    def _(index):
        block = pl.ds(pl.multiple_of(index * tile, tile), tile)
        acc[block] = jnp.dot(
            ow_ref[block, pl.ds(pl.multiple_of(row * width, width), width)],
            lw_ref[...],
            preferred_element_type=f32,
        )

    relay(1)
    for to in targets:
        hand(2, to).start()
    cross_over(0)
    for j in range(1, near):
        source = home + lax.rem(place_in + near - j, near)
        for which in range(2):
            landed(which, source)
            share(which, source).start()
    for j in range(near):
        source = away + lax.rem(place_in + near - j, near)
        for which in range(2):
            landed(which, source)
            share(which, source).start()
    for source in range(chips):
        for which in range(2):
            buffer = (kb, vb)[which]
            slot = 2 * source + 1 - core
            remote(
                buffer.at[slot], buffer.at[slot], f_send.at[which, source],
                f_recv.at[which, source], mate, row,
            ).wait_recv()

    lw_copy.wait_recv()
    lw_mate = remote(lwb.at[own_half], lwb.at[own_half], y_send.at[1], y_recv.at[1], mate, row)
    lw_mate.start()
    factor = 1.0 / math.sqrt(HEAD) / math.log(2.0)
    span = chips * rows

    def attend(i, late_half):
        query = qb[i]
        start = chips if late_half else 0
        fresh = contract(query, kb[start : start + chips].reshape(span, HEAD), 1, 1)
        places = lax.broadcasted_iota(jnp.int32, (rows, span), 1)
        queries = lax.broadcasted_iota(jnp.int32, (rows, span), 0) + (
            (2 * i + core - start) * rows
        )
        fresh = jnp.where(places <= queries, fresh, -1e30)
        top = jnp.max(fresh, axis=1, keepdims=True)
        if late_half:
            scores = contract(query, kb[:start].reshape(span, HEAD), 1, 1)
            top = jnp.maximum(top, jnp.max(scores, axis=1, keepdims=True))
        weights = jnp.exp2((fresh - top) * factor)
        mass = jnp.sum(weights, axis=1, keepdims=True)
        mixed = jnp.dot(
            weights.astype(bf), vb[start : start + chips].reshape(span, HEAD),
            preferred_element_type=f32,
        )
        if late_half:
            weights = jnp.exp2((scores - top) * factor)
            mass = mass + jnp.sum(weights, axis=1, keepdims=True)
            mixed = mixed + jnp.dot(
                weights.astype(bf), vb[:start].reshape(span, HEAD), preferred_element_type=f32
            )
        ob[i] = (mixed / mass).astype(bf)

    @pl.loop(0, chips)
    def _(step):
        @pl.when(step == 1)
        def _():
            relay(2)
            cross_over(1)

        at_home = (step < near - 1) | (step == chips - 1)
        stage = jnp.where(at_home, lax.rem(step + 1, near), step - (near - 1))
        i = jnp.where(at_home, home, away) + lax.rem(place_in + near - stage, near)

        @pl.when(i != chip)
        def _():
            landed(2, i)

        @pl.when(i < near)
        def _():
            attend(i, False)

        @pl.when(i >= near)
        def _():
            attend(i, True)

        @pl.when(i != chip)
        def _():
            remote(
                ob.at[i], att.at[:, own], o_send.at[i], o_recv.at[chip], 2 * i + core, row
            ).start()

    att[:, own] = ob[chip]

    lw_mate.wait_recv()
    @pl.loop(0, width // tile)
    def _(index):
        block = pl.ds(pl.multiple_of(index * tile, tile), tile)
        summed = acc[block] + jnp.dot(
            ow_ref[block, pl.ds(pl.multiple_of(other * width, width), width)],
            lwb[...],
            preferred_element_type=f32,
        )
        w2[block] = summed.astype(bf)

    for name in ("res", "gd", "lu", "ld", "table", "tasks", "ids", "pos", "gain", "gs", "ls"):
        loads[name].wait()
    picks = (
        lax.broadcasted_iota(jnp.int32, (TASKS, rows), 0) == tasks_ref[...]
    ).astype(f32)

    def widen(table):
        return jnp.concatenate([table, jnp.zeros((TASKS, HEAD - rank), f32)], axis=1)

    task_scales = exact(gs_ref[...], picks, 0, 0)
    high, low_part = split_pair(exact(picks, widen(ls_ref[...]), 0, 0))
    emb[vocab : vocab + rows, columns:wide] = high
    emb[vocab : vocab + rows, wide:] = low_part
    emb[vocab + rows : vocab + rows + 2 * PATCH, :columns] = jnp.concatenate(
        [pos_ref[...].astype(f32), jnp.zeros((PATCH, columns), f32)], axis=0
    ).astype(bf)
    direct = jnp.dot(res_ref[...], lw_ref[...], preferred_element_type=f32)
    inp[:rows] = direct

    cot_copy.wait_recv()
    m_copy.wait_recv()
    bridge[...] = (mb[...].astype(f32) + mr[...].astype(f32)).astype(bf)
    belongs = (
        lax.broadcasted_iota(jnp.int32, (rows, total), 1) // PATCH
        == lax.broadcasted_iota(jnp.int32, (rows, total), 0)
    ).astype(f32).astype(bf)
    own_bytes = total // 2
    cot_sum = sum(
        jnp.dot(
            belongs[:, index * own_bytes : (index + 1) * own_bytes], cot_ref[index],
            preferred_element_type=f32,
        )
        for index in range(2)
    )

    for hop in range(3, levels):
        relay(hop)
    for hop in range(2, levels - 1):
        cross_over(hop)
    for i in range(chips):

        @pl.when(i != chip)
        def _():
            back = remote(
                ob.at[i], att.at[:, heads_of(i)], o_send.at[i], o_recv.at[i], 2 * i + core, row
            )
            back.wait_recv()
            back.wait_send()

    e_copies = []
    red[...] = contract(gd_ref[...], att[...], 1, 1).astype(bf)
    red_copy = remote(red, redr, y_send.at[3], y_recv.at[3], me, other)
    red_copy.start()
    e1[...] = (
        jnp.dot(att[...], w2[...], preferred_element_type=f32) + inp[:rows]
    ).astype(bf)
    for index in range(pieces):
        patches = pl.ds(index * per_piece, per_piece)
        copy = remote(e1.at[patches], e1r.at[patches], e_send.at[index], e_recv.at[index], me, other)
        copy.start()
        e_copies.append(copy)
    red_copy.wait_recv()
    reduced = red[...].astype(f32) + redr[...].astype(f32)
    scaled = (reduced * task_scales).astype(bf)
    lifted = contract(scaled, bridge[...], 0, 0)

    depth_all = emb.shape[0]
    lif[...] = lifted

    @pl.loop(0, pieces)
    def _(index):
        block = pl.ds(pl.multiple_of(index * SPAN, SPAN), SPAN)
        patches = pl.ds(pl.multiple_of(index * per_piece, per_piece), per_piece)
        remote(
            e1.at[patches], e1r.at[patches], e_send.at[index], e_recv.at[index], me, other
        ).wait_recv()
        emb[pl.ds(pl.multiple_of(vocab + index * per_piece, per_piece), per_piece), :columns] = (
            e1[patches].astype(f32) + e1r[patches].astype(f32) + lif[patches]
        ).astype(bf)

        @pl.when(index == pieces // 2)
        def _():
            cross_over(levels - 1)

        line = lax.broadcasted_iota(jnp.int32, (depth_all, SPAN), 0)
        byte = lax.broadcasted_iota(jnp.int32, (depth_all, SPAN), 1) + index * SPAN
        chosen = (
            (line == ids_ref[:, block])
            | (line == vocab + byte // PATCH)
            | (line == vocab + rows + lax.rem(byte, PATCH))
        )
        found = contract(jnp.where(chosen, 1.0, 0.0).astype(bf), emb[...], 0, 0)
        inputs = found[:, :columns]
        scales = found[:, columns:wide] + found[:, wide:]
        inverse = lax.rsqrt(jnp.mean(inputs * inputs, axis=1, keepdims=True) + 1e-06)
        normed = (inputs * inverse * gain_ref[...]).astype(bf)
        lowered = contract(normed, ld_ref[...], 1, 1)
        inp[block] = inputs
        inv[block] = jnp.broadcast_to(inverse, (SPAN, HEAD))
        sca[block] = scales
        low[block] = lowered
        nrm[block, :columns] = normed
        nrm[block, columns:] = (lowered * scales).astype(bf)

    def mates_weights(which):
        for source in range(levels):
            for line in (side, 1 - side):
                to_mate(which, source, line).wait_recv()

    mates_weights(1)
    mates_weights(0)
    wit[...] = jnp.transpose(wi[...])
    @pl.loop(0, pieces)
    def _(index):
        block = pl.ds(pl.multiple_of(index * SPAN, SPAN), SPAN)
        upper = jnp.dot(nrm[block], wi[...], preferred_element_type=f32)
        inner = pl.ds(pl.multiple_of(lax.rem(index * SPAN, own_bytes), SPAN), SPAN)
        through = jnp.dot(
            cot_ref[index * SPAN // own_bytes, inner], wo[...], preferred_element_type=f32
        )
        grown = (through * gelu_slope(upper)).astype(bf)
        gr[block] = grown
        both = jnp.dot(grown, wit[...], preferred_element_type=f32)
        back_rank = both[:, columns:]
        moved = (back_rank * sca[block]).astype(bf)
        mv[block] = moved
        bl[block] = back_rank * low[block]
        back_total = both[:, :columns] + jnp.dot(
            moved, ld_ref[...], preferred_element_type=f32
        )
        inputs = inp[block]
        inverse = inv[block][:, :1]
        gained = back_total * gain_ref[...]
        average = jnp.mean(gained * inputs, axis=1, keepdims=True)
        back_inputs = inverse * (gained - inputs * (inverse * inverse * average))
        near = (
            lax.broadcasted_iota(jnp.int32, (per_piece, SPAN), 1) // PATCH
            == lax.broadcasted_iota(jnp.int32, (per_piece, SPAN), 0)
        ).astype(f32).astype(bf)
        patches = pl.ds(pl.multiple_of(index * per_piece, per_piece), per_piece)
        bp[patches] = jnp.dot(
            near, back_inputs.astype(bf), preferred_element_type=f32
        ).astype(bf)
        remote(
            bp.at[patches], bpr.at[patches], b_send.at[index], b_recv.at[index], me, other
        ).start()

    down = contract(mv[...], nrm[:, :columns], 0, 0)[:rank]
    high, low_part = split_pair(bl[...])
    by_patch = jnp.dot(belongs, high, preferred_element_type=f32) + jnp.dot(
        belongs, low_part, preferred_element_type=f32
    )
    small = exact(picks, by_patch, 1, 0)
    small = jnp.concatenate([small, jnp.zeros_like(small)], axis=0)
    cross[:, :columns] = down.astype(bf)
    cross[:, columns:] = small.astype(bf)
    cross_copy = remote(cross, crossr, y_send.at[4], y_recv.at[4], me, other)
    cross_copy.start()
    lift = contract(nrm[:, columns:], gr[...], 0, 0)[:rank].astype(bf)
    spread = width // HEAD
    thin = columns // HEAD
    for t in range(spread):
        early[t] = lift[:, t * HEAD : (t + 1) * HEAD]
    base = owners // 2

    def spread_out(kind, source, landing, first, last):
        for t in range(first, last):
            to = base + t

            @pl.when(to != me)
            def _():
                remote(
                    source.at[pl.ds(2 * t, 2)], landing.at[me], r_send.at[kind, t],
                    r_recv.at[kind, me], to, row,
                ).start()

            @pl.when(to == me)
            def _():
                landing[me] = source[2 * t : 2 * t + 2]

    def settle_out(kind, source, landing):
        for t in range(owners):
            to = base + t

            @pl.when(to != me)
            def _():
                remote(
                    source.at[pl.ds(2 * t, 2)], landing.at[me], r_send.at[kind, t],
                    r_recv.at[kind, me], to, row,
                ).wait_send()

    mine = (me >= base) & (me < base + owners)
    place = jnp.where(mine, me - base, 0)

    def gather_in(kind, landing, final):
        @pl.when(mine)
        def _():
            for d in range(1, count):
                source = lax.rem(me + d, count)
                remote(
                    landing.at[source], landing.at[source], r_send.at[kind, 0],
                    r_recv.at[kind, source], me, row,
                ).wait_recv()
            final[place] = jnp.sum(landing[...].astype(f32), axis=0).astype(bf)
            for d in range(1, count):
                to = lax.rem(me + d, count)
                remote(
                    final.at[place], final.at[place], g_send.at[kind, d],
                    g_recv.at[kind, place], to, row,
                ).start()

    def finish_in(kind, final):
        for t in range(owners):

            @pl.when(me != base + t)
            def _():
                remote(
                    final.at[t], final.at[t], g_send.at[kind, 0], g_recv.at[kind, t], me, row
                ).wait_recv()

    def settle_in(kind, final):
        @pl.when(mine)
        def _():
            for d in range(1, count):
                to = lax.rem(me + d, count)
                remote(
                    final.at[place], final.at[place], g_send.at[kind, d],
                    g_recv.at[kind, place], to, row,
                ).wait_send()

    spread_out(0, early, early_in, 0, spread // 2)

    for index in range(pieces):
        patches = pl.ds(index * per_piece, per_piece)
        remote(
            bp.at[patches], bpr.at[patches], b_send.at[index], b_recv.at[index], me, other
        ).wait()
    patch_grad = (bp[...].astype(f32) + bpr[...].astype(f32) + cot_sum).astype(bf)
    pulled = jnp.dot(scaled, patch_grad, preferred_element_type=f32).astype(bf)
    back_scaled = contract(bridge[...], patch_grad, 1, 1)
    back_reduced = (back_scaled * task_scales).astype(bf)
    outward = jnp.dot(back_reduced, att[...], preferred_element_type=f32).astype(bf)
    product = back_scaled * reduced
    product = jnp.concatenate([product, jnp.zeros((HEAD - rank, rows), f32)], axis=0)
    tops = exact(picks, product, 1, 1)
    tops = jnp.concatenate([tops, jnp.zeros_like(tops)], axis=0)
    for t in range(spread):
        late[t] = outward[:, t * HEAD : (t + 1) * HEAD]
    for t in range(thin):
        late[spread + t] = pulled[:, t * HEAD : (t + 1) * HEAD]
    late[spread + thin] = tops.astype(bf)
    spread_out(1, late, late_in, 0, owners)
    cross_copy.wait_recv()
    joint = (cross[...].astype(f32) + crossr[...].astype(f32)).astype(bf)
    for t in range(thin):
        early[spread + t] = joint[:, t * HEAD : (t + 1) * HEAD]
    early[spread + thin] = joint[:, columns:]
    spread_out(0, early, early_in, spread // 2, owners)
    gather_in(0, early_in, early_full)
    gather_in(1, late_in, late_full)
    finish_in(0, early_full)

    def tile_of(final, t):
        return final[t // 2, t % 2]

    for t in range(spread):
        glu_out[:, t * HEAD : (t + 1) * HEAD] = tile_of(early_full, t).astype(f32)
    for t in range(thin):
        gld_out[:, t * HEAD : (t + 1) * HEAD] = tile_of(early_full, spread + t).astype(f32)
    lsc_out[...] = tile_of(early_full, spread + thin)[:TASKS, :rank].astype(f32)
    finish_in(1, late_full)
    for t in range(spread):
        ggd_out[:, t * HEAD : (t + 1) * HEAD] = tile_of(late_full, t).astype(f32)
    for t in range(thin):
        bridge[:, t * HEAD : (t + 1) * HEAD] = tile_of(late_full, spread + t)
    ggu_out[...] = contract(bridge[...], lw_ref[...], 1, 1)
    gsc_out[...] = tile_of(late_full, spread + thin)[:TASKS, :rank].astype(f32)
    for kind, source, landing, final in (
        (0, early, early_in, early_full), (1, late, late_in, late_full)
    ):
        settle_out(kind, source, landing)
        settle_in(kind, final)
    for which, buffer in weights_in:
        for source in range(levels):
            settle_along(which, source)
            across(which, source, side).wait_send()
            for line in (side, 1 - side):
                to_mate(which, source, line).wait_send()
    for to in targets:
        for which in range(3):
            hand(which, to).wait_send()
    for source in range(chips):
        for which in range(2):
            share(which, source).wait_send()
    for copy in [lw_copy, lw_mate, cot_copy, m_copy, red_copy, cross_copy] + e_copies:
        copy.wait_send()


def copy_kernel(*refs):
    number = len(refs) // 2
    for source, target in zip(refs[:number], refs[number:]):
        target[...] = source[...]


def paired_body(
    patch_queries, patch_keys, patch_values, patch_tasks, residual, output_weight, global_down,
    global_up, global_scales, local_weight, byte_ids, byte_table, position_table, norm_gain,
    hidden_in, hidden_out, local_down, local_up, local_scales, cotangent,
):
    count = lax.axis_size("seq")
    rows, width = patch_queries.shape
    chips = count // 2
    depth = 2
    levels = chips // depth
    columns = local_weight.shape[1]
    rank = global_up.shape[0]
    vocab = byte_table.shape[0]
    total = byte_ids.shape[0]
    wide = columns + HEAD
    pieces = total // SPAN
    bf, f32 = jnp.bfloat16, jnp.float32
    vm = pltpu.VMEM
    dma = pltpu.SemaphoreType.DMA
    args = (
        patch_queries, patch_keys, patch_values, patch_tasks.reshape(1, rows), residual,
        output_weight, jnp.transpose(global_down), global_up, global_scales, local_weight,
        byte_ids.reshape(1, total), byte_table, position_table, norm_gain.reshape(1, columns),
        jnp.transpose(hidden_in), jnp.transpose(hidden_out), jnp.transpose(local_down), local_up,
        local_scales, cotangent,
    )
    outs = pl.pallas_call(
        functools.partial(step_kernel, chips, depth),
        out_shape=(
            jax.ShapeDtypeStruct((rank, width), f32),
            jax.ShapeDtypeStruct((rank, width), f32),
            jax.ShapeDtypeStruct((TASKS, rank), f32),
            jax.ShapeDtypeStruct((rank, columns), f32),
            jax.ShapeDtypeStruct((rank, width), f32),
            jax.ShapeDtypeStruct((TASKS, rank), f32),
        ),
        in_specs=[pl.BlockSpec(memory_space=pl.ANY)] * len(args),
        out_specs=(pl.BlockSpec(memory_space=vm),) * 6,
        scratch_shapes=[
            vm((rows, width), bf), vm((rows, width), bf), vm((rows, width), bf),
            vm((1, rows), jnp.int32), vm((rows, width), bf), vm(output_weight.shape, bf),
            vm((rank, width), bf), vm((rank, width), bf), vm((TASKS, rank), f32),
            vm((width, columns), bf), vm((1, total), jnp.int32), vm((PATCH, columns), bf),
            vm((1, columns), f32), vm((HEAD, columns), bf), vm((TASKS, rank), f32),
            vm((2, total // 2, columns), bf), vm((wide, width), bf), vm((columns, width), bf),
            vm((width, wide), bf),
            vm((chips, rows, HEAD), bf), vm((count, rows, HEAD), bf), vm((count, rows, HEAD), bf),
            vm((chips, rows, HEAD), bf), vm((rows, width), bf), vm((width, columns), bf),
            vm((width, columns), bf), vm((width, columns), f32), vm((rows, columns), bf),
            vm((rows, columns), bf), vm((rank, columns), bf), vm((rank, columns), bf),
            vm((rank, columns), bf), vm((rank, rows), bf), vm((rank, rows), bf),
            vm((rows, columns), f32),
            vm((vocab + 2 * HEAD, wide + HEAD), bf), vm((total, columns), f32),
            vm((total, wide), bf), vm((total, HEAD), f32), vm((total, HEAD), f32),
            vm((total, HEAD), f32), vm((total, HEAD), f32), vm((total, width), bf),
            vm((total, HEAD), bf), vm((rows, columns), bf), vm((rows, columns), bf),
            vm((rank, wide), bf), vm((rank, wide), bf),
        ]
        + [
            vm((count, rank, HEAD), bf), vm((count, 2, rank, HEAD), bf),
            vm((chips, 2, rank, HEAD), bf),
        ]
        * 2
        + [
            dma((len(args),)), dma((3, chips)), dma((3, chips)), dma((2, chips)), dma((2, chips)),
            dma((chips,)), dma((chips,)), dma((2, levels, 2)), dma((2, levels)), dma((2, levels)),
            dma((2, levels)), dma((2, chips)), dma((2, chips)), dma((1,)), dma((1,)), dma((5,)),
            dma((5,)), dma((pieces,)), dma((pieces,)), dma((pieces,)), dma((pieces,)),
            dma((2, chips)), dma((2, count)), dma((2, count)), dma((2, chips)),
        ],
        compiler_params=pltpu.CompilerParams(
            collective_id=0, has_side_effects=True, vmem_limit_bytes=60 * 1024 * 1024
        ),
        name="step",
    )(*args)
    ggd, ggu, gsc, gld, glu, lsc = pl.pallas_call(
        copy_kernel,
        out_shape=tuple(jax.ShapeDtypeStruct(item.shape, item.dtype) for item in outs),
        in_specs=[pl.BlockSpec(memory_space=vm)] * len(outs),
        out_specs=(pl.BlockSpec(memory_space=vm),) * len(outs),
        name="spill",
    )(*outs)
    return (jnp.transpose(ggd), ggu, gsc, jnp.transpose(gld), glu, lsc)


def pick_body(seq_count, row_count, *args):
    heads = args[0].shape[1] // HEAD
    rank = args[7].shape[0]
    hidden = args[14].shape[0]
    fits = (
        row_count == 2
        and seq_count == 2 * heads
        and heads % 4 == 0
        and rank == 2 * TASKS
        and args[0].shape[1] == hidden
        and (4 * rank * hidden) % (seq_count * 16 * HEAD) == 0
        and hidden // HEAD + args[9].shape[1] // HEAD < seq_count
        and args[0].shape[0] == HEAD
    )
    return paired_body(*args) if fits else general_body(*args)


def solution(mesh):
    placed = (
        P("seq", "row"),
        P("seq", "row"),
        P("seq", "row"),
        P("seq"),
        P("seq", "row"),
        P("row", None),
        P("row", None),
        P(None, "row"),
        P(),
        P("row", None),
        P("seq"),
        P(),
        P(),
        P(),
        P("row", "seq"),
        P("row", "seq"),
        P(),
        P(None, "row"),
        P(),
        P(("seq", "row"), None),
    )
    chosen = functools.partial(pick_body, mesh.shape["seq"], mesh.shape["row"])
    return jax.shard_map(
        chosen,
        mesh=mesh,
        in_specs=placed,
        out_specs=(P("row", None), P(None, "row"), P(), P(), P(None, "row"), P()),
        check_vma=False,
    )
```

```python
import functools
import math

import jax
import jax.numpy as jnp
from jax import lax
from jax.experimental import pallas as pl
from jax.experimental.pallas import tpu as pltpu
from jax.sharding import PartitionSpec as P

HEAD = 128
VOCAB = 256
PATCH = 8
TASKS = 8


def contract(left, right, left_dim, right_dim):
    return lax.dot_general(
        left, right, (((left_dim,), (right_dim,)), ((), ())), preferred_element_type=jnp.float32
    )


def select_rows(table, tasks):
    picks = (tasks[:, None] == jnp.arange(table.shape[0], dtype=jnp.int32)[None, :]).astype(
        jnp.float32
    )
    return jnp.dot(picks, table, precision=lax.Precision.HIGHEST)


def task_totals(tasks, values):
    picks = (tasks[:, None] == jnp.arange(TASKS, dtype=jnp.int32)[None, :]).astype(jnp.float32)
    return lax.dot_general(picks, values, (((0,), (0,)), ((), ())), precision=lax.Precision.HIGHEST)


def gelu_slope(upper):
    cumulative = 0.5 * (1.0 + lax.erf(upper * 0.7071067811865476))
    density = jnp.exp(-0.5 * upper * upper) * 0.3989422804014327
    return cumulative + upper * density


def local_inputs(
    identities, projected, tasks, byte_table, position_table, norm_gain, local_down, local_scales
):
    count = identities.shape[0]
    picks = (identities[:, None] == jnp.arange(VOCAB, dtype=jnp.int32)[None, :]).astype(
        jnp.bfloat16
    )
    embedded = jnp.dot(picks, byte_table, preferred_element_type=jnp.float32)
    patches = count // PATCH
    inputs = (
        embedded.reshape(patches, PATCH, -1)
        + position_table.astype(jnp.float32)[None]
        + projected.astype(jnp.float32)[:, None, :]
    )
    inputs = inputs.reshape(count, -1)
    inverse = lax.rsqrt(jnp.mean(inputs * inputs, axis=1, keepdims=True) + 1e-06)
    normed = (inputs * inverse * norm_gain).astype(jnp.bfloat16)
    lowered = jnp.dot(normed, local_down, preferred_element_type=jnp.float32)
    byte_tasks = jnp.repeat(tasks, PATCH)
    scales = select_rows(local_scales, byte_tasks)
    shrunk = (lowered * scales).astype(jnp.bfloat16)
    return (inputs, inverse, normed, lowered, scales, shrunk, byte_tasks)


def keep_state(current):
    return current


def update_state(state, query_rows, first, key_heads, value_heads, key_places, scale):
    running_max, running_sum, running_out = state
    count = query_rows.shape[0]
    heads = key_heads.shape[1]
    query_heads = query_rows.reshape(count, heads, HEAD)
    scores = (
        jnp.einsum("qhd,khd->hqk", query_heads, key_heads, preferred_element_type=jnp.float32)
        * scale
    )
    query_places = first + jnp.arange(count, dtype=jnp.int32)
    allowed = key_places[None, :] <= query_places[:, None]
    scores = jnp.where(allowed[None], scores, -1e30)
    new_max = jnp.maximum(running_max, jnp.max(scores, axis=2))
    weights = jnp.where(allowed[None], jnp.exp(scores - new_max[:, :, None]), 0.0)
    shrink = jnp.exp(running_max - new_max)
    running_sum = running_sum * shrink + jnp.sum(weights, axis=2)
    mixed = jnp.einsum(
        "hqk,khd->qhd",
        weights.astype(jnp.bfloat16),
        value_heads,
        preferred_element_type=jnp.float32,
    )
    running_out = running_out * jnp.transpose(shrink)[:, :, None] + mixed
    return (new_max, running_sum, running_out)


def finish_state(state):
    running_max, running_sum, running_out = state
    result = running_out / jnp.transpose(running_sum)[:, :, None]
    return result.reshape(result.shape[0], -1).astype(jnp.bfloat16)


def general_body(
    patch_queries,
    patch_keys,
    patch_values,
    patch_tasks,
    residual,
    output_weight,
    global_down,
    global_up,
    global_scales,
    local_weight,
    byte_ids,
    byte_table,
    position_table,
    norm_gain,
    hidden_in,
    hidden_out,
    local_down,
    local_up,
    local_scales,
    cotangent,
):
    rows = patch_queries.shape[0]
    width = patch_queries.shape[1]
    heads = width // HEAD
    row_count = lax.axis_size("row")
    seq_index = lax.axis_index("seq")
    row_index = lax.axis_index("row")
    scale = 1.0 / math.sqrt(HEAD)
    own_first = seq_index * rows
    groups = [(patch_queries, own_first)]

    def visit(state, query_rows, first, key_heads, value_heads, key_places):

        def refresh(current):
            return update_state(
                current, query_rows, first, key_heads, value_heads, key_places, scale
            )

        return lax.cond(
            key_places[0] <= first + query_rows.shape[0] - 1, refresh, keep_state, state
        )

    initial = tuple(
        (
            (
                jnp.full((heads, query_rows.shape[0]), -1e30, jnp.float32),
                jnp.zeros((heads, query_rows.shape[0]), jnp.float32),
                jnp.zeros((query_rows.shape[0], heads, HEAD), jnp.float32),
            )
            for query_rows, first in groups
        )
    )
    key_piece = lax.all_gather(patch_keys, "seq", axis=0, tiled=True)
    value_piece = lax.all_gather(patch_values, "seq", axis=0, tiled=True)
    count = key_piece.shape[0]
    span = math.gcd(count, 1024)

    def one_span(index, states):
        offset = index * span
        key_heads = lax.dynamic_slice_in_dim(key_piece, offset, span, 0).reshape(span, heads, HEAD)
        value_heads = lax.dynamic_slice_in_dim(value_piece, offset, span, 0).reshape(
            span, heads, HEAD
        )
        key_places = offset + jnp.arange(span, dtype=jnp.int32)
        updated = []
        for (query_rows, first), state in zip(groups, states):
            updated.append(visit(state, query_rows, first, key_heads, value_heads, key_places))
        return tuple(updated)

    states = lax.fori_loop(0, count // span, one_span, initial)
    outputs = [finish_state(state) for state in states]
    attended = outputs[0]
    reduced = lax.psum(jnp.dot(attended, global_down, preferred_element_type=jnp.float32), "row")
    task_scales = select_rows(global_scales, patch_tasks)
    scaled = (reduced * task_scales).astype(jnp.bfloat16)
    mixed = lax.psum_scatter(
        contract(output_weight, attended, 0, 1).astype(jnp.bfloat16),
        "row",
        scatter_dimension=0,
        tiled=True,
    ).astype(jnp.float32)
    mixed = mixed + jnp.transpose(residual.astype(jnp.float32)) + contract(global_up, scaled, 0, 1)
    mixed_b = mixed.astype(jnp.bfloat16)
    own_patches = rows // row_count
    own_bytes = own_patches * PATCH
    rows_in, rows_out = (
        lax.all_gather(hidden_in, "seq", axis=1, tiled=True),
        lax.all_gather(hidden_out, "seq", axis=1, tiled=True),
    )
    partial_value = contract(mixed_b, local_weight, 0, 0)
    projected = lax.psum(partial_value.astype(jnp.bfloat16), "row")
    every = local_inputs(
        byte_ids,
        projected,
        patch_tasks,
        byte_table,
        position_table,
        norm_gain,
        local_down,
        local_scales,
    )
    normed_all = every[2]
    shrunk_all = every[5]
    cotangent_all = lax.all_gather(cotangent, "row", axis=0, tiled=True)
    inputs, inverse, normed, lowered, scales, shrunk, byte_tasks = [
        lax.dynamic_slice_in_dim(value, row_index * own_bytes, own_bytes, 0) for value in every
    ]
    upper = contract(normed_all, rows_in, 1, 1) + jnp.dot(
        shrunk_all, local_up, preferred_element_type=jnp.float32
    )
    through = contract(cotangent_all, rows_out, 1, 1)
    grown = (through * gelu_slope(upper)).astype(jnp.bfloat16)
    grad_local_up = contract(shrunk_all, grown, 0, 0)
    back_norm, back_rank = (
        lax.psum_scatter(
            jnp.dot(grown, rows_in, preferred_element_type=jnp.float32).astype(jnp.bfloat16),
            "row",
            scatter_dimension=0,
            tiled=True,
        ).astype(jnp.float32),
        lax.psum_scatter(
            contract(grown, local_up, 1, 1).astype(jnp.bfloat16),
            "row",
            scatter_dimension=0,
            tiled=True,
        ).astype(jnp.float32),
    )
    grad_local_scales = task_totals(byte_tasks, back_rank * lowered)
    moved = (back_rank * scales).astype(jnp.bfloat16)
    grad_local_down = contract(normed, moved, 0, 0)
    back_total = back_norm + contract(moved, local_down, 1, 1)
    gained = back_total * norm_gain
    average = jnp.mean(gained * inputs, axis=1, keepdims=True)
    back_inputs = cotangent.astype(jnp.float32) + inverse * (
        gained - inputs * inverse * inverse * average
    )
    patch_grad = back_inputs.reshape(own_patches, PATCH, -1).sum(axis=1).astype(jnp.bfloat16)
    back_mixed = contract(
        lax.all_gather(patch_grad, "row", axis=0, tiled=True), local_weight, 1, 1
    ).astype(jnp.bfloat16)
    grad_global_up = contract(scaled, back_mixed, 0, 0)
    back_scaled = lax.psum(contract(back_mixed, global_up, 1, 1), "row")
    grad_global_scales = task_totals(patch_tasks, back_scaled * reduced)
    back_reduced = (back_scaled * task_scales).astype(jnp.bfloat16)
    grad_global_down = contract(attended, back_reduced, 0, 0)
    grad_global_down, grad_global_up, grad_global_scales, grad_local_up = lax.psum(
        (grad_global_down, grad_global_up, grad_global_scales, grad_local_up), "seq"
    )
    grad_local_down, grad_local_scales = lax.psum(
        (grad_local_down, grad_local_scales), ("seq", "row")
    )
    return (
        grad_global_down,
        grad_global_up,
        grad_global_scales,
        grad_local_down,
        grad_local_up,
        grad_local_scales,
    )


MESH = pl.DeviceIdType.MESH
SPAN = 256


def remote(src, dst, send, recv, seq, row):
    return pltpu.make_async_remote_copy(
        src_ref=src,
        dst_ref=dst,
        send_sem=send,
        recv_sem=recv,
        device_id=(seq, row),
        device_id_type=MESH,
    )


def exact(left, right, left_dim, right_dim):
    return lax.dot_general(
        left, right, (((left_dim,), (right_dim,)), ((), ())), precision=lax.Precision.HIGHEST,
        preferred_element_type=jnp.float32,
    )


def split_pair(value):
    high = value.astype(jnp.bfloat16)
    low = (value - high.astype(jnp.float32)).astype(jnp.bfloat16)
    return high, low


def step_kernel(
    chips, depth,
    q_hbm, k_hbm, v_hbm, tasks_hbm, res_hbm, ow_hbm, gd_hbm, gu_hbm, gs_hbm, lw_hbm, ids_hbm,
    table_hbm, pos_hbm, gain_hbm, hi_hbm, ho_hbm, ld_hbm, lu_hbm, ls_hbm, cot_hbm,
    ggd_out, ggu_out, gsc_out, gld_out, glu_out, lsc_out,
    q_ref, k_ref, v_ref, tasks_ref, res_ref, ow_ref, gd_ref, gu_ref, gs_ref, lw_ref, ids_ref,
    pos_ref, gain_ref, ld_ref, ls_ref, cot_ref, wi, wo, wit,
    qb, kb, vb, ob, att, lwb, w2, acc, e1, e1r, mb, mr, bridge,
    red, redr, lif, emb, inp, nrm, inv, low, sca, bl, gr, mv, bp, bpr, cross, crossr,
    early, early_in, early_full, late, late_in, late_full,
    in_sem, a_send, a_recv, f_send, f_recv, o_send, o_recv, z_send, z_recv, x_send, x_recv,
    p_send, p_recv, c_send, c_recv, y_send, y_recv, e_send, e_recv, b_send, b_recv,
    r_send, r_recv, g_send, g_recv,
):
    bf, f32 = jnp.bfloat16, jnp.float32
    count = 2 * chips
    owners = chips // 2
    share_of = count // owners
    me = lax.axis_index("seq")
    row = lax.axis_index("row")
    other = 1 - row
    chip, core = me // 2, lax.rem(me, 2)
    mate = 2 * chip + (1 - core)
    rows, width = q_hbm.shape
    half = width // 2
    columns = lw_hbm.shape[1]
    rank = gu_hbm.shape[0]
    wide = columns + HEAD
    shard = hi_hbm.shape[0]
    vocab = table_hbm.shape[0]
    total = rows * PATCH
    pieces = total // SPAN
    per_piece = SPAN // PATCH
    tiles = width // HEAD + columns // HEAD + 1

    def heads_of(number):
        return pl.ds(pl.multiple_of(number * HEAD, HEAD), HEAD)

    def shard_of(slot):
        return pl.ds(pl.multiple_of(slot * shard, shard), shard)

    barrier = pltpu.get_barrier_semaphore()
    peers = [(lax.rem(me + d, count), row) for d in range(1, count)] + [(me, other)]
    for seq, line in peers:
        pl.semaphore_signal(barrier, inc=1, device_id=(seq, line), device_id_type=MESH)

    loads = {}

    def load(name, src, dst):
        copy = pltpu.make_async_copy(src, dst, in_sem.at[len(loads)])
        copy.start()
        loads[name] = copy

    load("ho", ho_hbm, wo.at[shard_of(me)])
    load("hi", hi_hbm, wi.at[shard_of(me)])
    load("k", k_hbm, k_ref)
    load("v", v_hbm, v_ref)
    load("q", q_hbm, q_ref)
    load("lw", lw_hbm, lw_ref)
    load("cot", cot_hbm, cot_ref.at[row])
    load("gu", gu_hbm, gu_ref)
    load("ow", ow_hbm, ow_ref)
    load("res", res_hbm, res_ref)
    load("gd", gd_hbm, gd_ref)
    load("lu", lu_hbm, wi.at[pl.ds(columns, rank)])
    load("ld", ld_hbm, ld_ref.at[pl.ds(0, rank)])
    load("table", table_hbm, emb.at[pl.ds(0, vocab), pl.ds(0, columns)])
    load("tasks", tasks_hbm, tasks_ref)
    load("ids", ids_hbm, ids_ref)
    load("pos", pos_hbm, pos_ref)
    load("gain", gain_hbm, gain_ref)
    load("gs", gs_hbm, gs_ref)
    load("ls", ls_hbm, ls_ref)

    ld_ref[rank:] = jnp.zeros((HEAD - rank, columns), bf)
    wi[columns + rank :] = jnp.zeros((HEAD - rank, width), bf)
    emb[vocab : vocab + rows, :columns] = jnp.zeros((rows, columns), bf)
    emb[:vocab, columns:] = jnp.zeros((vocab, 2 * HEAD), bf)
    emb[vocab + HEAD :] = jnp.zeros((HEAD, wide + HEAD), bf)

    pl.semaphore_wait(barrier, len(peers))

    own = heads_of(chip)
    near = chips // 2
    place_in = lax.rem(chip, near)
    home = chip - place_in
    away = near - home
    own_half = pl.ds(pl.multiple_of(core * half, half), half)

    def hand(which, to):
        src, dst = (
            (k_ref, kb.at[me]), (v_ref, vb.at[me]), (q_ref, qb.at[chip])
        )[which]
        return remote(
            src.at[:, heads_of(to)], dst, a_send.at[which, to], a_recv.at[which, chip],
            2 * to + core, row,
        )

    def landed(which, source):
        dst = (kb.at[2 * source + core], vb.at[2 * source + core], qb.at[source])[which]
        remote(
            dst, dst, a_send.at[which, source], a_recv.at[which, source], me, row
        ).wait_recv()

    targets = [away + lax.rem(place_in + j, near) for j in range(near)] + [
        home + lax.rem(place_in + j, near) for j in range(1, near)
    ]
    levels = chips // depth
    level, side = chip // depth, lax.rem(chip, depth)
    weights_in = ((1, wo), (0, wi))
    neighbour = 2 * (level * depth + (1 - side)) + core

    def slot_of(number, line):
        return 2 * (number * depth + line) + core

    def move(which, slot, sends, recvs, to):
        buffer = wo if which else wi
        piece = buffer.at[shard_of(slot)]
        return remote(piece, piece, sends, recvs, to, row)

    def pass_along(which, source):
        slot = slot_of(source, side)
        for way, step in ((0, 1), (1, -1)):
            ahead = level + step
            fits = (ahead >= 0) & (ahead < levels) & ((source - level) * step <= 0)

            @pl.when(fits)
            def _():
                move(
                    which, slot, z_send.at[which, source, way], z_recv.at[which, source],
                    slot_of(ahead, side),
                ).start()

    def settle_along(which, source):
        slot = slot_of(source, side)
        for way, step in ((0, 1), (1, -1)):
            ahead = level + step
            fits = (ahead >= 0) & (ahead < levels) & ((source - level) * step <= 0)

            @pl.when(fits)
            def _():
                move(
                    which, slot, z_send.at[which, source, way], z_recv.at[which, source],
                    slot_of(ahead, side),
                ).wait_send()

    def across(which, source, line):
        return move(
            which, slot_of(source, line), x_send.at[which, source], x_recv.at[which, source],
            neighbour,
        )

    def to_mate(which, source, line):
        number = jnp.where(line == side, source, levels + source)
        return move(
            which, slot_of(source, line), p_send.at[which, number], p_recv.at[which, number], mate
        )

    def relay(hop):
        for which, buffer in weights_in:
            for source in (level - hop, level + hop):

                @pl.when((source >= 0) & (source < levels))
                def _():
                    move(
                        which, slot_of(source, side), z_send.at[which, source, 0],
                        z_recv.at[which, source], me,
                    ).wait_recv()
                    pass_along(which, source)
                    across(which, source, side).start()
                    to_mate(which, source, side).start()

    def cross_over(hop):
        for which, buffer in weights_in:
            for source in {0: (level,)}.get(hop, (level - hop, level + hop)):

                @pl.when((source >= 0) & (source < levels))
                def _():
                    across(which, source, 1 - side).wait_recv()
                    to_mate(which, source, 1 - side).start()

    loads["ho"].wait()
    loads["hi"].wait()
    for which, buffer in weights_in:
        pass_along(which, level)
        across(which, level, side).start()
        to_mate(which, level, side).start()

    loads["k"].wait()
    loads["v"].wait()
    loads["q"].wait()


    def share(which, source):
        buffer = (kb, vb)[which]
        slot = 2 * source + core
        return remote(
            buffer.at[slot], buffer.at[slot], f_send.at[which, source], f_recv.at[which, source],
            mate, row,
        )

    kb[me] = k_ref[:, own]
    vb[me] = v_ref[:, own]
    qb[chip] = q_ref[:, own]
    for to in targets:
        for which in range(2):
            hand(which, to).start()
    for which, src in enumerate((k_ref, v_ref)):
        remote(
            src.at[:, own], (kb, vb)[which].at[me], f_send.at[which, chip],
            f_recv.at[which, chip], mate, row,
        ).start()
    loads["lw"].wait()
    lw_copy = remote(lw_ref.at[own_half], lwb.at[own_half], y_send.at[0], y_recv.at[0], me, other)
    lw_copy.start()
    loads["cot"].wait()
    cot_copy = remote(
        cot_ref.at[row], cot_ref.at[row], c_send.at[0], c_recv.at[0], me, other
    )
    cot_copy.start()

    loads["gu"].wait()
    mb[...] = jnp.dot(gu_ref[...], lw_ref[...], preferred_element_type=f32).astype(bf)
    m_copy = remote(mb, mr, y_send.at[2], y_recv.at[2], me, other)
    m_copy.start()

    tile = math.gcd(width, SPAN)
    loads["ow"].wait()

    @pl.loop(0, width // tile)
    def _(index):
        block = pl.ds(pl.multiple_of(index * tile, tile), tile)
        acc[block] = jnp.dot(
            ow_ref[block, pl.ds(pl.multiple_of(row * width, width), width)],
            lw_ref[...],
            preferred_element_type=f32,
        )

    relay(1)
    for to in targets:
        hand(2, to).start()
    cross_over(0)
    for j in range(1, near):
        source = home + lax.rem(place_in + near - j, near)
        for which in range(2):
            landed(which, source)
            share(which, source).start()
    for j in range(near):
        source = away + lax.rem(place_in + near - j, near)
        for which in range(2):
            landed(which, source)
            share(which, source).start()
    for source in range(chips):
        for which in range(2):
            buffer = (kb, vb)[which]
            slot = 2 * source + 1 - core
            remote(
                buffer.at[slot], buffer.at[slot], f_send.at[which, source],
                f_recv.at[which, source], mate, row,
            ).wait_recv()

    lw_copy.wait_recv()
    lw_mate = remote(lwb.at[own_half], lwb.at[own_half], y_send.at[1], y_recv.at[1], mate, row)
    lw_mate.start()
    factor = 1.0 / math.sqrt(HEAD) / math.log(2.0)
    span = chips * rows

    def attend(pair, late_half):
        query = jnp.concatenate([qb[i] for i in pair], axis=0)
        start = chips if late_half else 0
        fresh = contract(query, kb[start : start + chips].reshape(span, HEAD), 1, 1)
        places = lax.broadcasted_iota(jnp.int32, (2 * rows, span), 1)
        queries = lax.broadcasted_iota(jnp.int32, (2 * rows, span), 0)
        first, second = [(2 * i + core - start) * rows for i in pair]
        queries = queries + jnp.where(queries < rows, first, second - rows)
        fresh = jnp.where(places <= queries, fresh, -1e30)
        top = jnp.max(fresh, axis=1, keepdims=True)
        if late_half:
            scores = contract(query, kb[:start].reshape(span, HEAD), 1, 1)
            top = jnp.maximum(top, jnp.max(scores, axis=1, keepdims=True))
        weights = jnp.exp2((fresh - top) * factor)
        mass = jnp.sum(weights, axis=1, keepdims=True)
        mixed = jnp.dot(
            weights.astype(bf), vb[start : start + chips].reshape(span, HEAD),
            preferred_element_type=f32,
        )
        if late_half:
            weights = jnp.exp2((scores - top) * factor)
            mass = mass + jnp.sum(weights, axis=1, keepdims=True)
            mixed = mixed + jnp.dot(
                weights.astype(bf), vb[:start].reshape(span, HEAD), preferred_element_type=f32
            )
        mixed = (mixed / mass).astype(bf)
        for number, i in enumerate(pair):
            ob[i] = mixed[number * rows : (number + 1) * rows]

    @pl.loop(0, near)
    def _(step):
        @pl.when(step == 1)
        def _():
            relay(2)
            cross_over(1)

        at_home = step < near // 2
        stages = (
            jnp.where(at_home, 2 * step + 1, 2 * step - near),
            jnp.where(at_home, lax.rem(2 * step + 2, near), 2 * step - near + 1),
        )
        pair = [
            jnp.where(at_home, home, away) + lax.rem(place_in + near - stage, near)
            for stage in stages
        ]
        for i in pair:

            @pl.when(i != chip)
            def _():
                landed(2, i)

        @pl.when(pair[0] < near)
        def _():
            attend(pair, False)

        @pl.when(pair[0] >= near)
        def _():
            attend(pair, True)

        for i in pair:

            @pl.when(i != chip)
            def _():
                remote(
                    ob.at[i], att.at[:, own], o_send.at[i], o_recv.at[chip], 2 * i + core, row
                ).start()

    att[:, own] = ob[chip]

    lw_mate.wait_recv()
    @pl.loop(0, width // tile)
    def _(index):
        block = pl.ds(pl.multiple_of(index * tile, tile), tile)
        summed = acc[block] + jnp.dot(
            ow_ref[block, pl.ds(pl.multiple_of(other * width, width), width)],
            lwb[...],
            preferred_element_type=f32,
        )
        w2[block] = summed.astype(bf)

    for name in ("res", "gd", "lu", "ld", "table", "tasks", "ids", "pos", "gain", "gs", "ls"):
        loads[name].wait()
    picks = (
        lax.broadcasted_iota(jnp.int32, (TASKS, rows), 0) == tasks_ref[...]
    ).astype(f32)

    def widen(table):
        return jnp.concatenate([table, jnp.zeros((TASKS, HEAD - rank), f32)], axis=1)

    task_scales = exact(gs_ref[...], picks, 0, 0)
    high, low_part = split_pair(exact(picks, widen(ls_ref[...]), 0, 0))
    emb[vocab : vocab + rows, columns:wide] = high
    emb[vocab : vocab + rows, wide:] = low_part
    emb[vocab + rows : vocab + rows + 2 * PATCH, :columns] = jnp.concatenate(
        [pos_ref[...].astype(f32), jnp.zeros((PATCH, columns), f32)], axis=0
    ).astype(bf)
    direct = jnp.dot(res_ref[...], lw_ref[...], preferred_element_type=f32)
    inp[:rows] = direct

    cot_copy.wait_recv()
    m_copy.wait_recv()
    bridge[...] = (mb[...].astype(f32) + mr[...].astype(f32)).astype(bf)
    belongs = (
        lax.broadcasted_iota(jnp.int32, (rows, total), 1) // PATCH
        == lax.broadcasted_iota(jnp.int32, (rows, total), 0)
    ).astype(f32).astype(bf)
    own_bytes = total // 2
    cot_sum = sum(
        jnp.dot(
            belongs[:, index * own_bytes : (index + 1) * own_bytes], cot_ref[index],
            preferred_element_type=f32,
        )
        for index in range(2)
    )

    for hop in range(3, levels):
        relay(hop)
    for hop in range(2, levels - 1):
        cross_over(hop)
    for i in range(chips):

        @pl.when(i != chip)
        def _():
            back = remote(
                ob.at[i], att.at[:, heads_of(i)], o_send.at[i], o_recv.at[i], 2 * i + core, row
            )
            back.wait_recv()
            back.wait_send()

    e_copies = []
    red[...] = contract(gd_ref[...], att[...], 1, 1).astype(bf)
    red_copy = remote(red, redr, y_send.at[3], y_recv.at[3], me, other)
    red_copy.start()
    e1[...] = (
        jnp.dot(att[...], w2[...], preferred_element_type=f32) + inp[:rows]
    ).astype(bf)
    for index in range(pieces):
        patches = pl.ds(index * per_piece, per_piece)
        copy = remote(e1.at[patches], e1r.at[patches], e_send.at[index], e_recv.at[index], me, other)
        copy.start()
        e_copies.append(copy)
    red_copy.wait_recv()
    reduced = red[...].astype(f32) + redr[...].astype(f32)
    scaled = (reduced * task_scales).astype(bf)
    lifted = contract(scaled, bridge[...], 0, 0)

    depth_all = emb.shape[0]
    lif[...] = lifted

    @pl.loop(0, pieces)
    def _(index):
        block = pl.ds(pl.multiple_of(index * SPAN, SPAN), SPAN)
        patches = pl.ds(pl.multiple_of(index * per_piece, per_piece), per_piece)
        remote(
            e1.at[patches], e1r.at[patches], e_send.at[index], e_recv.at[index], me, other
        ).wait_recv()
        emb[pl.ds(pl.multiple_of(vocab + index * per_piece, per_piece), per_piece), :columns] = (
            e1[patches].astype(f32) + e1r[patches].astype(f32) + lif[patches]
        ).astype(bf)

        @pl.when(index == pieces // 2)
        def _():
            cross_over(levels - 1)

        line = lax.broadcasted_iota(jnp.int32, (depth_all, SPAN), 0)
        byte = lax.broadcasted_iota(jnp.int32, (depth_all, SPAN), 1) + index * SPAN
        chosen = (
            (line == ids_ref[:, block])
            | (line == vocab + byte // PATCH)
            | (line == vocab + rows + lax.rem(byte, PATCH))
        )
        found = contract(jnp.where(chosen, 1.0, 0.0).astype(bf), emb[...], 0, 0)
        inputs = found[:, :columns]
        scales = found[:, columns:wide] + found[:, wide:]
        inverse = lax.rsqrt(jnp.mean(inputs * inputs, axis=1, keepdims=True) + 1e-06)
        normed = (inputs * inverse * gain_ref[...]).astype(bf)
        lowered = contract(normed, ld_ref[...], 1, 1)
        inp[block] = inputs
        inv[block] = jnp.broadcast_to(inverse, (SPAN, HEAD))
        sca[block] = scales
        low[block] = lowered
        nrm[block, :columns] = normed
        nrm[block, columns:] = (lowered * scales).astype(bf)

    def mates_weights(which):
        for source in range(levels):
            for line in (side, 1 - side):
                to_mate(which, source, line).wait_recv()

    mates_weights(1)
    mates_weights(0)
    wit[...] = jnp.transpose(wi[...])
    @pl.loop(0, pieces)
    def _(index):
        block = pl.ds(pl.multiple_of(index * SPAN, SPAN), SPAN)
        upper = jnp.dot(nrm[block], wi[...], preferred_element_type=f32)
        inner = pl.ds(pl.multiple_of(lax.rem(index * SPAN, own_bytes), SPAN), SPAN)
        through = jnp.dot(
            cot_ref[index * SPAN // own_bytes, inner], wo[...], preferred_element_type=f32
        )
        grown = (through * gelu_slope(upper)).astype(bf)
        gr[block] = grown
        both = jnp.dot(grown, wit[...], preferred_element_type=f32)
        back_rank = both[:, columns:]
        moved = (back_rank * sca[block]).astype(bf)
        mv[block] = moved
        bl[block] = back_rank * low[block]
        back_total = both[:, :columns] + jnp.dot(
            moved, ld_ref[...], preferred_element_type=f32
        )
        inputs = inp[block]
        inverse = inv[block][:, :1]
        gained = back_total * gain_ref[...]
        average = jnp.mean(gained * inputs, axis=1, keepdims=True)
        back_inputs = inverse * (gained - inputs * (inverse * inverse * average))
        near = (
            lax.broadcasted_iota(jnp.int32, (per_piece, SPAN), 1) // PATCH
            == lax.broadcasted_iota(jnp.int32, (per_piece, SPAN), 0)
        ).astype(f32).astype(bf)
        patches = pl.ds(pl.multiple_of(index * per_piece, per_piece), per_piece)
        bp[patches] = jnp.dot(
            near, back_inputs.astype(bf), preferred_element_type=f32
        ).astype(bf)
        remote(
            bp.at[patches], bpr.at[patches], b_send.at[index], b_recv.at[index], me, other
        ).start()

    down = contract(mv[...], nrm[:, :columns], 0, 0)[:rank]
    high, low_part = split_pair(bl[...])
    by_patch = jnp.dot(belongs, high, preferred_element_type=f32) + jnp.dot(
        belongs, low_part, preferred_element_type=f32
    )
    small = exact(picks, by_patch, 1, 0)
    small = jnp.concatenate([small, jnp.zeros_like(small)], axis=0)
    down = down.astype(bf)
    lift = contract(nrm[:, columns:], gr[...], 0, 0)[:rank].astype(bf)
    spread = width // HEAD
    thin = columns // HEAD
    for t in range(spread):
        early[t] = lift[:, t * HEAD : (t + 1) * HEAD]
    for t in range(thin):
        early[spread + t] = down[:, t * HEAD : (t + 1) * HEAD]
    early[spread + thin] = small.astype(bf)
    base = chips // 4

    def owner(t):
        return 2 * (base + t) + 1

    def held(t):
        return pl.ds(0, min(share_of, tiles - t * share_of))

    def parcel(kind, t):
        source, landing = (early, late)[kind], (early_in, late_in)[kind]
        size = min(share_of, tiles - t * share_of)
        return remote(
            source.at[pl.ds(share_of * t, size)], landing.at[me, held(t)], r_send.at[kind, t],
            r_recv.at[kind, me], owner(t), row,
        )

    def spread_out(kind):
        for t in range(owners):

            @pl.when(owner(t) != me)
            def _():
                parcel(kind, t).start()

            @pl.when(owner(t) == me)
            def _():
                size = min(share_of, tiles - t * share_of)
                source, landing = (early, late)[kind], (early_in, late_in)[kind]
                landing[me, :size] = source[share_of * t : share_of * t + size]

    def settle_out(kind):
        for t in range(owners):

            @pl.when(owner(t) != me)
            def _():
                parcel(kind, t).wait_send()

    def gather_in(kind, final):
        landing = (early_in, late_in)[kind]
        for t in range(owners):

            @pl.when(owner(t) == me)
            def _():
                size = min(share_of, tiles - t * share_of)
                for d in range(1, count):
                    source = lax.rem(me + d, count)
                    remote(
                        landing.at[source, held(t)], landing.at[source, held(t)],
                        r_send.at[kind, 0], r_recv.at[kind, source], me, row,
                    ).wait_recv()
                summed = jnp.sum(landing[:, :size].astype(f32), axis=0)
                if kind == 0 and t * share_of >= spread:
                    cross[:size] = summed.astype(bf)
                    swap = remote(
                        cross.at[held(t)], crossr.at[held(t)], y_send.at[4], y_recv.at[4], me, other
                    )
                    swap.start()
                    swap.wait_recv()
                    summed = cross[:size].astype(f32) + crossr[:size].astype(f32)
                final[t, :size] = summed.astype(bf)
                for d in range(1, count):
                    issue(kind, final, t, d).start()

    def issue(kind, final, t, d):
        piece = final.at[t, held(t)]
        return remote(
            piece, piece, g_send.at[kind, d], g_recv.at[kind, t], lax.rem(me + d, count), row
        )

    def finish_in(kind, final):
        for t in range(owners):

            @pl.when(owner(t) != me)
            def _():
                piece = final.at[t, held(t)]
                remote(
                    piece, piece, g_send.at[kind, 0], g_recv.at[kind, t], me, row
                ).wait_recv()

    def settle_in(kind, final):
        for t in range(owners):

            @pl.when(owner(t) == me)
            def _():
                for d in range(1, count):
                    issue(kind, final, t, d).wait_send()
                if kind == 0 and t * share_of >= spread:
                    remote(
                        cross.at[held(t)], crossr.at[held(t)], y_send.at[4], y_recv.at[4], me, other
                    ).wait_send()

    spread_out(0)

    for index in range(pieces):
        patches = pl.ds(index * per_piece, per_piece)
        remote(
            bp.at[patches], bpr.at[patches], b_send.at[index], b_recv.at[index], me, other
        ).wait()
    patch_grad = (bp[...].astype(f32) + bpr[...].astype(f32) + cot_sum).astype(bf)
    pulled = jnp.dot(scaled, patch_grad, preferred_element_type=f32).astype(bf)
    back_scaled = contract(bridge[...], patch_grad, 1, 1)
    back_reduced = (back_scaled * task_scales).astype(bf)
    outward = jnp.dot(back_reduced, att[...], preferred_element_type=f32).astype(bf)
    product = back_scaled * reduced
    product = jnp.concatenate([product, jnp.zeros((HEAD - rank, rows), f32)], axis=0)
    tops = exact(picks, product, 1, 1)
    tops = jnp.concatenate([tops, jnp.zeros_like(tops)], axis=0)
    for t in range(spread):
        late[t] = outward[:, t * HEAD : (t + 1) * HEAD]
    for t in range(thin):
        late[spread + t] = pulled[:, t * HEAD : (t + 1) * HEAD]
    late[spread + thin] = tops.astype(bf)
    spread_out(1)
    gather_in(0, early_full)
    gather_in(1, late_full)
    finish_in(0, early_full)

    def tile_of(final, t):
        return final[t // share_of, t % share_of]

    for t in range(spread):
        glu_out[:, t * HEAD : (t + 1) * HEAD] = tile_of(early_full, t).astype(f32)
    for t in range(thin):
        gld_out[:, t * HEAD : (t + 1) * HEAD] = tile_of(early_full, spread + t).astype(f32)
    lsc_out[...] = tile_of(early_full, spread + thin)[:TASKS, :rank].astype(f32)
    finish_in(1, late_full)
    for t in range(spread):
        ggd_out[:, t * HEAD : (t + 1) * HEAD] = tile_of(late_full, t).astype(f32)
    for t in range(thin):
        bridge[:, t * HEAD : (t + 1) * HEAD] = tile_of(late_full, spread + t)
    ggu_out[...] = contract(bridge[...], lw_ref[...], 1, 1)
    gsc_out[...] = tile_of(late_full, spread + thin)[:TASKS, :rank].astype(f32)
    for kind, final in ((0, early_full), (1, late_full)):
        settle_out(kind)
        settle_in(kind, final)
    for which, buffer in weights_in:
        for source in range(levels):
            settle_along(which, source)
            across(which, source, side).wait_send()
            for line in (side, 1 - side):
                to_mate(which, source, line).wait_send()
    for to in targets:
        for which in range(3):
            hand(which, to).wait_send()
    for source in range(chips):
        for which in range(2):
            share(which, source).wait_send()
    for copy in [lw_copy, lw_mate, cot_copy, m_copy, red_copy] + e_copies:
        copy.wait_send()


def copy_kernel(*refs):
    number = len(refs) // 2
    for source, target in zip(refs[:number], refs[number:]):
        target[...] = source[...]


def paired_body(
    patch_queries, patch_keys, patch_values, patch_tasks, residual, output_weight, global_down,
    global_up, global_scales, local_weight, byte_ids, byte_table, position_table, norm_gain,
    hidden_in, hidden_out, local_down, local_up, local_scales, cotangent,
):
    count = lax.axis_size("seq")
    rows, width = patch_queries.shape
    chips = count // 2
    depth = 2
    levels = chips // depth
    columns = local_weight.shape[1]
    rank = global_up.shape[0]
    vocab = byte_table.shape[0]
    total = byte_ids.shape[0]
    wide = columns + HEAD
    pieces = total // SPAN
    bf, f32 = jnp.bfloat16, jnp.float32
    vm = pltpu.VMEM
    dma = pltpu.SemaphoreType.DMA
    args = (
        patch_queries, patch_keys, patch_values, patch_tasks.reshape(1, rows), residual,
        output_weight, jnp.transpose(global_down), global_up, global_scales, local_weight,
        byte_ids.reshape(1, total), byte_table, position_table, norm_gain.reshape(1, columns),
        jnp.transpose(hidden_in), jnp.transpose(hidden_out), jnp.transpose(local_down), local_up,
        local_scales, cotangent,
    )
    outs = pl.pallas_call(
        functools.partial(step_kernel, chips, depth),
        out_shape=(
            jax.ShapeDtypeStruct((rank, width), f32),
            jax.ShapeDtypeStruct((rank, width), f32),
            jax.ShapeDtypeStruct((TASKS, rank), f32),
            jax.ShapeDtypeStruct((rank, columns), f32),
            jax.ShapeDtypeStruct((rank, width), f32),
            jax.ShapeDtypeStruct((TASKS, rank), f32),
        ),
        in_specs=[pl.BlockSpec(memory_space=pl.ANY)] * len(args),
        out_specs=(pl.BlockSpec(memory_space=vm),) * 6,
        scratch_shapes=[
            vm((rows, width), bf), vm((rows, width), bf), vm((rows, width), bf),
            vm((1, rows), jnp.int32), vm((rows, width), bf), vm(output_weight.shape, bf),
            vm((rank, width), bf), vm((rank, width), bf), vm((TASKS, rank), f32),
            vm((width, columns), bf), vm((1, total), jnp.int32), vm((PATCH, columns), bf),
            vm((1, columns), f32), vm((HEAD, columns), bf), vm((TASKS, rank), f32),
            vm((2, total // 2, columns), bf), vm((wide, width), bf), vm((columns, width), bf),
            vm((width, wide), bf),
            vm((chips, rows, HEAD), bf), vm((count, rows, HEAD), bf), vm((count, rows, HEAD), bf),
            vm((chips, rows, HEAD), bf), vm((rows, width), bf), vm((width, columns), bf),
            vm((width, columns), bf), vm((width, columns), f32), vm((rows, columns), bf),
            vm((rows, columns), bf), vm((rank, columns), bf), vm((rank, columns), bf),
            vm((rank, columns), bf), vm((rank, rows), bf), vm((rank, rows), bf),
            vm((rows, columns), f32),
            vm((vocab + 2 * HEAD, wide + HEAD), bf), vm((total, columns), f32),
            vm((total, wide), bf), vm((total, HEAD), f32), vm((total, HEAD), f32),
            vm((total, HEAD), f32), vm((total, HEAD), f32), vm((total, width), bf),
            vm((total, HEAD), bf), vm((rows, columns), bf), vm((rows, columns), bf),
            vm((4, rank, HEAD), bf), vm((4, rank, HEAD), bf),
        ]
        + [
            vm((count, rank, HEAD), bf), vm((count, 4, rank, HEAD), bf),
            vm((chips // 2, 4, rank, HEAD), bf),
        ]
        * 2
        + [
            dma((len(args),)), dma((3, chips)), dma((3, chips)), dma((2, chips)), dma((2, chips)),
            dma((chips,)), dma((chips,)), dma((2, levels, 2)), dma((2, levels)), dma((2, levels)),
            dma((2, levels)), dma((2, chips)), dma((2, chips)), dma((1,)), dma((1,)), dma((5,)),
            dma((5,)), dma((pieces,)), dma((pieces,)), dma((pieces,)), dma((pieces,)),
            dma((2, chips)), dma((2, count)), dma((2, count)), dma((2, chips)),
        ],
        compiler_params=pltpu.CompilerParams(
            collective_id=0, has_side_effects=True, vmem_limit_bytes=60 * 1024 * 1024
        ),
        name="step",
    )(*args)
    ggd, ggu, gsc, gld, glu, lsc = pl.pallas_call(
        copy_kernel,
        out_shape=tuple(jax.ShapeDtypeStruct(item.shape, item.dtype) for item in outs),
        in_specs=[pl.BlockSpec(memory_space=vm)] * len(outs),
        out_specs=(pl.BlockSpec(memory_space=vm),) * len(outs),
        name="spill",
    )(*outs)
    return (jnp.transpose(ggd), ggu, gsc, jnp.transpose(gld), glu, lsc)


def pick_body(seq_count, row_count, *args):
    heads = args[0].shape[1] // HEAD
    rank = args[7].shape[0]
    hidden = args[14].shape[0]
    fits = (
        row_count == 2
        and seq_count == 2 * heads
        and heads % 4 == 0
        and rank == 2 * TASKS
        and args[0].shape[1] == hidden
        and (4 * rank * hidden) % (seq_count * 16 * HEAD) == 0
        and hidden // HEAD + args[9].shape[1] // HEAD < seq_count
        and args[0].shape[0] == HEAD
    )
    return paired_body(*args) if fits else general_body(*args)


def solution(mesh):
    placed = (
        P("seq", "row"),
        P("seq", "row"),
        P("seq", "row"),
        P("seq"),
        P("seq", "row"),
        P("row", None),
        P("row", None),
        P(None, "row"),
        P(),
        P("row", None),
        P("seq"),
        P(),
        P(),
        P(),
        P("row", "seq"),
        P("row", "seq"),
        P(),
        P(None, "row"),
        P(),
        P(("seq", "row"), None),
    )
    chosen = functools.partial(pick_body, mesh.shape["seq"], mesh.shape["row"])
    return jax.shard_map(
        chosen,
        mesh=mesh,
        in_specs=placed,
        out_specs=(P("row", None), P(None, "row"), P(), P(), P(None, "row"), P()),
        check_vma=False,
    )
```

```python
import functools
import math

import jax
import jax.numpy as jnp
from jax import lax
from jax.experimental import pallas as pl
from jax.experimental.pallas import tpu as pltpu
from jax.sharding import PartitionSpec as P

HEAD = 128
VOCAB = 256
PATCH = 8
TASKS = 8


def contract(left, right, left_dim, right_dim):
    return lax.dot_general(
        left, right, (((left_dim,), (right_dim,)), ((), ())), preferred_element_type=jnp.float32
    )


def select_rows(table, tasks):
    picks = (tasks[:, None] == jnp.arange(table.shape[0], dtype=jnp.int32)[None, :]).astype(
        jnp.float32
    )
    return jnp.dot(picks, table, precision=lax.Precision.HIGHEST)


def task_totals(tasks, values):
    picks = (tasks[:, None] == jnp.arange(TASKS, dtype=jnp.int32)[None, :]).astype(jnp.float32)
    return lax.dot_general(picks, values, (((0,), (0,)), ((), ())), precision=lax.Precision.HIGHEST)


def gelu_slope(upper):
    cumulative = 0.5 * (1.0 + lax.erf(upper * 0.7071067811865476))
    density = jnp.exp(-0.5 * upper * upper) * 0.3989422804014327
    return cumulative + upper * density


def local_inputs(
    identities, projected, tasks, byte_table, position_table, norm_gain, local_down, local_scales
):
    count = identities.shape[0]
    picks = (identities[:, None] == jnp.arange(VOCAB, dtype=jnp.int32)[None, :]).astype(
        jnp.bfloat16
    )
    embedded = jnp.dot(picks, byte_table, preferred_element_type=jnp.float32)
    patches = count // PATCH
    inputs = (
        embedded.reshape(patches, PATCH, -1)
        + position_table.astype(jnp.float32)[None]
        + projected.astype(jnp.float32)[:, None, :]
    )
    inputs = inputs.reshape(count, -1)
    inverse = lax.rsqrt(jnp.mean(inputs * inputs, axis=1, keepdims=True) + 1e-06)
    normed = (inputs * inverse * norm_gain).astype(jnp.bfloat16)
    lowered = jnp.dot(normed, local_down, preferred_element_type=jnp.float32)
    byte_tasks = jnp.repeat(tasks, PATCH)
    scales = select_rows(local_scales, byte_tasks)
    shrunk = (lowered * scales).astype(jnp.bfloat16)
    return (inputs, inverse, normed, lowered, scales, shrunk, byte_tasks)


def keep_state(current):
    return current


def update_state(state, query_rows, first, key_heads, value_heads, key_places, scale):
    running_max, running_sum, running_out = state
    count = query_rows.shape[0]
    heads = key_heads.shape[1]
    query_heads = query_rows.reshape(count, heads, HEAD)
    scores = (
        jnp.einsum("qhd,khd->hqk", query_heads, key_heads, preferred_element_type=jnp.float32)
        * scale
    )
    query_places = first + jnp.arange(count, dtype=jnp.int32)
    allowed = key_places[None, :] <= query_places[:, None]
    scores = jnp.where(allowed[None], scores, -1e30)
    new_max = jnp.maximum(running_max, jnp.max(scores, axis=2))
    weights = jnp.where(allowed[None], jnp.exp(scores - new_max[:, :, None]), 0.0)
    shrink = jnp.exp(running_max - new_max)
    running_sum = running_sum * shrink + jnp.sum(weights, axis=2)
    mixed = jnp.einsum(
        "hqk,khd->qhd",
        weights.astype(jnp.bfloat16),
        value_heads,
        preferred_element_type=jnp.float32,
    )
    running_out = running_out * jnp.transpose(shrink)[:, :, None] + mixed
    return (new_max, running_sum, running_out)


def finish_state(state):
    running_max, running_sum, running_out = state
    result = running_out / jnp.transpose(running_sum)[:, :, None]
    return result.reshape(result.shape[0], -1).astype(jnp.bfloat16)


def general_body(
    patch_queries,
    patch_keys,
    patch_values,
    patch_tasks,
    residual,
    output_weight,
    global_down,
    global_up,
    global_scales,
    local_weight,
    byte_ids,
    byte_table,
    position_table,
    norm_gain,
    hidden_in,
    hidden_out,
    local_down,
    local_up,
    local_scales,
    cotangent,
):
    rows = patch_queries.shape[0]
    width = patch_queries.shape[1]
    heads = width // HEAD
    row_count = lax.axis_size("row")
    seq_index = lax.axis_index("seq")
    row_index = lax.axis_index("row")
    scale = 1.0 / math.sqrt(HEAD)
    own_first = seq_index * rows
    groups = [(patch_queries, own_first)]

    def visit(state, query_rows, first, key_heads, value_heads, key_places):

        def refresh(current):
            return update_state(
                current, query_rows, first, key_heads, value_heads, key_places, scale
            )

        return lax.cond(
            key_places[0] <= first + query_rows.shape[0] - 1, refresh, keep_state, state
        )

    initial = tuple(
        (
            (
                jnp.full((heads, query_rows.shape[0]), -1e30, jnp.float32),
                jnp.zeros((heads, query_rows.shape[0]), jnp.float32),
                jnp.zeros((query_rows.shape[0], heads, HEAD), jnp.float32),
            )
            for query_rows, first in groups
        )
    )
    key_piece = lax.all_gather(patch_keys, "seq", axis=0, tiled=True)
    value_piece = lax.all_gather(patch_values, "seq", axis=0, tiled=True)
    count = key_piece.shape[0]
    span = math.gcd(count, 1024)

    def one_span(index, states):
        offset = index * span
        key_heads = lax.dynamic_slice_in_dim(key_piece, offset, span, 0).reshape(span, heads, HEAD)
        value_heads = lax.dynamic_slice_in_dim(value_piece, offset, span, 0).reshape(
            span, heads, HEAD
        )
        key_places = offset + jnp.arange(span, dtype=jnp.int32)
        updated = []
        for (query_rows, first), state in zip(groups, states):
            updated.append(visit(state, query_rows, first, key_heads, value_heads, key_places))
        return tuple(updated)

    states = lax.fori_loop(0, count // span, one_span, initial)
    outputs = [finish_state(state) for state in states]
    attended = outputs[0]
    reduced = lax.psum(jnp.dot(attended, global_down, preferred_element_type=jnp.float32), "row")
    task_scales = select_rows(global_scales, patch_tasks)
    scaled = (reduced * task_scales).astype(jnp.bfloat16)
    mixed = lax.psum_scatter(
        contract(output_weight, attended, 0, 1).astype(jnp.bfloat16),
        "row",
        scatter_dimension=0,
        tiled=True,
    ).astype(jnp.float32)
    mixed = mixed + jnp.transpose(residual.astype(jnp.float32)) + contract(global_up, scaled, 0, 1)
    mixed_b = mixed.astype(jnp.bfloat16)
    own_patches = rows // row_count
    own_bytes = own_patches * PATCH
    rows_in, rows_out = (
        lax.all_gather(hidden_in, "seq", axis=1, tiled=True),
        lax.all_gather(hidden_out, "seq", axis=1, tiled=True),
    )
    partial_value = contract(mixed_b, local_weight, 0, 0)
    projected = lax.psum(partial_value.astype(jnp.bfloat16), "row")
    every = local_inputs(
        byte_ids,
        projected,
        patch_tasks,
        byte_table,
        position_table,
        norm_gain,
        local_down,
        local_scales,
    )
    normed_all = every[2]
    shrunk_all = every[5]
    cotangent_all = lax.all_gather(cotangent, "row", axis=0, tiled=True)
    inputs, inverse, normed, lowered, scales, shrunk, byte_tasks = [
        lax.dynamic_slice_in_dim(value, row_index * own_bytes, own_bytes, 0) for value in every
    ]
    upper = contract(normed_all, rows_in, 1, 1) + jnp.dot(
        shrunk_all, local_up, preferred_element_type=jnp.float32
    )
    through = contract(cotangent_all, rows_out, 1, 1)
    grown = (through * gelu_slope(upper)).astype(jnp.bfloat16)
    grad_local_up = contract(shrunk_all, grown, 0, 0)
    back_norm, back_rank = (
        lax.psum_scatter(
            jnp.dot(grown, rows_in, preferred_element_type=jnp.float32).astype(jnp.bfloat16),
            "row",
            scatter_dimension=0,
            tiled=True,
        ).astype(jnp.float32),
        lax.psum_scatter(
            contract(grown, local_up, 1, 1).astype(jnp.bfloat16),
            "row",
            scatter_dimension=0,
            tiled=True,
        ).astype(jnp.float32),
    )
    grad_local_scales = task_totals(byte_tasks, back_rank * lowered)
    moved = (back_rank * scales).astype(jnp.bfloat16)
    grad_local_down = contract(normed, moved, 0, 0)
    back_total = back_norm + contract(moved, local_down, 1, 1)
    gained = back_total * norm_gain
    average = jnp.mean(gained * inputs, axis=1, keepdims=True)
    back_inputs = cotangent.astype(jnp.float32) + inverse * (
        gained - inputs * inverse * inverse * average
    )
    patch_grad = back_inputs.reshape(own_patches, PATCH, -1).sum(axis=1).astype(jnp.bfloat16)
    back_mixed = contract(
        lax.all_gather(patch_grad, "row", axis=0, tiled=True), local_weight, 1, 1
    ).astype(jnp.bfloat16)
    grad_global_up = contract(scaled, back_mixed, 0, 0)
    back_scaled = lax.psum(contract(back_mixed, global_up, 1, 1), "row")
    grad_global_scales = task_totals(patch_tasks, back_scaled * reduced)
    back_reduced = (back_scaled * task_scales).astype(jnp.bfloat16)
    grad_global_down = contract(attended, back_reduced, 0, 0)
    grad_global_down, grad_global_up, grad_global_scales, grad_local_up = lax.psum(
        (grad_global_down, grad_global_up, grad_global_scales, grad_local_up), "seq"
    )
    grad_local_down, grad_local_scales = lax.psum(
        (grad_local_down, grad_local_scales), ("seq", "row")
    )
    return (
        grad_global_down,
        grad_global_up,
        grad_global_scales,
        grad_local_down,
        grad_local_up,
        grad_local_scales,
    )


MESH = pl.DeviceIdType.MESH
SPAN = 256


def remote(src, dst, send, recv, seq, row):
    return pltpu.make_async_remote_copy(
        src_ref=src,
        dst_ref=dst,
        send_sem=send,
        recv_sem=recv,
        device_id=(seq, row),
        device_id_type=MESH,
    )


def exact(left, right, left_dim, right_dim):
    return lax.dot_general(
        left, right, (((left_dim,), (right_dim,)), ((), ())), precision=lax.Precision.HIGHEST,
        preferred_element_type=jnp.float32,
    )


def split_pair(value):
    high = value.astype(jnp.bfloat16)
    low = (value - high.astype(jnp.float32)).astype(jnp.bfloat16)
    return high, low


def step_kernel(
    chips, depth,
    q_hbm, k_hbm, v_hbm, tasks_hbm, res_hbm, ow_hbm, gd_hbm, gu_hbm, gs_hbm, lw_hbm, ids_hbm,
    table_hbm, pos_hbm, gain_hbm, hi_hbm, ho_hbm, ld_hbm, lu_hbm, ls_hbm, cot_hbm,
    ggd_out, ggu_out, gsc_out, gld_out, glu_out, lsc_out,
    q_ref, k_ref, v_ref, tasks_ref, res_ref, ow_ref, gd_ref, gu_ref, gs_ref, lw_ref, ids_ref,
    pos_ref, gain_ref, ld_ref, ls_ref, cot_ref, wi, wo, wit,
    qb, kb, vb, ob, att, lwb, w2, acc, e1, e1r, mb, mr, bridge,
    red, redr, lif, emb, inp, nrm, inv, low, sca, bl, gr, mv, bp, bpr, cross, crossr,
    early, early_in, early_full, late, late_in, late_full,
    in_sem, a_send, a_recv, f_send, f_recv, o_send, o_recv, z_send, z_recv, x_send, x_recv,
    p_send, p_recv, c_send, c_recv, y_send, y_recv, e_send, e_recv, b_send, b_recv,
    r_send, r_recv, g_send, g_recv,
):
    bf, f32 = jnp.bfloat16, jnp.float32
    count = 2 * chips
    owners = chips // 2
    share_of = count // owners
    me = lax.axis_index("seq")
    row = lax.axis_index("row")
    other = 1 - row
    chip, core = me // 2, lax.rem(me, 2)
    mate = 2 * chip + (1 - core)
    rows, width = q_hbm.shape
    half = width // 2
    columns = lw_hbm.shape[1]
    rank = gu_hbm.shape[0]
    wide = columns + HEAD
    shard = hi_hbm.shape[0]
    vocab = table_hbm.shape[0]
    total = rows * PATCH
    pieces = total // SPAN
    per_piece = SPAN // PATCH
    tiles = width // HEAD + columns // HEAD + 1

    def heads_of(number):
        return pl.ds(pl.multiple_of(number * HEAD, HEAD), HEAD)

    def shard_of(slot):
        return pl.ds(pl.multiple_of(slot * shard, shard), shard)

    barrier = pltpu.get_barrier_semaphore()
    peers = [(lax.rem(me + d, count), row) for d in range(1, count)] + [(me, other)]
    for seq, line in peers:
        pl.semaphore_signal(barrier, inc=1, device_id=(seq, line), device_id_type=MESH)

    loads = {}

    def load(name, src, dst):
        copy = pltpu.make_async_copy(src, dst, in_sem.at[len(loads)])
        copy.start()
        loads[name] = copy

    load("ho", ho_hbm, wo.at[shard_of(me)])
    load("hi", hi_hbm, wi.at[shard_of(me)])
    load("k", k_hbm, k_ref)
    load("v", v_hbm, v_ref)
    load("q", q_hbm, q_ref)
    load("lw", lw_hbm, lw_ref)
    load("cot", cot_hbm, cot_ref.at[row])
    load("gu", gu_hbm, gu_ref)
    load("ow", ow_hbm, ow_ref)
    load("res", res_hbm, res_ref)
    load("gd", gd_hbm, gd_ref)
    load("lu", lu_hbm, wi.at[pl.ds(columns, rank)])
    load("ld", ld_hbm, ld_ref.at[pl.ds(0, rank)])
    load("table", table_hbm, emb.at[pl.ds(0, vocab), pl.ds(0, columns)])
    load("tasks", tasks_hbm, tasks_ref)
    load("ids", ids_hbm, ids_ref)
    load("pos", pos_hbm, pos_ref)
    load("gain", gain_hbm, gain_ref)
    load("gs", gs_hbm, gs_ref)
    load("ls", ls_hbm, ls_ref)

    ld_ref[rank:] = jnp.zeros((HEAD - rank, columns), bf)
    wi[columns + rank :] = jnp.zeros((HEAD - rank, width), bf)
    emb[vocab : vocab + rows, :columns] = jnp.zeros((rows, columns), bf)
    emb[:vocab, columns:] = jnp.zeros((vocab, 2 * HEAD), bf)
    emb[vocab + HEAD :] = jnp.zeros((HEAD, wide + HEAD), bf)

    pl.semaphore_wait(barrier, len(peers))

    own = heads_of(chip)
    near = chips // 2
    place_in = lax.rem(chip, near)
    home = chip - place_in
    away = near - home
    own_half = pl.ds(pl.multiple_of(core * half, half), half)

    def hand(which, to):
        src, dst = (
            (k_ref, kb.at[me]), (v_ref, vb.at[me]), (q_ref, qb.at[chip])
        )[which]
        return remote(
            src.at[:, heads_of(to)], dst, a_send.at[which, to], a_recv.at[which, chip],
            2 * to + core, row,
        )

    def landed(which, source):
        dst = (kb.at[2 * source + core], vb.at[2 * source + core], qb.at[source])[which]
        remote(
            dst, dst, a_send.at[which, source], a_recv.at[which, source], me, row
        ).wait_recv()

    targets = [away + lax.rem(place_in + j, near) for j in range(near)] + [
        home + lax.rem(place_in + j, near) for j in range(1, near)
    ]
    levels = chips // depth
    level, side = chip // depth, lax.rem(chip, depth)
    weights_in = ((1, wo), (0, wi))
    neighbour = 2 * (level * depth + (1 - side)) + core

    def slot_of(number, line):
        return 2 * (number * depth + line) + core

    def move(which, slot, sends, recvs, to):
        buffer = wo if which else wi
        piece = buffer.at[shard_of(slot)]
        return remote(piece, piece, sends, recvs, to, row)

    def pass_along(which, source):
        slot = slot_of(source, side)
        for way, step in ((0, 1), (1, -1)):
            ahead = level + step
            fits = (ahead >= 0) & (ahead < levels) & ((source - level) * step <= 0)

            @pl.when(fits)
            def _():
                move(
                    which, slot, z_send.at[which, source, way], z_recv.at[which, source],
                    slot_of(ahead, side),
                ).start()

    def settle_along(which, source):
        slot = slot_of(source, side)
        for way, step in ((0, 1), (1, -1)):
            ahead = level + step
            fits = (ahead >= 0) & (ahead < levels) & ((source - level) * step <= 0)

            @pl.when(fits)
            def _():
                move(
                    which, slot, z_send.at[which, source, way], z_recv.at[which, source],
                    slot_of(ahead, side),
                ).wait_send()

    def across(which, source, line):
        return move(
            which, slot_of(source, line), x_send.at[which, source], x_recv.at[which, source],
            neighbour,
        )

    def to_mate(which, source, line):
        number = jnp.where(line == side, source, levels + source)
        return move(
            which, slot_of(source, line), p_send.at[which, number], p_recv.at[which, number], mate
        )

    def relay(hop):
        for which, buffer in weights_in:
            for source in (level - hop, level + hop):

                @pl.when((source >= 0) & (source < levels))
                def _():
                    move(
                        which, slot_of(source, side), z_send.at[which, source, 0],
                        z_recv.at[which, source], me,
                    ).wait_recv()
                    pass_along(which, source)
                    across(which, source, side).start()
                    to_mate(which, source, side).start()

    def cross_over(hop):
        for which, buffer in weights_in:
            for source in {0: (level,)}.get(hop, (level - hop, level + hop)):

                @pl.when((source >= 0) & (source < levels))
                def _():
                    across(which, source, 1 - side).wait_recv()
                    to_mate(which, source, 1 - side).start()

    loads["ho"].wait()
    loads["hi"].wait()
    for which, buffer in weights_in:
        pass_along(which, level)
        across(which, level, side).start()
        to_mate(which, level, side).start()

    loads["k"].wait()
    loads["v"].wait()
    loads["q"].wait()


    def share(which, source):
        buffer = (kb, vb)[which]
        slot = 2 * source + core
        return remote(
            buffer.at[slot], buffer.at[slot], f_send.at[which, source], f_recv.at[which, source],
            mate, row,
        )

    kb[me] = k_ref[:, own]
    vb[me] = v_ref[:, own]
    qb[chip] = q_ref[:, own]
    for to in targets:
        for which in range(2):
            hand(which, to).start()
    for which, src in enumerate((k_ref, v_ref)):
        remote(
            src.at[:, own], (kb, vb)[which].at[me], f_send.at[which, chip],
            f_recv.at[which, chip], mate, row,
        ).start()
    loads["lw"].wait()
    lw_copy = remote(lw_ref.at[own_half], lwb.at[own_half], y_send.at[0], y_recv.at[0], me, other)
    lw_copy.start()
    loads["cot"].wait()
    cot_copy = remote(
        cot_ref.at[row], cot_ref.at[row], c_send.at[0], c_recv.at[0], me, other
    )
    cot_copy.start()

    loads["gu"].wait()
    mb[...] = jnp.dot(gu_ref[...], lw_ref[...], preferred_element_type=f32).astype(bf)
    m_copy = remote(mb, mr, y_send.at[2], y_recv.at[2], me, other)
    m_copy.start()

    tile = math.gcd(width, SPAN)
    loads["ow"].wait()

    @pl.loop(0, width // tile)
    def _(index):
        block = pl.ds(pl.multiple_of(index * tile, tile), tile)
        acc[block] = jnp.dot(
            ow_ref[block, pl.ds(pl.multiple_of(row * width, width), width)],
            lw_ref[...],
            preferred_element_type=f32,
        )

    relay(1)
    for to in targets:
        hand(2, to).start()
    cross_over(0)
    for name in ("res", "gd", "lu", "ld", "table", "tasks", "ids", "pos", "gain", "gs", "ls"):
        loads[name].wait()
    picks = (
        lax.broadcasted_iota(jnp.int32, (TASKS, rows), 0) == tasks_ref[...]
    ).astype(f32)

    def widen(table):
        return jnp.concatenate([table, jnp.zeros((TASKS, HEAD - rank), f32)], axis=1)

    task_scales = exact(gs_ref[...], picks, 0, 0)
    high, low_part = split_pair(exact(picks, widen(ls_ref[...]), 0, 0))
    emb[vocab : vocab + rows, columns:wide] = high
    emb[vocab : vocab + rows, wide:] = low_part
    emb[vocab + rows : vocab + rows + 2 * PATCH, :columns] = jnp.concatenate(
        [pos_ref[...].astype(f32), jnp.zeros((PATCH, columns), f32)], axis=0
    ).astype(bf)
    depth_all = emb.shape[0]

    @pl.loop(0, pieces)
    def _(index):
        block = pl.ds(pl.multiple_of(index * SPAN, SPAN), SPAN)
        line = lax.broadcasted_iota(jnp.int32, (depth_all, SPAN), 0)
        byte = lax.broadcasted_iota(jnp.int32, (depth_all, SPAN), 1) + index * SPAN
        chosen = (
            (line == ids_ref[:, block])
            | (line == vocab + byte // PATCH)
            | (line == vocab + rows + lax.rem(byte, PATCH))
        )
        found = contract(jnp.where(chosen, 1.0, 0.0).astype(bf), emb[...], 0, 0)
        inp[block] = found[:, :columns]
        sca[block] = found[:, columns:wide] + found[:, wide:]

    for j in range(1, near):
        source = home + lax.rem(place_in + near - j, near)
        for which in range(2):
            landed(which, source)
            share(which, source).start()
    for j in range(near):
        source = away + lax.rem(place_in + near - j, near)
        for which in range(2):
            landed(which, source)
            share(which, source).start()
    for source in range(chips):
        for which in range(2):
            buffer = (kb, vb)[which]
            slot = 2 * source + 1 - core
            remote(
                buffer.at[slot], buffer.at[slot], f_send.at[which, source],
                f_recv.at[which, source], mate, row,
            ).wait_recv()

    lw_copy.wait_recv()
    lw_mate = remote(lwb.at[own_half], lwb.at[own_half], y_send.at[1], y_recv.at[1], mate, row)
    lw_mate.start()
    factor = 1.0 / math.sqrt(HEAD) / math.log(2.0)
    span = chips * rows

    def attend(pair, late_half):
        query = jnp.concatenate([qb[i] for i in pair], axis=0)
        start = chips if late_half else 0
        fresh = contract(query, kb[start : start + chips].reshape(span, HEAD), 1, 1)
        places = lax.broadcasted_iota(jnp.int32, (2 * rows, span), 1)
        queries = lax.broadcasted_iota(jnp.int32, (2 * rows, span), 0)
        first, second = [(2 * i + core - start) * rows for i in pair]
        queries = queries + jnp.where(queries < rows, first, second - rows)
        fresh = jnp.where(places <= queries, fresh, -1e30)
        top = jnp.max(fresh, axis=1, keepdims=True)
        if late_half:
            scores = contract(query, kb[:start].reshape(span, HEAD), 1, 1)
            top = jnp.maximum(top, jnp.max(scores, axis=1, keepdims=True))
        weights = jnp.exp2((fresh - top) * factor)
        mass = jnp.sum(weights, axis=1, keepdims=True)
        mixed = jnp.dot(
            weights.astype(bf), vb[start : start + chips].reshape(span, HEAD),
            preferred_element_type=f32,
        )
        if late_half:
            weights = jnp.exp2((scores - top) * factor)
            mass = mass + jnp.sum(weights, axis=1, keepdims=True)
            mixed = mixed + jnp.dot(
                weights.astype(bf), vb[:start].reshape(span, HEAD), preferred_element_type=f32
            )
        mixed = (mixed / mass).astype(bf)
        for number, i in enumerate(pair):
            ob[i] = mixed[number * rows : (number + 1) * rows]

    @pl.loop(0, near)
    def _(step):
        @pl.when(step == 1)
        def _():
            relay(2)
            cross_over(1)

        at_home = step < near // 2
        stages = (
            jnp.where(at_home, 2 * step + 1, 2 * step - near),
            jnp.where(at_home, lax.rem(2 * step + 2, near), 2 * step - near + 1),
        )
        pair = [
            jnp.where(at_home, home, away) + lax.rem(place_in + near - stage, near)
            for stage in stages
        ]
        for i in pair:

            @pl.when(i != chip)
            def _():
                landed(2, i)

        @pl.when(pair[0] < near)
        def _():
            attend(pair, False)

        @pl.when(pair[0] >= near)
        def _():
            attend(pair, True)

        for i in pair:

            @pl.when(i != chip)
            def _():
                remote(
                    ob.at[i], att.at[:, own], o_send.at[i], o_recv.at[chip], 2 * i + core, row
                ).start()

    att[:, own] = ob[chip]

    lw_mate.wait_recv()
    @pl.loop(0, width // tile)
    def _(index):
        block = pl.ds(pl.multiple_of(index * tile, tile), tile)
        summed = acc[block] + jnp.dot(
            ow_ref[block, pl.ds(pl.multiple_of(other * width, width), width)],
            lwb[...],
            preferred_element_type=f32,
        )
        w2[block] = summed.astype(bf)

    direct = jnp.dot(res_ref[...], lw_ref[...], preferred_element_type=f32)
    lif[...] = direct

    cot_copy.wait_recv()
    m_copy.wait_recv()
    bridge[...] = (mb[...].astype(f32) + mr[...].astype(f32)).astype(bf)
    belongs = (
        lax.broadcasted_iota(jnp.int32, (rows, total), 1) // PATCH
        == lax.broadcasted_iota(jnp.int32, (rows, total), 0)
    ).astype(f32).astype(bf)
    own_bytes = total // 2
    cot_sum = sum(
        jnp.dot(
            belongs[:, index * own_bytes : (index + 1) * own_bytes], cot_ref[index],
            preferred_element_type=f32,
        )
        for index in range(2)
    )

    def mates_weights_of(which, source):
        for line in (side, 1 - side):
            to_mate(which, source, line).wait_recv()

    def turn(source):
        lanes = pl.ds(pl.multiple_of(source * 2 * depth * shard, HEAD), 2 * depth * shard)
        wit[:, lanes] = jnp.transpose(wi[lanes])

    for hop in range(3, levels):
        relay(hop)
    for hop in range(2, levels - 1):
        cross_over(hop)
    for i in range(chips):

        @pl.when(i != chip)
        def _():
            back = remote(
                ob.at[i], att.at[:, heads_of(i)], o_send.at[i], o_recv.at[i], 2 * i + core, row
            )
            back.wait_recv()
            back.wait_send()

    e_copies = []
    red[...] = contract(gd_ref[...], att[...], 1, 1).astype(bf)
    red_copy = remote(red, redr, y_send.at[3], y_recv.at[3], me, other)
    red_copy.start()
    e1[...] = (
        jnp.dot(att[...], w2[...], preferred_element_type=f32) + lif[...]
    ).astype(bf)
    for index in range(pieces):
        patches = pl.ds(index * per_piece, per_piece)
        copy = remote(e1.at[patches], e1r.at[patches], e_send.at[index], e_recv.at[index], me, other)
        copy.start()
        e_copies.append(copy)
    mates_weights_of(0, level)
    for hop in range(1, levels - 1):
        for source in (level - hop, level + hop):

            @pl.when((source >= 0) & (source < levels))
            def _():
                mates_weights_of(0, source)
                turn(source)

    cross_over(levels - 1)
    turn(level)
    wit[:, columns:] = jnp.transpose(wi[columns:])
    red_copy.wait_recv()
    reduced = red[...].astype(f32) + redr[...].astype(f32)
    scaled = (reduced * task_scales).astype(bf)
    lifted = contract(scaled, bridge[...], 0, 0)

    lif[...] = lifted

    @pl.loop(0, pieces)
    def _(index):
        block = pl.ds(pl.multiple_of(index * SPAN, SPAN), SPAN)
        patches = pl.ds(pl.multiple_of(index * per_piece, per_piece), per_piece)
        remote(
            e1.at[patches], e1r.at[patches], e_send.at[index], e_recv.at[index], me, other
        ).wait_recv()
        projected = (
            e1[patches].astype(f32) + e1r[patches].astype(f32) + lif[patches]
        ).astype(bf)
        near_by = (
            lax.broadcasted_iota(jnp.int32, (per_piece, SPAN), 1) // PATCH
            == lax.broadcasted_iota(jnp.int32, (per_piece, SPAN), 0)
        ).astype(f32).astype(bf)
        inputs = inp[block] + contract(near_by, projected, 0, 0)
        scales = sca[block]
        inverse = lax.rsqrt(jnp.mean(inputs * inputs, axis=1, keepdims=True) + 1e-06)
        normed = (inputs * inverse * gain_ref[...]).astype(bf)
        lowered = contract(normed, ld_ref[...], 1, 1)
        inp[block] = inputs
        inv[block] = jnp.broadcast_to(inverse, (SPAN, HEAD))
        low[block] = lowered
        nrm[block, :columns] = normed
        nrm[block, columns:] = (lowered * scales).astype(bf)

    for source in range(levels):
        mates_weights_of(1, source)
    for source in (level - (levels - 1), level + (levels - 1)):

        @pl.when((source >= 0) & (source < levels))
        def _():
            mates_weights_of(0, source)
            turn(source)

    @pl.loop(0, pieces)
    def _(index):
        block = pl.ds(pl.multiple_of(index * SPAN, SPAN), SPAN)
        upper = jnp.dot(nrm[block], wi[...], preferred_element_type=f32)
        inner = pl.ds(pl.multiple_of(lax.rem(index * SPAN, own_bytes), SPAN), SPAN)
        through = jnp.dot(
            cot_ref[index * SPAN // own_bytes, inner], wo[...], preferred_element_type=f32
        )
        grown = (through * gelu_slope(upper)).astype(bf)
        gr[block] = grown
        both = jnp.dot(grown, wit[...], preferred_element_type=f32)
        back_rank = both[:, columns:]
        moved = (back_rank * sca[block]).astype(bf)
        mv[block] = moved
        bl[block] = back_rank * low[block]
        back_total = both[:, :columns] + jnp.dot(
            moved, ld_ref[...], preferred_element_type=f32
        )
        inputs = inp[block]
        inverse = inv[block][:, :1]
        gained = back_total * gain_ref[...]
        average = jnp.mean(gained * inputs, axis=1, keepdims=True)
        back_inputs = inverse * (gained - inputs * (inverse * inverse * average))
        near = (
            lax.broadcasted_iota(jnp.int32, (per_piece, SPAN), 1) // PATCH
            == lax.broadcasted_iota(jnp.int32, (per_piece, SPAN), 0)
        ).astype(f32).astype(bf)
        patches = pl.ds(pl.multiple_of(index * per_piece, per_piece), per_piece)
        bp[patches] = jnp.dot(
            near, back_inputs.astype(bf), preferred_element_type=f32
        ).astype(bf)
        remote(
            bp.at[patches], bpr.at[patches], b_send.at[index], b_recv.at[index], me, other
        ).start()

    down = contract(mv[...], nrm[:, :columns], 0, 0)[:rank]
    high, low_part = split_pair(bl[...])
    by_patch = jnp.dot(belongs, high, preferred_element_type=f32) + jnp.dot(
        belongs, low_part, preferred_element_type=f32
    )
    small = exact(picks, by_patch, 1, 0)
    small = jnp.concatenate([small, jnp.zeros_like(small)], axis=0)
    down = down.astype(bf)
    lift = contract(nrm[:, columns:], gr[...], 0, 0)[:rank].astype(bf)
    spread = width // HEAD
    thin = columns // HEAD
    for t in range(spread):
        early[t] = lift[:, t * HEAD : (t + 1) * HEAD]
    for t in range(thin):
        early[spread + t] = down[:, t * HEAD : (t + 1) * HEAD]
    early[spread + thin] = small.astype(bf)
    base = chips // 4

    def owner(t):
        return 2 * (base + t) + 1

    def held(t):
        return pl.ds(0, min(share_of, tiles - t * share_of))

    def parcel(kind, t):
        source, landing = (early, late)[kind], (early_in, late_in)[kind]
        size = min(share_of, tiles - t * share_of)
        return remote(
            source.at[pl.ds(share_of * t, size)], landing.at[me, held(t)], r_send.at[kind, t],
            r_recv.at[kind, me], owner(t), row,
        )

    def spread_out(kind):
        for t in range(owners):

            @pl.when(owner(t) != me)
            def _():
                parcel(kind, t).start()

            @pl.when(owner(t) == me)
            def _():
                size = min(share_of, tiles - t * share_of)
                source, landing = (early, late)[kind], (early_in, late_in)[kind]
                landing[me, :size] = source[share_of * t : share_of * t + size]

    def settle_out(kind):
        for t in range(owners):

            @pl.when(owner(t) != me)
            def _():
                parcel(kind, t).wait_send()

    def gather_in(kind, final):
        landing = (early_in, late_in)[kind]
        for t in range(owners):

            @pl.when(owner(t) == me)
            def _():
                size = min(share_of, tiles - t * share_of)
                for d in range(1, count):
                    source = lax.rem(me + d, count)
                    remote(
                        landing.at[source, held(t)], landing.at[source, held(t)],
                        r_send.at[kind, 0], r_recv.at[kind, source], me, row,
                    ).wait_recv()
                summed = jnp.sum(landing[:, :size].astype(f32), axis=0)
                if kind == 0 and t * share_of >= spread:
                    cross[:size] = summed.astype(bf)
                    swap = remote(
                        cross.at[held(t)], crossr.at[held(t)], y_send.at[4], y_recv.at[4], me, other
                    )
                    swap.start()
                    swap.wait_recv()
                    summed = cross[:size].astype(f32) + crossr[:size].astype(f32)
                final[t, :size] = summed.astype(bf)
                for d in range(1, count):
                    issue(kind, final, t, d).start()

    def issue(kind, final, t, d):
        piece = final.at[t, held(t)]
        return remote(
            piece, piece, g_send.at[kind, d], g_recv.at[kind, t], lax.rem(me + d, count), row
        )

    def finish_in(kind, final):
        for t in range(owners):

            @pl.when(owner(t) != me)
            def _():
                piece = final.at[t, held(t)]
                remote(
                    piece, piece, g_send.at[kind, 0], g_recv.at[kind, t], me, row
                ).wait_recv()

    def settle_in(kind, final):
        for t in range(owners):

            @pl.when(owner(t) == me)
            def _():
                for d in range(1, count):
                    issue(kind, final, t, d).wait_send()
                if kind == 0 and t * share_of >= spread:
                    remote(
                        cross.at[held(t)], crossr.at[held(t)], y_send.at[4], y_recv.at[4], me, other
                    ).wait_send()

    spread_out(0)

    for index in range(pieces):
        patches = pl.ds(index * per_piece, per_piece)
        remote(
            bp.at[patches], bpr.at[patches], b_send.at[index], b_recv.at[index], me, other
        ).wait()
    patch_grad = (bp[...].astype(f32) + bpr[...].astype(f32) + cot_sum).astype(bf)
    pulled = jnp.dot(scaled, patch_grad, preferred_element_type=f32).astype(bf)
    back_scaled = contract(bridge[...], patch_grad, 1, 1)
    back_reduced = (back_scaled * task_scales).astype(bf)
    outward = jnp.dot(back_reduced, att[...], preferred_element_type=f32).astype(bf)
    product = back_scaled * reduced
    product = jnp.concatenate([product, jnp.zeros((HEAD - rank, rows), f32)], axis=0)
    tops = exact(picks, product, 1, 1)
    tops = jnp.concatenate([tops, jnp.zeros_like(tops)], axis=0)
    for t in range(spread):
        late[t] = outward[:, t * HEAD : (t + 1) * HEAD]
    for t in range(thin):
        late[spread + t] = pulled[:, t * HEAD : (t + 1) * HEAD]
    late[spread + thin] = tops.astype(bf)
    spread_out(1)
    gather_in(0, early_full)
    gather_in(1, late_full)
    finish_in(0, early_full)

    def tile_of(final, t):
        return final[t // share_of, t % share_of]

    for t in range(spread):
        glu_out[:, t * HEAD : (t + 1) * HEAD] = tile_of(early_full, t).astype(f32)
    for t in range(thin):
        gld_out[:, t * HEAD : (t + 1) * HEAD] = tile_of(early_full, spread + t).astype(f32)
    lsc_out[...] = tile_of(early_full, spread + thin)[:TASKS, :rank].astype(f32)
    settle_out(0)
    settle_in(0, early_full)
    settle_out(1)
    for which, buffer in weights_in:
        for source in range(levels):
            settle_along(which, source)
            across(which, source, side).wait_send()
            for line in (side, 1 - side):
                to_mate(which, source, line).wait_send()
    for to in targets:
        for which in range(3):
            hand(which, to).wait_send()
    for source in range(chips):
        for which in range(2):
            share(which, source).wait_send()
    for copy in [lw_copy, lw_mate, cot_copy, m_copy, red_copy] + e_copies:
        copy.wait_send()
    finish_in(1, late_full)
    for t in range(spread):
        ggd_out[:, t * HEAD : (t + 1) * HEAD] = tile_of(late_full, t).astype(f32)
    for t in range(thin):
        bridge[:, t * HEAD : (t + 1) * HEAD] = tile_of(late_full, spread + t)
    ggu_out[...] = contract(bridge[...], lw_ref[...], 1, 1)
    gsc_out[...] = tile_of(late_full, spread + thin)[:TASKS, :rank].astype(f32)
    settle_in(1, late_full)


def copy_kernel(*refs):
    number = len(refs) // 2
    for source, target in zip(refs[:number], refs[number:]):
        target[...] = source[...]


def paired_body(
    patch_queries, patch_keys, patch_values, patch_tasks, residual, output_weight, global_down,
    global_up, global_scales, local_weight, byte_ids, byte_table, position_table, norm_gain,
    hidden_in, hidden_out, local_down, local_up, local_scales, cotangent,
):
    count = lax.axis_size("seq")
    rows, width = patch_queries.shape
    chips = count // 2
    depth = 2
    levels = chips // depth
    columns = local_weight.shape[1]
    rank = global_up.shape[0]
    vocab = byte_table.shape[0]
    total = byte_ids.shape[0]
    wide = columns + HEAD
    pieces = total // SPAN
    bf, f32 = jnp.bfloat16, jnp.float32
    vm = pltpu.VMEM
    dma = pltpu.SemaphoreType.DMA
    args = (
        patch_queries, patch_keys, patch_values, patch_tasks.reshape(1, rows), residual,
        output_weight, jnp.transpose(global_down), global_up, global_scales, local_weight,
        byte_ids.reshape(1, total), byte_table, position_table, norm_gain.reshape(1, columns),
        jnp.transpose(hidden_in), jnp.transpose(hidden_out), jnp.transpose(local_down), local_up,
        local_scales, cotangent,
    )
    outs = pl.pallas_call(
        functools.partial(step_kernel, chips, depth),
        out_shape=(
            jax.ShapeDtypeStruct((rank, width), f32),
            jax.ShapeDtypeStruct((rank, width), f32),
            jax.ShapeDtypeStruct((TASKS, rank), f32),
            jax.ShapeDtypeStruct((rank, columns), f32),
            jax.ShapeDtypeStruct((rank, width), f32),
            jax.ShapeDtypeStruct((TASKS, rank), f32),
        ),
        in_specs=[pl.BlockSpec(memory_space=pl.ANY)] * len(args),
        out_specs=(pl.BlockSpec(memory_space=vm),) * 6,
        scratch_shapes=[
            vm((rows, width), bf), vm((rows, width), bf), vm((rows, width), bf),
            vm((1, rows), jnp.int32), vm((rows, width), bf), vm(output_weight.shape, bf),
            vm((rank, width), bf), vm((rank, width), bf), vm((TASKS, rank), f32),
            vm((width, columns), bf), vm((1, total), jnp.int32), vm((PATCH, columns), bf),
            vm((1, columns), f32), vm((HEAD, columns), bf), vm((TASKS, rank), f32),
            vm((2, total // 2, columns), bf), vm((wide, width), bf), vm((columns, width), bf),
            vm((width, wide), bf),
            vm((chips, rows, HEAD), bf), vm((count, rows, HEAD), bf), vm((count, rows, HEAD), bf),
            vm((chips, rows, HEAD), bf), vm((rows, width), bf), vm((width, columns), bf),
            vm((width, columns), bf), vm((width, columns), f32), vm((rows, columns), bf),
            vm((rows, columns), bf), vm((rank, columns), bf), vm((rank, columns), bf),
            vm((rank, columns), bf), vm((rank, rows), bf), vm((rank, rows), bf),
            vm((rows, columns), f32),
            vm((vocab + 2 * HEAD, wide + HEAD), bf), vm((total, columns), f32),
            vm((total, wide), bf), vm((total, HEAD), f32), vm((total, HEAD), f32),
            vm((total, HEAD), f32), vm((total, HEAD), f32), vm((total, width), bf),
            vm((total, HEAD), bf), vm((rows, columns), bf), vm((rows, columns), bf),
            vm((4, rank, HEAD), bf), vm((4, rank, HEAD), bf),
        ]
        + [
            vm((count, rank, HEAD), bf), vm((count, 4, rank, HEAD), bf),
            vm((chips // 2, 4, rank, HEAD), bf),
        ]
        * 2
        + [
            dma((len(args),)), dma((3, chips)), dma((3, chips)), dma((2, chips)), dma((2, chips)),
            dma((chips,)), dma((chips,)), dma((2, levels, 2)), dma((2, levels)), dma((2, levels)),
            dma((2, levels)), dma((2, chips)), dma((2, chips)), dma((1,)), dma((1,)), dma((5,)),
            dma((5,)), dma((pieces,)), dma((pieces,)), dma((pieces,)), dma((pieces,)),
            dma((2, chips)), dma((2, count)), dma((2, count)), dma((2, chips)),
        ],
        compiler_params=pltpu.CompilerParams(
            collective_id=0, has_side_effects=True, vmem_limit_bytes=60 * 1024 * 1024
        ),
        name="step",
    )(*args)
    ggd, ggu, gsc, gld, glu, lsc = pl.pallas_call(
        copy_kernel,
        out_shape=tuple(jax.ShapeDtypeStruct(item.shape, item.dtype) for item in outs),
        in_specs=[pl.BlockSpec(memory_space=vm)] * len(outs),
        out_specs=(pl.BlockSpec(memory_space=vm),) * len(outs),
        name="spill",
    )(*outs)
    return (jnp.transpose(ggd), ggu, gsc, jnp.transpose(gld), glu, lsc)


def pick_body(seq_count, row_count, *args):
    heads = args[0].shape[1] // HEAD
    rank = args[7].shape[0]
    hidden = args[14].shape[0]
    fits = (
        row_count == 2
        and seq_count == 2 * heads
        and heads % 4 == 0
        and rank == 2 * TASKS
        and args[0].shape[1] == hidden
        and (4 * rank * hidden) % (seq_count * 16 * HEAD) == 0
        and hidden // HEAD + args[9].shape[1] // HEAD < seq_count
        and args[0].shape[0] == HEAD
    )
    return paired_body(*args) if fits else general_body(*args)


def solution(mesh):
    placed = (
        P("seq", "row"),
        P("seq", "row"),
        P("seq", "row"),
        P("seq"),
        P("seq", "row"),
        P("row", None),
        P("row", None),
        P(None, "row"),
        P(),
        P("row", None),
        P("seq"),
        P(),
        P(),
        P(),
        P("row", "seq"),
        P("row", "seq"),
        P(),
        P(None, "row"),
        P(),
        P(("seq", "row"), None),
    )
    chosen = functools.partial(pick_body, mesh.shape["seq"], mesh.shape["row"])
    return jax.shard_map(
        chosen,
        mesh=mesh,
        in_specs=placed,
        out_specs=(P("row", None), P(None, "row"), P(), P(), P(None, "row"), P()),
        check_vma=False,
    )
```

```python
import functools
import math

import jax
import jax.numpy as jnp
from jax import lax
from jax.experimental import pallas as pl
from jax.experimental.pallas import tpu as pltpu
from jax.sharding import PartitionSpec as P

HEAD = 128
VOCAB = 256
PATCH = 8
TASKS = 8


def contract(left, right, left_dim, right_dim):
    return lax.dot_general(
        left, right, (((left_dim,), (right_dim,)), ((), ())), preferred_element_type=jnp.float32
    )


def select_rows(table, tasks):
    picks = (tasks[:, None] == jnp.arange(table.shape[0], dtype=jnp.int32)[None, :]).astype(
        jnp.float32
    )
    return jnp.dot(picks, table, precision=lax.Precision.HIGHEST)


def task_totals(tasks, values):
    picks = (tasks[:, None] == jnp.arange(TASKS, dtype=jnp.int32)[None, :]).astype(jnp.float32)
    return lax.dot_general(picks, values, (((0,), (0,)), ((), ())), precision=lax.Precision.HIGHEST)


def gelu_slope(upper):
    cumulative = 0.5 * (1.0 + lax.erf(upper * 0.7071067811865476))
    density = jnp.exp(-0.5 * upper * upper) * 0.3989422804014327
    return cumulative + upper * density


def local_inputs(
    identities, projected, tasks, byte_table, position_table, norm_gain, local_down, local_scales
):
    count = identities.shape[0]
    picks = (identities[:, None] == jnp.arange(VOCAB, dtype=jnp.int32)[None, :]).astype(
        jnp.bfloat16
    )
    embedded = jnp.dot(picks, byte_table, preferred_element_type=jnp.float32)
    patches = count // PATCH
    inputs = (
        embedded.reshape(patches, PATCH, -1)
        + position_table.astype(jnp.float32)[None]
        + projected.astype(jnp.float32)[:, None, :]
    )
    inputs = inputs.reshape(count, -1)
    inverse = lax.rsqrt(jnp.mean(inputs * inputs, axis=1, keepdims=True) + 1e-06)
    normed = (inputs * inverse * norm_gain).astype(jnp.bfloat16)
    lowered = jnp.dot(normed, local_down, preferred_element_type=jnp.float32)
    byte_tasks = jnp.repeat(tasks, PATCH)
    scales = select_rows(local_scales, byte_tasks)
    shrunk = (lowered * scales).astype(jnp.bfloat16)
    return (inputs, inverse, normed, lowered, scales, shrunk, byte_tasks)


def keep_state(current):
    return current


def update_state(state, query_rows, first, key_heads, value_heads, key_places, scale):
    running_max, running_sum, running_out = state
    count = query_rows.shape[0]
    heads = key_heads.shape[1]
    query_heads = query_rows.reshape(count, heads, HEAD)
    scores = (
        jnp.einsum("qhd,khd->hqk", query_heads, key_heads, preferred_element_type=jnp.float32)
        * scale
    )
    query_places = first + jnp.arange(count, dtype=jnp.int32)
    allowed = key_places[None, :] <= query_places[:, None]
    scores = jnp.where(allowed[None], scores, -1e30)
    new_max = jnp.maximum(running_max, jnp.max(scores, axis=2))
    weights = jnp.where(allowed[None], jnp.exp(scores - new_max[:, :, None]), 0.0)
    shrink = jnp.exp(running_max - new_max)
    running_sum = running_sum * shrink + jnp.sum(weights, axis=2)
    mixed = jnp.einsum(
        "hqk,khd->qhd",
        weights.astype(jnp.bfloat16),
        value_heads,
        preferred_element_type=jnp.float32,
    )
    running_out = running_out * jnp.transpose(shrink)[:, :, None] + mixed
    return (new_max, running_sum, running_out)


def finish_state(state):
    running_max, running_sum, running_out = state
    result = running_out / jnp.transpose(running_sum)[:, :, None]
    return result.reshape(result.shape[0], -1).astype(jnp.bfloat16)


def general_body(
    patch_queries,
    patch_keys,
    patch_values,
    patch_tasks,
    residual,
    output_weight,
    global_down,
    global_up,
    global_scales,
    local_weight,
    byte_ids,
    byte_table,
    position_table,
    norm_gain,
    hidden_in,
    hidden_out,
    local_down,
    local_up,
    local_scales,
    cotangent,
):
    rows = patch_queries.shape[0]
    width = patch_queries.shape[1]
    heads = width // HEAD
    row_count = lax.axis_size("row")
    seq_index = lax.axis_index("seq")
    row_index = lax.axis_index("row")
    scale = 1.0 / math.sqrt(HEAD)
    own_first = seq_index * rows
    groups = [(patch_queries, own_first)]

    def visit(state, query_rows, first, key_heads, value_heads, key_places):

        def refresh(current):
            return update_state(
                current, query_rows, first, key_heads, value_heads, key_places, scale
            )

        return lax.cond(
            key_places[0] <= first + query_rows.shape[0] - 1, refresh, keep_state, state
        )

    initial = tuple(
        (
            (
                jnp.full((heads, query_rows.shape[0]), -1e30, jnp.float32),
                jnp.zeros((heads, query_rows.shape[0]), jnp.float32),
                jnp.zeros((query_rows.shape[0], heads, HEAD), jnp.float32),
            )
            for query_rows, first in groups
        )
    )
    key_piece = lax.all_gather(patch_keys, "seq", axis=0, tiled=True)
    value_piece = lax.all_gather(patch_values, "seq", axis=0, tiled=True)
    count = key_piece.shape[0]
    span = math.gcd(count, 1024)

    def one_span(index, states):
        offset = index * span
        key_heads = lax.dynamic_slice_in_dim(key_piece, offset, span, 0).reshape(span, heads, HEAD)
        value_heads = lax.dynamic_slice_in_dim(value_piece, offset, span, 0).reshape(
            span, heads, HEAD
        )
        key_places = offset + jnp.arange(span, dtype=jnp.int32)
        updated = []
        for (query_rows, first), state in zip(groups, states):
            updated.append(visit(state, query_rows, first, key_heads, value_heads, key_places))
        return tuple(updated)

    states = lax.fori_loop(0, count // span, one_span, initial)
    outputs = [finish_state(state) for state in states]
    attended = outputs[0]
    reduced = lax.psum(jnp.dot(attended, global_down, preferred_element_type=jnp.float32), "row")
    task_scales = select_rows(global_scales, patch_tasks)
    scaled = (reduced * task_scales).astype(jnp.bfloat16)
    mixed = lax.psum_scatter(
        contract(output_weight, attended, 0, 1).astype(jnp.bfloat16),
        "row",
        scatter_dimension=0,
        tiled=True,
    ).astype(jnp.float32)
    mixed = mixed + jnp.transpose(residual.astype(jnp.float32)) + contract(global_up, scaled, 0, 1)
    mixed_b = mixed.astype(jnp.bfloat16)
    own_patches = rows // row_count
    own_bytes = own_patches * PATCH
    rows_in, rows_out = (
        lax.all_gather(hidden_in, "seq", axis=1, tiled=True),
        lax.all_gather(hidden_out, "seq", axis=1, tiled=True),
    )
    partial_value = contract(mixed_b, local_weight, 0, 0)
    projected = lax.psum(partial_value.astype(jnp.bfloat16), "row")
    every = local_inputs(
        byte_ids,
        projected,
        patch_tasks,
        byte_table,
        position_table,
        norm_gain,
        local_down,
        local_scales,
    )
    normed_all = every[2]
    shrunk_all = every[5]
    cotangent_all = lax.all_gather(cotangent, "row", axis=0, tiled=True)
    inputs, inverse, normed, lowered, scales, shrunk, byte_tasks = [
        lax.dynamic_slice_in_dim(value, row_index * own_bytes, own_bytes, 0) for value in every
    ]
    upper = contract(normed_all, rows_in, 1, 1) + jnp.dot(
        shrunk_all, local_up, preferred_element_type=jnp.float32
    )
    through = contract(cotangent_all, rows_out, 1, 1)
    grown = (through * gelu_slope(upper)).astype(jnp.bfloat16)
    grad_local_up = contract(shrunk_all, grown, 0, 0)
    back_norm, back_rank = (
        lax.psum_scatter(
            jnp.dot(grown, rows_in, preferred_element_type=jnp.float32).astype(jnp.bfloat16),
            "row",
            scatter_dimension=0,
            tiled=True,
        ).astype(jnp.float32),
        lax.psum_scatter(
            contract(grown, local_up, 1, 1).astype(jnp.bfloat16),
            "row",
            scatter_dimension=0,
            tiled=True,
        ).astype(jnp.float32),
    )
    grad_local_scales = task_totals(byte_tasks, back_rank * lowered)
    moved = (back_rank * scales).astype(jnp.bfloat16)
    grad_local_down = contract(normed, moved, 0, 0)
    back_total = back_norm + contract(moved, local_down, 1, 1)
    gained = back_total * norm_gain
    average = jnp.mean(gained * inputs, axis=1, keepdims=True)
    back_inputs = cotangent.astype(jnp.float32) + inverse * (
        gained - inputs * inverse * inverse * average
    )
    patch_grad = back_inputs.reshape(own_patches, PATCH, -1).sum(axis=1).astype(jnp.bfloat16)
    back_mixed = contract(
        lax.all_gather(patch_grad, "row", axis=0, tiled=True), local_weight, 1, 1
    ).astype(jnp.bfloat16)
    grad_global_up = contract(scaled, back_mixed, 0, 0)
    back_scaled = lax.psum(contract(back_mixed, global_up, 1, 1), "row")
    grad_global_scales = task_totals(patch_tasks, back_scaled * reduced)
    back_reduced = (back_scaled * task_scales).astype(jnp.bfloat16)
    grad_global_down = contract(attended, back_reduced, 0, 0)
    grad_global_down, grad_global_up, grad_global_scales, grad_local_up = lax.psum(
        (grad_global_down, grad_global_up, grad_global_scales, grad_local_up), "seq"
    )
    grad_local_down, grad_local_scales = lax.psum(
        (grad_local_down, grad_local_scales), ("seq", "row")
    )
    return (
        grad_global_down,
        grad_global_up,
        grad_global_scales,
        grad_local_down,
        grad_local_up,
        grad_local_scales,
    )


MESH = pl.DeviceIdType.MESH
SPAN = 256


def remote(src, dst, send, recv, seq, row):
    return pltpu.make_async_remote_copy(
        src_ref=src,
        dst_ref=dst,
        send_sem=send,
        recv_sem=recv,
        device_id=(seq, row),
        device_id_type=MESH,
    )


def exact(left, right, left_dim, right_dim):
    return lax.dot_general(
        left, right, (((left_dim,), (right_dim,)), ((), ())), precision=lax.Precision.HIGHEST,
        preferred_element_type=jnp.float32,
    )


def split_pair(value):
    high = value.astype(jnp.bfloat16)
    low = (value - high.astype(jnp.float32)).astype(jnp.bfloat16)
    return high, low


def step_kernel(
    chips, depth,
    q_hbm, k_hbm, v_hbm, tasks_hbm, res_hbm, ow_hbm, gd_hbm, gu_hbm, gs_hbm, lw_hbm, ids_hbm,
    table_hbm, pos_hbm, gain_hbm, hi_hbm, ho_hbm, ld_hbm, lu_hbm, ls_hbm, cot_hbm,
    ggd_out, ggu_out, gsc_out, gld_out, glu_out, lsc_out,
    q_ref, k_ref, v_ref, tasks_ref, res_ref, ow_ref, gd_ref, gu_ref, gs_ref, lw_ref, ids_ref,
    pos_ref, gain_ref, ld_ref, ls_ref, cot_ref, wi, wo, wit,
    qb, kb, vb, ob, att, lwb, w2, acc, e1, e1r, mb, mr, bridge,
    red, redr, lif, emb, inp, nrm, inv, low, sca, bl, gr, mv, bp, bpr, cross, crossr,
    early, early_in, early_full, late, late_in, late_full,
    in_sem, a_send, a_recv, f_send, f_recv, o_send, o_recv, z_send, z_recv, x_send, x_recv,
    p_send, p_recv, c_send, c_recv, y_send, y_recv, e_send, e_recv, b_send, b_recv,
    r_send, r_recv, g_send, g_recv,
):
    bf, f32 = jnp.bfloat16, jnp.float32
    count = 2 * chips
    owners = chips // 2
    share_of = count // owners
    me = lax.axis_index("seq")
    row = lax.axis_index("row")
    other = 1 - row
    chip, core = me // 2, lax.rem(me, 2)
    mate = 2 * chip + (1 - core)
    rows, width = q_hbm.shape
    half = width // 2
    columns = lw_hbm.shape[1]
    rank = gu_hbm.shape[0]
    wide = columns + HEAD
    shard = hi_hbm.shape[0]
    vocab = table_hbm.shape[0]
    total = rows * PATCH
    pieces = total // SPAN
    per_piece = SPAN // PATCH
    tiles = width // HEAD + columns // HEAD + 1

    def heads_of(number):
        return pl.ds(pl.multiple_of(number * HEAD, HEAD), HEAD)

    def shard_of(slot):
        return pl.ds(pl.multiple_of(slot * shard, shard), shard)

    barrier = pltpu.get_barrier_semaphore()
    peers = [(lax.rem(me + d, count), row) for d in range(1, count)] + [(me, other)]
    for seq, line in peers:
        pl.semaphore_signal(barrier, inc=1, device_id=(seq, line), device_id_type=MESH)

    loads = {}

    def load(name, src, dst):
        copy = pltpu.make_async_copy(src, dst, in_sem.at[len(loads)])
        copy.start()
        loads[name] = copy

    load("ho", ho_hbm, wo.at[shard_of(me)])
    load("hi", hi_hbm, wi.at[shard_of(me)])
    load("k", k_hbm, k_ref)
    load("v", v_hbm, v_ref)
    load("q", q_hbm, q_ref)
    load("lw", lw_hbm, lw_ref)
    load("cot", cot_hbm, cot_ref.at[row])
    load("gu", gu_hbm, gu_ref)
    load("ow", ow_hbm, ow_ref)
    load("res", res_hbm, res_ref)
    load("gd", gd_hbm, gd_ref)
    load("lu", lu_hbm, wi.at[pl.ds(columns, rank)])
    load("ld", ld_hbm, ld_ref.at[pl.ds(0, rank)])
    load("table", table_hbm, emb.at[pl.ds(0, vocab), pl.ds(0, columns)])
    load("tasks", tasks_hbm, tasks_ref)
    load("ids", ids_hbm, ids_ref)
    load("pos", pos_hbm, pos_ref)
    load("gain", gain_hbm, gain_ref)
    load("gs", gs_hbm, gs_ref)
    load("ls", ls_hbm, ls_ref)

    ld_ref[rank:] = jnp.zeros((HEAD - rank, columns), bf)
    wi[columns + rank :] = jnp.zeros((HEAD - rank, width), bf)
    emb[vocab : vocab + rows, :columns] = jnp.zeros((rows, columns), bf)
    emb[:vocab, columns:] = jnp.zeros((vocab, 2 * HEAD), bf)
    emb[vocab + HEAD :] = jnp.zeros((HEAD, wide + HEAD), bf)

    pl.semaphore_wait(barrier, len(peers))

    own = heads_of(chip)
    near = chips // 2
    place_in = lax.rem(chip, near)
    home = chip - place_in
    away = near - home
    own_half = pl.ds(pl.multiple_of(core * half, half), half)

    def hand(which, to):
        src, dst = (
            (k_ref, kb.at[me]), (v_ref, vb.at[me]), (q_ref, qb.at[chip])
        )[which]
        return remote(
            src.at[:, heads_of(to)], dst, a_send.at[which, to], a_recv.at[which, chip],
            2 * to + core, row,
        )

    def landed(which, source):
        dst = (kb.at[2 * source + core], vb.at[2 * source + core], qb.at[source])[which]
        remote(
            dst, dst, a_send.at[which, source], a_recv.at[which, source], me, row
        ).wait_recv()

    targets = [away + lax.rem(place_in + j, near) for j in range(near)] + [
        home + lax.rem(place_in + j, near) for j in range(1, near)
    ]
    levels = chips // depth
    level, side = chip // depth, lax.rem(chip, depth)
    weights_in = ((1, wo), (0, wi))
    neighbour = 2 * (level * depth + (1 - side)) + core

    def slot_of(number, line):
        return 2 * (number * depth + line) + core

    def move(which, slot, sends, recvs, to):
        buffer = wo if which else wi
        piece = buffer.at[shard_of(slot)]
        return remote(piece, piece, sends, recvs, to, row)

    def pass_along(which, source):
        slot = slot_of(source, side)
        for way, step in ((0, 1), (1, -1)):
            ahead = level + step
            fits = (ahead >= 0) & (ahead < levels) & ((source - level) * step <= 0)

            @pl.when(fits)
            def _():
                move(
                    which, slot, z_send.at[which, source, way], z_recv.at[which, source],
                    slot_of(ahead, side),
                ).start()

    def settle_along(which, source):
        slot = slot_of(source, side)
        for way, step in ((0, 1), (1, -1)):
            ahead = level + step
            fits = (ahead >= 0) & (ahead < levels) & ((source - level) * step <= 0)

            @pl.when(fits)
            def _():
                move(
                    which, slot, z_send.at[which, source, way], z_recv.at[which, source],
                    slot_of(ahead, side),
                ).wait_send()

    def across(which, source, line):
        return move(
            which, slot_of(source, line), x_send.at[which, source], x_recv.at[which, source],
            neighbour,
        )

    def to_mate(which, source, line):
        number = jnp.where(line == side, source, levels + source)
        return move(
            which, slot_of(source, line), p_send.at[which, number], p_recv.at[which, number], mate
        )

    def relay(hop):
        for which, buffer in weights_in:
            for source in (level - hop, level + hop):

                @pl.when((source >= 0) & (source < levels))
                def _():
                    move(
                        which, slot_of(source, side), z_send.at[which, source, 0],
                        z_recv.at[which, source], me,
                    ).wait_recv()
                    pass_along(which, source)
                    across(which, source, side).start()
                    to_mate(which, source, side).start()

    def cross_over(hop):
        for which, buffer in weights_in:
            for source in {0: (level,)}.get(hop, (level - hop, level + hop)):

                @pl.when((source >= 0) & (source < levels))
                def _():
                    across(which, source, 1 - side).wait_recv()
                    to_mate(which, source, 1 - side).start()

    loads["ho"].wait()
    loads["hi"].wait()
    for which, buffer in weights_in:
        pass_along(which, level)
        across(which, level, side).start()
        to_mate(which, level, side).start()

    loads["k"].wait()
    loads["v"].wait()
    loads["q"].wait()


    def share(which, source):
        buffer = (kb, vb)[which]
        slot = 2 * source + core
        return remote(
            buffer.at[slot], buffer.at[slot], f_send.at[which, source], f_recv.at[which, source],
            mate, row,
        )

    kb[me] = k_ref[:, own]
    vb[me] = v_ref[:, own]
    qb[chip] = q_ref[:, own]
    for to in targets:
        for which in range(2):
            hand(which, to).start()
    for which, src in enumerate((k_ref, v_ref)):
        remote(
            src.at[:, own], (kb, vb)[which].at[me], f_send.at[which, chip],
            f_recv.at[which, chip], mate, row,
        ).start()
    loads["lw"].wait()
    lw_copy = remote(lw_ref.at[own_half], lwb.at[own_half], y_send.at[0], y_recv.at[0], me, other)
    lw_copy.start()
    loads["cot"].wait()
    cot_copy = remote(
        cot_ref.at[row], cot_ref.at[row], c_send.at[0], c_recv.at[0], me, other
    )
    cot_copy.start()

    loads["gu"].wait()
    mb[...] = jnp.dot(gu_ref[...], lw_ref[...], preferred_element_type=f32).astype(bf)
    m_copy = remote(mb, mr, y_send.at[2], y_recv.at[2], me, other)
    m_copy.start()

    tile = math.gcd(width, SPAN)
    loads["ow"].wait()

    @pl.loop(0, width // tile)
    def _(index):
        block = pl.ds(pl.multiple_of(index * tile, tile), tile)
        acc[block] = jnp.dot(
            ow_ref[block, pl.ds(pl.multiple_of(row * width, width), width)],
            lw_ref[...],
            preferred_element_type=f32,
        )

    relay(1)
    for to in targets:
        hand(2, to).start()
    cross_over(0)
    for name in ("res", "gd", "lu", "ld", "table", "tasks", "ids", "pos", "gain", "gs", "ls"):
        loads[name].wait()
    picks = (
        lax.broadcasted_iota(jnp.int32, (TASKS, rows), 0) == tasks_ref[...]
    ).astype(f32)

    def widen(table):
        return jnp.concatenate([table, jnp.zeros((TASKS, HEAD - rank), f32)], axis=1)

    task_scales = exact(gs_ref[...], picks, 0, 0)
    high, low_part = split_pair(exact(picks, widen(ls_ref[...]), 0, 0))
    emb[vocab : vocab + rows, columns:wide] = high
    emb[vocab : vocab + rows, wide:] = low_part
    emb[vocab + rows : vocab + rows + 2 * PATCH, :columns] = jnp.concatenate(
        [pos_ref[...].astype(f32), jnp.zeros((PATCH, columns), f32)], axis=0
    ).astype(bf)
    depth_all = emb.shape[0]

    @pl.loop(0, pieces)
    def _(index):
        block = pl.ds(pl.multiple_of(index * SPAN, SPAN), SPAN)
        line = lax.broadcasted_iota(jnp.int32, (depth_all, SPAN), 0)
        byte = lax.broadcasted_iota(jnp.int32, (depth_all, SPAN), 1) + index * SPAN
        chosen = (
            (line == ids_ref[:, block])
            | (line == vocab + byte // PATCH)
            | (line == vocab + rows + lax.rem(byte, PATCH))
        )
        found = contract(jnp.where(chosen, 1.0, 0.0).astype(bf), emb[...], 0, 0)
        inp[block] = found[:, :columns]
        sca[block] = found[:, columns:wide] + found[:, wide:]

    for j in range(1, near):
        source = home + lax.rem(place_in + near - j, near)
        for which in range(2):
            landed(which, source)
            share(which, source).start()
    for j in range(near):
        source = away + lax.rem(place_in + near - j, near)
        for which in range(2):
            landed(which, source)
            share(which, source).start()
    for source in range(chips):
        for which in range(2):
            buffer = (kb, vb)[which]
            slot = 2 * source + 1 - core
            remote(
                buffer.at[slot], buffer.at[slot], f_send.at[which, source],
                f_recv.at[which, source], mate, row,
            ).wait_recv()

    lw_copy.wait_recv()
    lw_mate = remote(lwb.at[own_half], lwb.at[own_half], y_send.at[1], y_recv.at[1], mate, row)
    lw_mate.start()
    factor = 1.0 / math.sqrt(HEAD) / math.log(2.0)
    span = chips * rows

    def attend(pair, late_half):
        query = jnp.concatenate([qb[i] for i in pair], axis=0)
        start = chips if late_half else 0
        fresh = contract(query, kb[start : start + chips].reshape(span, HEAD), 1, 1)
        places = lax.broadcasted_iota(jnp.int32, (2 * rows, span), 1)
        queries = lax.broadcasted_iota(jnp.int32, (2 * rows, span), 0)
        first, second = [(2 * i + core - start) * rows for i in pair]
        queries = queries + jnp.where(queries < rows, first, second - rows)
        fresh = jnp.where(places <= queries, fresh, -1e30)
        top = jnp.max(fresh, axis=1, keepdims=True)
        if late_half:
            scores = contract(query, kb[:start].reshape(span, HEAD), 1, 1)
            top = jnp.maximum(top, jnp.max(scores, axis=1, keepdims=True))
        weights = jnp.exp2((fresh - top) * factor)
        mass = jnp.sum(weights, axis=1, keepdims=True)
        mixed = jnp.dot(
            weights.astype(bf), vb[start : start + chips].reshape(span, HEAD),
            preferred_element_type=f32,
        )
        if late_half:
            weights = jnp.exp2((scores - top) * factor)
            mass = mass + jnp.sum(weights, axis=1, keepdims=True)
            mixed = mixed + jnp.dot(
                weights.astype(bf), vb[:start].reshape(span, HEAD), preferred_element_type=f32
            )
        mixed = (mixed / mass).astype(bf)
        for number, i in enumerate(pair):
            ob[i] = mixed[number * rows : (number + 1) * rows]

    @pl.loop(0, near)
    def _(step):
        @pl.when(step == near // 2)
        def _():
            relay(2)
            cross_over(1)

        at_home = step < near // 2
        stages = (
            jnp.where(at_home, 2 * step + 1, 2 * step - near),
            jnp.where(at_home, lax.rem(2 * step + 2, near), 2 * step - near + 1),
        )
        pair = [
            jnp.where(at_home, home, away) + lax.rem(place_in + near - stage, near)
            for stage in stages
        ]
        for i in pair:

            @pl.when(i != chip)
            def _():
                landed(2, i)

        @pl.when(pair[0] < near)
        def _():
            attend(pair, False)

        @pl.when(pair[0] >= near)
        def _():
            attend(pair, True)

        for i in pair:

            @pl.when(i != chip)
            def _():
                remote(
                    ob.at[i], att.at[:, own], o_send.at[i], o_recv.at[chip], 2 * i + core, row
                ).start()

    att[:, own] = ob[chip]

    lw_mate.wait_recv()
    @pl.loop(0, width // tile)
    def _(index):
        block = pl.ds(pl.multiple_of(index * tile, tile), tile)
        summed = acc[block] + jnp.dot(
            ow_ref[block, pl.ds(pl.multiple_of(other * width, width), width)],
            lwb[...],
            preferred_element_type=f32,
        )
        w2[block] = summed.astype(bf)

    direct = jnp.dot(res_ref[...], lw_ref[...], preferred_element_type=f32)
    lif[...] = direct

    cot_copy.wait_recv()
    m_copy.wait_recv()
    bridge[...] = (mb[...].astype(f32) + mr[...].astype(f32)).astype(bf)
    belongs = (
        lax.broadcasted_iota(jnp.int32, (rows, total), 1) // PATCH
        == lax.broadcasted_iota(jnp.int32, (rows, total), 0)
    ).astype(f32).astype(bf)
    own_bytes = total // 2
    cot_sum = sum(
        jnp.dot(
            belongs[:, index * own_bytes : (index + 1) * own_bytes], cot_ref[index],
            preferred_element_type=f32,
        )
        for index in range(2)
    )

    def mates_weights_of(which, source):
        for line in (side, 1 - side):
            to_mate(which, source, line).wait_recv()

    def turn(source):
        lanes = pl.ds(pl.multiple_of(source * 2 * depth * shard, HEAD), 2 * depth * shard)
        wit[:, lanes] = jnp.transpose(wi[lanes])

    for hop in range(3, levels):
        relay(hop)
    for hop in range(2, levels - 1):
        cross_over(hop)
    for i in range(chips):

        @pl.when(i != chip)
        def _():
            back = remote(
                ob.at[i], att.at[:, heads_of(i)], o_send.at[i], o_recv.at[i], 2 * i + core, row
            )
            back.wait_recv()
            back.wait_send()

    e_copies = []
    red[...] = contract(gd_ref[...], att[...], 1, 1).astype(bf)
    red_copy = remote(red, redr, y_send.at[3], y_recv.at[3], me, other)
    red_copy.start()
    e1[...] = (
        jnp.dot(att[...], w2[...], preferred_element_type=f32) + lif[...]
    ).astype(bf)
    for index in range(pieces):
        patches = pl.ds(index * per_piece, per_piece)
        copy = remote(e1.at[patches], e1r.at[patches], e_send.at[index], e_recv.at[index], me, other)
        copy.start()
        e_copies.append(copy)
    mates_weights_of(0, level)
    for hop in range(1, levels - 1):
        for source in (level - hop, level + hop):

            @pl.when((source >= 0) & (source < levels))
            def _():
                mates_weights_of(0, source)
                turn(source)

    cross_over(levels - 1)
    turn(level)
    wit[:, columns:] = jnp.transpose(wi[columns:])
    red_copy.wait_recv()
    reduced = red[...].astype(f32) + redr[...].astype(f32)
    scaled = (reduced * task_scales).astype(bf)
    lifted = contract(scaled, bridge[...], 0, 0)

    lif[...] = lifted

    @pl.loop(0, pieces)
    def _(index):
        block = pl.ds(pl.multiple_of(index * SPAN, SPAN), SPAN)
        patches = pl.ds(pl.multiple_of(index * per_piece, per_piece), per_piece)
        remote(
            e1.at[patches], e1r.at[patches], e_send.at[index], e_recv.at[index], me, other
        ).wait_recv()
        projected = (
            e1[patches].astype(f32) + e1r[patches].astype(f32) + lif[patches]
        ).astype(bf)
        near_by = (
            lax.broadcasted_iota(jnp.int32, (per_piece, SPAN), 1) // PATCH
            == lax.broadcasted_iota(jnp.int32, (per_piece, SPAN), 0)
        ).astype(f32).astype(bf)
        inputs = inp[block] + contract(near_by, projected, 0, 0)
        scales = sca[block]
        inverse = lax.rsqrt(jnp.mean(inputs * inputs, axis=1, keepdims=True) + 1e-06)
        normed = (inputs * inverse * gain_ref[...]).astype(bf)
        lowered = contract(normed, ld_ref[...], 1, 1)
        inp[block] = inputs
        inv[block] = jnp.broadcast_to(inverse, (SPAN, HEAD))
        low[block] = lowered
        nrm[block, :columns] = normed
        nrm[block, columns:] = (lowered * scales).astype(bf)

    for source in range(levels):
        mates_weights_of(1, source)
    for source in (level - (levels - 1), level + (levels - 1)):

        @pl.when((source >= 0) & (source < levels))
        def _():
            mates_weights_of(0, source)
            turn(source)

    @pl.loop(0, pieces)
    def _(index):
        block = pl.ds(pl.multiple_of(index * SPAN, SPAN), SPAN)
        upper = jnp.dot(nrm[block], wi[...], preferred_element_type=f32)
        inner = pl.ds(pl.multiple_of(lax.rem(index * SPAN, own_bytes), SPAN), SPAN)
        through = jnp.dot(
            cot_ref[index * SPAN // own_bytes, inner], wo[...], preferred_element_type=f32
        )
        grown = (through * gelu_slope(upper)).astype(bf)
        gr[block] = grown
        both = jnp.dot(grown, wit[...], preferred_element_type=f32)
        back_rank = both[:, columns:]
        moved = (back_rank * sca[block]).astype(bf)
        mv[block] = moved
        bl[block] = back_rank * low[block]
        back_total = both[:, :columns] + jnp.dot(
            moved, ld_ref[...], preferred_element_type=f32
        )
        inputs = inp[block]
        inverse = inv[block][:, :1]
        gained = back_total * gain_ref[...]
        average = jnp.mean(gained * inputs, axis=1, keepdims=True)
        back_inputs = inverse * (gained - inputs * (inverse * inverse * average))
        near = (
            lax.broadcasted_iota(jnp.int32, (per_piece, SPAN), 1) // PATCH
            == lax.broadcasted_iota(jnp.int32, (per_piece, SPAN), 0)
        ).astype(f32).astype(bf)
        patches = pl.ds(pl.multiple_of(index * per_piece, per_piece), per_piece)
        bp[patches] = jnp.dot(
            near, back_inputs.astype(bf), preferred_element_type=f32
        ).astype(bf)
        remote(
            bp.at[patches], bpr.at[patches], b_send.at[index], b_recv.at[index], me, other
        ).start()

    down = contract(mv[...], nrm[:, :columns], 0, 0)[:rank]
    high, low_part = split_pair(bl[...])
    by_patch = jnp.dot(belongs, high, preferred_element_type=f32) + jnp.dot(
        belongs, low_part, preferred_element_type=f32
    )
    small = exact(picks, by_patch, 1, 0)
    small = jnp.concatenate([small, jnp.zeros_like(small)], axis=0)
    down = down.astype(bf)
    lift = contract(nrm[:, columns:], gr[...], 0, 0)[:rank].astype(bf)
    spread = width // HEAD
    thin = columns // HEAD
    for t in range(spread):
        early[t] = lift[:, t * HEAD : (t + 1) * HEAD]
    for t in range(thin):
        early[spread + t] = down[:, t * HEAD : (t + 1) * HEAD]
    early[spread + thin] = small.astype(bf)
    base = chips // 4

    def owner(t):
        return 2 * (base + t) + 1

    def held(t):
        return pl.ds(0, min(share_of, tiles - t * share_of))

    def parcel(kind, t):
        source, landing = (early, late)[kind], (early_in, late_in)[kind]
        size = min(share_of, tiles - t * share_of)
        return remote(
            source.at[pl.ds(share_of * t, size)], landing.at[me, held(t)], r_send.at[kind, t],
            r_recv.at[kind, me], owner(t), row,
        )

    def spread_out(kind):
        for t in range(owners):

            @pl.when(owner(t) != me)
            def _():
                parcel(kind, t).start()

            @pl.when(owner(t) == me)
            def _():
                size = min(share_of, tiles - t * share_of)
                source, landing = (early, late)[kind], (early_in, late_in)[kind]
                landing[me, :size] = source[share_of * t : share_of * t + size]

    def settle_out(kind):
        for t in range(owners):

            @pl.when(owner(t) != me)
            def _():
                parcel(kind, t).wait_send()

    def gather_in(kind, final):
        landing = (early_in, late_in)[kind]
        for t in range(owners):

            @pl.when(owner(t) == me)
            def _():
                size = min(share_of, tiles - t * share_of)
                for d in range(1, count):
                    source = lax.rem(me + d, count)
                    remote(
                        landing.at[source, held(t)], landing.at[source, held(t)],
                        r_send.at[kind, 0], r_recv.at[kind, source], me, row,
                    ).wait_recv()
                summed = jnp.sum(landing[:, :size].astype(f32), axis=0)
                if kind == 0 and t * share_of >= spread:
                    cross[:size] = summed.astype(bf)
                    swap = remote(
                        cross.at[held(t)], crossr.at[held(t)], y_send.at[4], y_recv.at[4], me, other
                    )
                    swap.start()
                    swap.wait_recv()
                    summed = cross[:size].astype(f32) + crossr[:size].astype(f32)
                final[t, :size] = summed.astype(bf)
                for d in range(1, count):
                    issue(kind, final, t, d).start()

    def issue(kind, final, t, d):
        piece = final.at[t, held(t)]
        return remote(
            piece, piece, g_send.at[kind, d], g_recv.at[kind, t], lax.rem(me + d, count), row
        )

    def finish_in(kind, final):
        for t in range(owners):

            @pl.when(owner(t) != me)
            def _():
                piece = final.at[t, held(t)]
                remote(
                    piece, piece, g_send.at[kind, 0], g_recv.at[kind, t], me, row
                ).wait_recv()

    def settle_in(kind, final):
        for t in range(owners):

            @pl.when(owner(t) == me)
            def _():
                for d in range(1, count):
                    issue(kind, final, t, d).wait_send()
                if kind == 0 and t * share_of >= spread:
                    remote(
                        cross.at[held(t)], crossr.at[held(t)], y_send.at[4], y_recv.at[4], me, other
                    ).wait_send()

    spread_out(0)

    for index in range(pieces):
        patches = pl.ds(index * per_piece, per_piece)
        remote(
            bp.at[patches], bpr.at[patches], b_send.at[index], b_recv.at[index], me, other
        ).wait()
    patch_grad = (bp[...].astype(f32) + bpr[...].astype(f32) + cot_sum).astype(bf)
    pulled = jnp.dot(scaled, patch_grad, preferred_element_type=f32).astype(bf)
    back_scaled = contract(bridge[...], patch_grad, 1, 1)
    back_reduced = (back_scaled * task_scales).astype(bf)
    outward = jnp.dot(back_reduced, att[...], preferred_element_type=f32).astype(bf)
    product = back_scaled * reduced
    product = jnp.concatenate([product, jnp.zeros((HEAD - rank, rows), f32)], axis=0)
    tops = exact(picks, product, 1, 1)
    tops = jnp.concatenate([tops, jnp.zeros_like(tops)], axis=0)
    for t in range(spread):
        late[t] = outward[:, t * HEAD : (t + 1) * HEAD]
    for t in range(thin):
        late[spread + t] = pulled[:, t * HEAD : (t + 1) * HEAD]
    late[spread + thin] = tops.astype(bf)
    spread_out(1)
    gather_in(0, early_full)
    gather_in(1, late_full)
    finish_in(0, early_full)

    def tile_of(final, t):
        return final[t // share_of, t % share_of]

    for t in range(spread):
        glu_out[:, t * HEAD : (t + 1) * HEAD] = tile_of(early_full, t).astype(f32)
    for t in range(thin):
        gld_out[:, t * HEAD : (t + 1) * HEAD] = tile_of(early_full, spread + t).astype(f32)
    lsc_out[...] = tile_of(early_full, spread + thin)[:TASKS, :rank].astype(f32)
    settle_out(0)
    settle_in(0, early_full)
    settle_out(1)
    for which, buffer in weights_in:
        for source in range(levels):
            settle_along(which, source)
            across(which, source, side).wait_send()
            for line in (side, 1 - side):
                to_mate(which, source, line).wait_send()
    for to in targets:
        for which in range(3):
            hand(which, to).wait_send()
    for source in range(chips):
        for which in range(2):
            share(which, source).wait_send()
    for copy in [lw_copy, lw_mate, cot_copy, m_copy, red_copy] + e_copies:
        copy.wait_send()
    finish_in(1, late_full)
    for t in range(spread):
        ggd_out[:, t * HEAD : (t + 1) * HEAD] = tile_of(late_full, t).astype(f32)
    for t in range(thin):
        bridge[:, t * HEAD : (t + 1) * HEAD] = tile_of(late_full, spread + t)
    ggu_out[...] = contract(bridge[...], lw_ref[...], 1, 1)
    gsc_out[...] = tile_of(late_full, spread + thin)[:TASKS, :rank].astype(f32)
    settle_in(1, late_full)


def copy_kernel(*refs):
    number = len(refs) // 2
    for source, target in zip(refs[:number], refs[number:]):
        target[...] = source[...]


def paired_body(
    patch_queries, patch_keys, patch_values, patch_tasks, residual, output_weight, global_down,
    global_up, global_scales, local_weight, byte_ids, byte_table, position_table, norm_gain,
    hidden_in, hidden_out, local_down, local_up, local_scales, cotangent,
):
    count = lax.axis_size("seq")
    rows, width = patch_queries.shape
    chips = count // 2
    depth = 2
    levels = chips // depth
    columns = local_weight.shape[1]
    rank = global_up.shape[0]
    vocab = byte_table.shape[0]
    total = byte_ids.shape[0]
    wide = columns + HEAD
    pieces = total // SPAN
    bf, f32 = jnp.bfloat16, jnp.float32
    vm = pltpu.VMEM
    dma = pltpu.SemaphoreType.DMA
    args = (
        patch_queries, patch_keys, patch_values, patch_tasks.reshape(1, rows), residual,
        output_weight, jnp.transpose(global_down), global_up, global_scales, local_weight,
        byte_ids.reshape(1, total), byte_table, position_table, norm_gain.reshape(1, columns),
        jnp.transpose(hidden_in), jnp.transpose(hidden_out), jnp.transpose(local_down), local_up,
        local_scales, cotangent,
    )
    outs = pl.pallas_call(
        functools.partial(step_kernel, chips, depth),
        out_shape=(
            jax.ShapeDtypeStruct((rank, width), f32),
            jax.ShapeDtypeStruct((rank, width), f32),
            jax.ShapeDtypeStruct((TASKS, rank), f32),
            jax.ShapeDtypeStruct((rank, columns), f32),
            jax.ShapeDtypeStruct((rank, width), f32),
            jax.ShapeDtypeStruct((TASKS, rank), f32),
        ),
        in_specs=[pl.BlockSpec(memory_space=pl.ANY)] * len(args),
        out_specs=(pl.BlockSpec(memory_space=vm),) * 6,
        scratch_shapes=[
            vm((rows, width), bf), vm((rows, width), bf), vm((rows, width), bf),
            vm((1, rows), jnp.int32), vm((rows, width), bf), vm(output_weight.shape, bf),
            vm((rank, width), bf), vm((rank, width), bf), vm((TASKS, rank), f32),
            vm((width, columns), bf), vm((1, total), jnp.int32), vm((PATCH, columns), bf),
            vm((1, columns), f32), vm((HEAD, columns), bf), vm((TASKS, rank), f32),
            vm((2, total // 2, columns), bf), vm((wide, width), bf), vm((columns, width), bf),
            vm((width, wide), bf),
            vm((chips, rows, HEAD), bf), vm((count, rows, HEAD), bf), vm((count, rows, HEAD), bf),
            vm((chips, rows, HEAD), bf), vm((rows, width), bf), vm((width, columns), bf),
            vm((width, columns), bf), vm((width, columns), f32), vm((rows, columns), bf),
            vm((rows, columns), bf), vm((rank, columns), bf), vm((rank, columns), bf),
            vm((rank, columns), bf), vm((rank, rows), bf), vm((rank, rows), bf),
            vm((rows, columns), f32),
            vm((vocab + 2 * HEAD, wide + HEAD), bf), vm((total, columns), f32),
            vm((total, wide), bf), vm((total, HEAD), f32), vm((total, HEAD), f32),
            vm((total, HEAD), f32), vm((total, HEAD), f32), vm((total, width), bf),
            vm((total, HEAD), bf), vm((rows, columns), bf), vm((rows, columns), bf),
            vm((4, rank, HEAD), bf), vm((4, rank, HEAD), bf),
        ]
        + [
            vm((count, rank, HEAD), bf), vm((count, 4, rank, HEAD), bf),
            vm((chips // 2, 4, rank, HEAD), bf),
        ]
        * 2
        + [
            dma((len(args),)), dma((3, chips)), dma((3, chips)), dma((2, chips)), dma((2, chips)),
            dma((chips,)), dma((chips,)), dma((2, levels, 2)), dma((2, levels)), dma((2, levels)),
            dma((2, levels)), dma((2, chips)), dma((2, chips)), dma((1,)), dma((1,)), dma((5,)),
            dma((5,)), dma((pieces,)), dma((pieces,)), dma((pieces,)), dma((pieces,)),
            dma((2, chips)), dma((2, count)), dma((2, count)), dma((2, chips)),
        ],
        compiler_params=pltpu.CompilerParams(
            collective_id=0, has_side_effects=True, vmem_limit_bytes=60 * 1024 * 1024
        ),
        name="step",
    )(*args)
    ggd, ggu, gsc, gld, glu, lsc = pl.pallas_call(
        copy_kernel,
        out_shape=tuple(jax.ShapeDtypeStruct(item.shape, item.dtype) for item in outs),
        in_specs=[pl.BlockSpec(memory_space=vm)] * len(outs),
        out_specs=(pl.BlockSpec(memory_space=vm),) * len(outs),
        name="spill",
    )(*outs)
    return (jnp.transpose(ggd), ggu, gsc, jnp.transpose(gld), glu, lsc)


def pick_body(seq_count, row_count, *args):
    heads = args[0].shape[1] // HEAD
    rank = args[7].shape[0]
    hidden = args[14].shape[0]
    fits = (
        row_count == 2
        and seq_count == 2 * heads
        and heads % 4 == 0
        and rank == 2 * TASKS
        and args[0].shape[1] == hidden
        and (4 * rank * hidden) % (seq_count * 16 * HEAD) == 0
        and hidden // HEAD + args[9].shape[1] // HEAD < seq_count
        and args[0].shape[0] == HEAD
    )
    return paired_body(*args) if fits else general_body(*args)


def solution(mesh):
    placed = (
        P("seq", "row"),
        P("seq", "row"),
        P("seq", "row"),
        P("seq"),
        P("seq", "row"),
        P("row", None),
        P("row", None),
        P(None, "row"),
        P(),
        P("row", None),
        P("seq"),
        P(),
        P(),
        P(),
        P("row", "seq"),
        P("row", "seq"),
        P(),
        P(None, "row"),
        P(),
        P(("seq", "row"), None),
    )
    chosen = functools.partial(pick_body, mesh.shape["seq"], mesh.shape["row"])
    return jax.shard_map(
        chosen,
        mesh=mesh,
        in_specs=placed,
        out_specs=(P("row", None), P(None, "row"), P(), P(), P(None, "row"), P()),
        check_vma=False,
    )
```
